32 devices in a mesh: dp: 1 (over z), sp: 32 (over y, x, core).
Axes of the slice: x: 4, y: 4, z: 1, core: 2. Of those that a mesh axis runs over, the one named last changes fastest.
The devices are a block of a 4x4x8 slice.
Arguments:
- hidden: bfloat16 [8, 4096, 4096], P('dp', 'sp')
- pos_ids: int32 [8, 4096], P('dp', 'sp')
- block_ids: int32 [8, 4096], P('dp', 'sp')
- ctx_len: int32 [8], P('dp')
- ln_gamma: bfloat16 [4096], replicated
- ln_beta: bfloat16 [4096], replicated
- w_qkv: bfloat16 [4096, 32, 3, 128], replicated
- b_qkv: bfloat16 [32, 3, 128], replicated
- w_dense: bfloat16 [4096, 4096], replicated
- b_dense: bfloat16 [4096], replicated
Outputs:
- output 1: bfloat16 [8, 4096, 4096], P('dp', 'sp')
- output 2: bfloat16 [8, 4096, 32, 128], P('dp', None, 'sp')
- output 3: bfloat16 [8, 4096, 32, 128], P('dp', None, 'sp')
All inputs are finite; a program needn't handle non-finite values.
Results may differ from the reference program's by a relative error of at most 0.00685068.
Values are sent between devices in bfloat16 or wider.
A program may use at most 768 MiB of HBM per device.

```python
import math
import jax
import jax.numpy as jnp
from jax import lax

BATCH = 8
SEQ = 4096
HEADS = 32
HEAD = 128
HIDDEN = HEADS * HEAD
ALPHA = math.sqrt(56.0)
ROPE_BASE = 10000.0
LN_EPS = 1e-5
SCORE_SCALE = 1.0 / math.sqrt(HEAD)
QUERY_BLOCK = min(SEQ, 128)
GAIN = 1.0 / ALPHA
QKV_SCALE = ALPHA / math.sqrt(HIDDEN)
DENSE_SCALE = 0.5 * math.sqrt(SEQ / HIDDEN)
BIAS_SCALE = 1.0 / math.sqrt(SEQ)


def draw_positions(ctx_key, mask_key):
    ctx_len = jax.random.randint(ctx_key, (BATCH,), SEQ // 4, 3 * SEQ // 4 + 1, dtype=jnp.int32)
    mask_pos = jax.random.randint(mask_key, (BATCH,), 0, ctx_len, dtype=jnp.int32)
    token_pos = jnp.arange(SEQ, dtype=jnp.int32)[None, :]
    in_context = token_pos < ctx_len[:, None]
    pos_ids = jnp.where(in_context, token_pos, mask_pos[:, None]).astype(jnp.int32)
    block_ids = jnp.where(in_context, 0, token_pos - ctx_len[:, None] + 1).astype(jnp.int32)
    return pos_ids, block_ids, ctx_len


def setup_inputs(seed: int = 0, part: int = 0) -> dict:
    base_key = jax.random.key(seed)
    shared_key, part_key = jax.random.split(base_key)
    part_key = jax.random.fold_in(part_key, part)
    key_x, key_ctx, key_mask = jax.random.split(part_key, 3)
    key_g, key_b, key_w, key_wb, key_d, key_db = jax.random.split(shared_key, 6)
    pos_ids, block_ids, ctx_len = draw_positions(key_ctx, key_mask)
    hidden = jax.random.normal(key_x, (BATCH, SEQ, HIDDEN), jnp.float32)
    ln_gamma = (1.0 + 0.2 * jax.random.normal(key_g, (HIDDEN,), jnp.float32)) * GAIN
    ln_beta = jax.random.normal(key_b, (HIDDEN,), jnp.float32) * (GAIN * BIAS_SCALE)
    w_qkv = jax.random.normal(key_w, (HIDDEN, HEADS, 3, HEAD), jnp.float32) * QKV_SCALE
    b_qkv = jax.random.normal(key_wb, (HEADS, 3, HEAD), jnp.float32) * BIAS_SCALE
    w_dense = jax.random.normal(key_d, (HIDDEN, HIDDEN), jnp.float32) * DENSE_SCALE
    b_dense = jax.random.normal(key_db, (HIDDEN,), jnp.float32) * 0.5
    return {'hidden': hidden.astype(jnp.bfloat16), 'pos_ids': pos_ids, 'block_ids': block_ids, 'ctx_len': ctx_len, 'ln_gamma': ln_gamma.astype(jnp.bfloat16), 'ln_beta': ln_beta.astype(jnp.bfloat16), 'w_qkv': w_qkv.astype(jnp.bfloat16), 'b_qkv': b_qkv.astype(jnp.bfloat16), 'w_dense': w_dense.astype(jnp.bfloat16), 'b_dense': b_dense.astype(jnp.bfloat16)}


def layer_norm(hidden, ln_gamma, ln_beta):
    wide_in = hidden.astype(jnp.float32)
    row_mean = jnp.mean(wide_in, axis=-1, keepdims=True)
    centered = wide_in - row_mean
    row_var = jnp.mean(jnp.square(centered), axis=-1, keepdims=True)
    return (centered * lax.rsqrt(row_var + LN_EPS) * ln_gamma.astype(jnp.float32) + ln_beta.astype(jnp.float32)).astype(jnp.bfloat16)


def rotate(heads_in, pos_ids, block_ids):
    half_dim = heads_in.shape[-1] // 2
    quarter_dim = half_dim // 2
    inv_freq = ROPE_BASE ** (-jnp.arange(0, half_dim, 2).astype(jnp.float32) / half_dim)
    angles = jnp.stack([pos_ids, block_ids], axis=-1).astype(jnp.float32)[..., None] * inv_freq
    cos_a = jnp.cos(angles)[:, :, None]
    sin_a = jnp.sin(angles)[:, :, None]
    split_dims = heads_in.astype(jnp.float32).reshape(heads_in.shape[:-1] + (2, 2, quarter_dim))
    low_part = split_dims[..., 0, :]
    high_part = split_dims[..., 1, :]
    new_low = low_part * cos_a - high_part * sin_a
    new_high = high_part * cos_a + low_part * sin_a
    return jnp.stack([new_low, new_high], axis=-2).reshape(heads_in.shape).astype(jnp.bfloat16)


def reference(hidden, pos_ids, block_ids, ctx_len, ln_gamma, ln_beta, w_qkv, b_qkv, w_dense, b_dense):
    normed = layer_norm(hidden, ln_gamma, ln_beta)
    qkv_flat = jnp.dot(normed.reshape(BATCH * SEQ, HIDDEN), w_qkv.reshape(HIDDEN, 3 * HIDDEN), preferred_element_type=jnp.float32)
    qkv_proj = (qkv_flat.reshape(BATCH, SEQ, HEADS, 3, HEAD) + b_qkv.astype(jnp.float32)).astype(jnp.bfloat16)
    query_rot = rotate(qkv_proj[:, :, :, 0], pos_ids, block_ids)
    key_rot = rotate(qkv_proj[:, :, :, 1], pos_ids, block_ids)
    value_heads = qkv_proj[:, :, :, 2]
    key_pos = jnp.arange(SEQ)
    ctx_visible = key_pos[None, None, :] < ctx_len[:, None, None]

    def one_head(head_args):
        q_head, k_head, v_head = head_args
        k_wide = k_head.astype(jnp.float32)
        v_wide = v_head.astype(jnp.float32)

        def one_block(block_idx):
            block_start = block_idx * QUERY_BLOCK
            q_block = lax.dynamic_slice_in_dim(q_head, block_start, QUERY_BLOCK, axis=1).astype(jnp.float32)
            scores = jnp.einsum('bqe,bke->bqk', q_block, k_wide) * SCORE_SCALE
            q_pos = block_start + jnp.arange(QUERY_BLOCK)
            visible = ctx_visible | (key_pos[None, None, :] <= q_pos[None, :, None])
            attn_probs = jax.nn.softmax(jnp.where(visible, scores, -jnp.inf), axis=-1).astype(jnp.bfloat16)
            return jnp.einsum('bqk,bke->bqe', attn_probs.astype(jnp.float32), v_wide).astype(jnp.bfloat16)

        blocks = lax.map(one_block, jnp.arange(SEQ // QUERY_BLOCK))
        return jnp.moveaxis(blocks, 0, 1).reshape(BATCH, SEQ, HEAD)

    head_major = (jnp.moveaxis(query_rot, 2, 0), jnp.moveaxis(key_rot, 2, 0), jnp.moveaxis(value_heads, 2, 0))
    context = lax.map(one_head, head_major)
    context = jnp.moveaxis(context, 0, 2).reshape(BATCH * SEQ, HIDDEN)
    dense_out = jnp.dot(context, w_dense, preferred_element_type=jnp.float32) + b_dense.astype(jnp.float32)
    block_out = (normed.reshape(BATCH * SEQ, HIDDEN).astype(jnp.float32) * ALPHA + dense_out).astype(jnp.bfloat16)
    return block_out.reshape(BATCH, SEQ, HIDDEN), key_rot, value_heads
```

```python
import functools
import math

import jax
import jax.numpy as jnp
from jax import lax
from jax.experimental import pallas as pl
from jax.experimental.pallas import tpu as pltpu
from jax.sharding import PartitionSpec as P

ALPHA = math.sqrt(56.0)
ROPE_BASE = 10000.0
LN_EPS = 1e-5
F32 = jnp.float32
BF16 = jnp.bfloat16
VMEM_CAP = 60000 * 1024


def ln_kernel(x_ref, g_ref, b_ref, o_ref):
    x = x_ref[...].astype(F32)
    mean = jnp.mean(x, axis=-1, keepdims=True)
    cent = x - mean
    var = jnp.mean(jnp.square(cent), axis=-1, keepdims=True)
    o_ref[...] = (cent * lax.rsqrt(var + LN_EPS) * g_ref[...].astype(F32) + b_ref[...].astype(F32)).astype(BF16)


def layer_norm(x, gamma, beta, tile):
    tokens, width = x.shape
    return pl.pallas_call(
        ln_kernel,
        grid=(tokens // tile,),
        in_specs=[
            pl.BlockSpec((tile, width), lambda i: (i, 0)),
            pl.BlockSpec((1, width), lambda i: (0, 0)),
            pl.BlockSpec((1, width), lambda i: (0, 0)),
        ],
        out_specs=pl.BlockSpec((tile, width), lambda i: (i, 0)),
        out_shape=jax.ShapeDtypeStruct((tokens, width), BF16),
        cost_estimate=pl.CostEstimate(flops=tokens * width * 10, bytes_accessed=tokens * width * 4, transcendentals=0),
        name="ln",
    )(x, gamma.reshape(1, width), beta.reshape(1, width))


def qkv_kernel(rotary, k_tile, a_ref, w_ref, b_ref, cos_ref, sin_ref, o_ref, wb, acc):
    depth, _, group, dim = w_ref.shape
    for step in range(depth // k_tile):
        rows = pl.ds(step * k_tile, k_tile)
        sub = min(64, k_tile)
        for part in range(k_tile // sub):
            lo = step * k_tile + part * sub
            tile = jnp.swapaxes(w_ref[lo:lo + sub, 0], 0, 1)
            for head in range(group):
                wb[lo:lo + sub, head * dim:(head + 1) * dim] = tile[head]
        prod = jnp.dot(a_ref[:, rows], wb[rows, :], preferred_element_type=F32)
        if step == 0:
            acc[...] = prod
        else:
            acc[...] += prod
    for head in range(group):
        x = acc[:, head * dim:(head + 1) * dim] + b_ref[0, 0, head:head + 1, :].astype(F32)
        x = x.astype(BF16)
        if rotary:
            x = x.astype(F32)
            lane = lax.broadcasted_iota(jnp.int32, x.shape, 1)
            low = lax.rem(lane, dim // 2) < dim // 4
            pair = jnp.where(low, pltpu.roll(x, dim - dim // 4, 1), pltpu.roll(x, dim // 4, 1))
            x = (x * cos_ref[...] + pair * sin_ref[...]).astype(BF16)
        o_ref[head] = x


def qkv_part(normed, w_rows, bias, cos_t, sin_t, kind, first, tokens, group=8):
    depth, _, heads, dim = w_rows.shape
    base = first // tokens
    return pl.pallas_call(
        functools.partial(qkv_kernel, kind < 2, depth // 4),
        grid=(heads // group,),
        in_specs=[
            pl.BlockSpec((tokens, depth), lambda i: (base, 0)),
            pl.BlockSpec((depth, 1, group, dim), lambda i: (0, kind, i, 0)),
            pl.BlockSpec((1, 1, group, dim), lambda i: (0, kind, i, 0)),
            pl.BlockSpec((tokens, dim), lambda i: (base, 0)),
            pl.BlockSpec((tokens, dim), lambda i: (base, 0)),
        ],
        out_specs=pl.BlockSpec((group, tokens, dim), lambda i: (i, 0, 0)),
        out_shape=jax.ShapeDtypeStruct((heads, tokens, dim), BF16),
        scratch_shapes=[pltpu.VMEM((depth, group * dim), BF16), pltpu.VMEM((tokens, group * dim), F32)],
        compiler_params=pltpu.CompilerParams(vmem_limit_bytes=VMEM_CAP),
        cost_estimate=pl.CostEstimate(flops=2 * tokens * depth * heads * dim, bytes_accessed=2 * depth * heads * dim, transcendentals=0),
        name="qkv",
    )(normed, w_rows, bias, cos_t, sin_t)


def attn_kernel(row0, q_sub, n_sub, k_blk, ctx_ref, q_ref, k_ref, v_ref, _ka, _va, o_ref, ko_ref, vo_ref, vt, m_s, l_s, acc_s):
    chunks, _, chunk, dim = q_ref.shape
    seq = chunks * chunk
    ctx = ctx_ref[row0 + pl.program_id(0)]
    coef = math.log2(math.e) / math.sqrt(dim)
    ko_ref[...] = k_ref[...].reshape(ko_ref.shape)
    vo_ref[...] = v_ref[...].reshape(vo_ref.shape)
    step_v = 512
    for c in range(seq // step_v):
        n = step_v // chunk
        vt[:, c * step_v:(c + 1) * step_v] = v_ref[c * n:(c + 1) * n].reshape(step_v, dim).T
    q_blk = q_sub * n_sub
    per = q_sub // chunk

    def q_loop(qi, _):
        q0 = qi * q_blk
        for s in range(n_sub):
            m_s[s] = jnp.full(m_s.shape[1:], -jnp.inf, F32)
            l_s[s] = jnp.zeros(l_s.shape[1:], F32)
            acc_s[s] = jnp.zeros(acc_s.shape[1:], F32)

        def block(ki, masked):
            kn = k_blk // chunk
            k_tile = k_ref[pl.ds(ki * kn, kn)].reshape(k_blk, dim)
            v_tile = vt[:, pl.ds(pl.multiple_of(ki * k_blk, k_blk), k_blk)]
            for s in range(n_sub):
                q_tile = q_ref[pl.ds(qi * (n_sub * per) + s * per, per)].reshape(q_sub, dim)
                sc = lax.dot_general(k_tile, q_tile, (((1,), (1,)), ((), ())), preferred_element_type=F32) * coef
                if masked:
                    kpos = ki * k_blk + lax.broadcasted_iota(jnp.int32, sc.shape, 0)
                    qpos = q0 + s * q_sub + lax.broadcasted_iota(jnp.int32, sc.shape, 1)
                    sc = jnp.where((kpos < ctx) | (kpos <= qpos), sc, -jnp.inf)
                m_old = m_s[s]
                m_new = jnp.maximum(m_old, jnp.max(sc, axis=0, keepdims=True))
                scale = jnp.exp2(m_old - m_new)
                p = jnp.exp2(sc - m_new)
                part = jnp.sum(p.reshape(k_blk // 8, 8, q_sub), axis=0)
                l_s[s] = l_s[s] * scale + part
                m_s[s] = m_new
                acc_s[s] = acc_s[s] * scale + jnp.dot(v_tile, p.astype(BF16), preferred_element_type=F32)

        full = jnp.maximum(ctx, q0 + 1) // k_blk
        last = (jnp.maximum(ctx, q0 + q_blk) + k_blk - 1) // k_blk
        lax.fori_loop(0, full, lambda i, c: (block(i, False), c)[1], 0)
        lax.fori_loop(full, last, lambda i, c: (block(i, True), c)[1], 0)
        for s in range(n_sub):
            inv = 1.0 / jnp.sum(l_s[s], axis=0, keepdims=True)
            out = (acc_s[s] * inv).T.astype(BF16)
            o_ref[pl.ds(qi * (n_sub * per) + s * per, per)] = out.reshape(per, 1, chunk, dim)
        return 0

    lax.fori_loop(0, seq // q_blk, q_loop, 0)


def attention(ctx_len, q, k, v, keys_buf, values_buf, half_row, row0, rows, q_sub=256, n_sub=2, k_blk=512):
    chunks, _, chunk, dim = q.shape
    seq = chunks * chunk
    total = keys_buf.shape[0]
    blk = pl.BlockSpec((chunks, 1, chunk, dim), lambda i, c: (0, half_row + i, 0, 0))
    out_blk = pl.BlockSpec((1, seq, dim), lambda i, c: (row0 + i, 0, 0))
    any_spec = pl.BlockSpec(memory_space=pl.ANY)
    return pl.pallas_call(
        functools.partial(attn_kernel, row0, q_sub, n_sub, k_blk),
        grid_spec=pltpu.PrefetchScalarGridSpec(
            num_scalar_prefetch=1,
            grid=(rows,),
            in_specs=[blk, blk, blk, any_spec, any_spec],
            out_specs=[pl.BlockSpec((chunks, 1, chunk, dim), lambda i, c: (0, i, 0, 0)), out_blk, out_blk],
            scratch_shapes=[
                pltpu.VMEM((dim, seq), BF16),
                pltpu.VMEM((n_sub, 1, q_sub), F32),
                pltpu.VMEM((n_sub, 8, q_sub), F32),
                pltpu.VMEM((n_sub, dim, q_sub), F32),
            ],
        ),
        out_shape=[
            jax.ShapeDtypeStruct((chunks, rows, chunk, dim), BF16),
            jax.ShapeDtypeStruct((total, seq, dim), BF16),
            jax.ShapeDtypeStruct((total, seq, dim), BF16),
        ],
        input_output_aliases={4: 1, 5: 2},
        compiler_params=pltpu.CompilerParams(vmem_limit_bytes=VMEM_CAP),
        cost_estimate=pl.CostEstimate(flops=4 * rows * seq * seq * dim, bytes_accessed=12 * rows * seq * dim, transcendentals=rows * seq * seq),
        name="attn",
    )(ctx_len, q, k, v, keys_buf, values_buf)


def dense_kernel(c_ref, w_ref, a_ref, b_ref, _old, o_ref, lhs):
    heads, tokens, dim = c_ref.shape

    @pl.when(pl.program_id(0) == 0)
    def _():
        for h in range(heads):
            lhs[:, h * dim:(h + 1) * dim] = c_ref[h]

    acc = jnp.dot(lhs[...], w_ref[...], preferred_element_type=F32)
    out = a_ref[...].astype(F32) * ALPHA + (acc + b_ref[...].astype(F32))
    o_ref[...] = out.astype(BF16)


def dense(ctx_rows, w_dense, normed, bias, out_buf, chunk_id, tile=512):
    heads, tokens, dim = ctx_rows.shape
    depth, width = w_dense.shape
    return pl.pallas_call(
        dense_kernel,
        grid=(width // tile,),
        in_specs=[
            pl.BlockSpec((heads, tokens, dim), lambda i: (0, 0, 0)),
            pl.BlockSpec((depth, tile), lambda i: (0, i)),
            pl.BlockSpec((tokens, tile), lambda i: (chunk_id, i)),
            pl.BlockSpec((1, tile), lambda i: (0, i)),
            pl.BlockSpec(memory_space=pl.ANY),
        ],
        out_specs=pl.BlockSpec((tokens, tile), lambda i: (chunk_id, i)),
        out_shape=jax.ShapeDtypeStruct(out_buf.shape, BF16),
        scratch_shapes=[pltpu.VMEM((tokens, depth), BF16)],
        input_output_aliases={4: 0},
        compiler_params=pltpu.CompilerParams(vmem_limit_bytes=VMEM_CAP),
        cost_estimate=pl.CostEstimate(flops=2 * tokens * depth * width, bytes_accessed=2 * depth * width, transcendentals=0),
        name="dense",
    )(ctx_rows, w_dense, normed, bias.reshape(1, width), out_buf)


def blank_kernel(*refs):
    pass


def blank(shape):
    return pl.pallas_call(blank_kernel, out_specs=pl.BlockSpec(memory_space=pl.ANY), out_shape=jax.ShapeDtypeStruct(shape, BF16), name="blank")()


def rotary_tables(pos_ids, block_ids, dim):
    half = dim // 2
    inv_freq = ROPE_BASE ** (-jnp.arange(0, half, 2).astype(F32) / half)
    ang = jnp.stack([pos_ids, block_ids], axis=-1).reshape(-1, 2).astype(F32)[..., None] * inv_freq
    cos = jnp.cos(ang)
    sin = jnp.sin(ang)
    cos_t = jnp.stack([cos, cos], axis=2).reshape(-1, dim)
    sin_t = jnp.stack([-sin, sin], axis=2).reshape(-1, dim)
    return cos_t, sin_t


def solution(mesh):
    seq_spec = P('dp', 'sp', None)
    row_spec = P('dp', 'sp')
    head_spec = P('dp', None, 'sp', None)
    rep = P()
    devices = mesh.shape['sp']

    def local_block(hidden, pos_ids, block_ids, ctx_len, ln_gamma, ln_beta, w_qkv, b_qkv, w_dense, b_dense):
        rows, chunk, width = hidden.shape
        depth, heads, kinds, dim = w_qkv.shape
        seq = chunk * devices
        tokens = rows * chunk
        normed = layer_norm(hidden.reshape(tokens, width), ln_gamma, ln_beta, chunk)
        cos_t, sin_t = rotary_tables(pos_ids, block_ids, dim)
        w_rows = jnp.transpose(w_qkv, (0, 2, 1, 3))
        bias = jnp.transpose(b_qkv, (1, 0, 2)).reshape(1, kinds, heads, dim)
        halves = 2
        half_rows = rows // halves
        half_tokens = tokens // halves
        recv = []
        for hf in range(halves):
            parts = {}
            for kind in (1, 2, 0):
                out = qkv_part(normed, w_rows, bias, cos_t, sin_t, kind, hf * half_tokens, half_tokens)
                got = lax.all_to_all(out, 'sp', 0, 0, tiled=True)
                parts[kind] = got.reshape(devices, half_rows, chunk, dim)
            recv.append(parts)
        keys = blank((rows, seq, dim))
        values = blank((rows, seq, dim))
        per = 2
        backs = []
        for start in range(0, rows, per):
            parts = recv[start // half_rows]
            context, keys, values = attention(ctx_len, parts[0], parts[1], parts[2], keys, values, start % half_rows, start, per)
            backs.append(lax.all_to_all(context.reshape(devices, per * chunk, dim), 'sp', 0, 0, tiled=True))
        out = blank((tokens, width))
        for i, back in enumerate(backs):
            out = dense(back, w_dense, normed, b_dense, out, i)
        return out.reshape(rows, chunk, width), keys.reshape(rows, seq, 1, dim), values.reshape(rows, seq, 1, dim)

    return jax.shard_map(local_block, mesh=mesh, in_specs=(seq_spec, row_spec, row_spec, P('dp'), rep, rep, rep, rep, rep, rep), out_specs=(seq_spec, head_spec, head_spec), check_vma=False)
```

```python
import functools
import math

import jax
import jax.numpy as jnp
from jax import lax
from jax.experimental import pallas as pl
from jax.experimental.pallas import tpu as pltpu
from jax.sharding import PartitionSpec as P

ALPHA = math.sqrt(56.0)
ROPE_BASE = 10000.0
LN_EPS = 1e-5
CTX_LOW = 1024
CTX_HIGH = 3072
F32 = jnp.float32
BF16 = jnp.bfloat16
VMEM_CAP = 60000 * 1024
MESH_ID = pl.DeviceIdType.MESH


def rotary_tables(pos_ids, block_ids, dim):
    half = dim // 2
    inv_freq = ROPE_BASE ** (-jnp.arange(0, half, 2).astype(F32) / half)
    ang = jnp.stack([pos_ids, block_ids], axis=-1).reshape(-1, 2).astype(F32)[..., None] * inv_freq
    cos = jnp.cos(ang)
    sin = jnp.sin(ang)
    cos_t = jnp.stack([cos, cos], axis=2).reshape(-1, dim)
    sin_t = jnp.stack([-sin, sin], axis=2).reshape(-1, dim)
    return cos_t, sin_t


def split_sizes(rows, heads):
    return rows // 2, heads // 2


def exchange_kernel(cfg, ctx_ref, x_ref, g_ref, be_ref, w_ref, bias_ref, cos_ref, sin_ref,
                    a_out, snd, rc, c_snd, c_rc,
                    xb, ab, wbuf, wb0, wb1, acc, sb, qb, kb, vb, cb, vt, s_buf, p_buf, m_run, m_buf, a_buf, a_val, l_s, acc_s,
                    x_sem, a_sem, w_sem, l_sem, o_sem, snd_sem, rcv_sem, row_sem, c_sem, cs_sem, cr_sem):
    n, depth, k_tile, q_blk, k_blk, low, high = cfg
    _, heads, rows, chunk, dim = snd.shape
    half_rows, group = split_sizes(rows, heads)
    half_tok = half_rows * chunk
    seq = n * chunk
    pieces = 12
    chunks = depth // k_tile
    total = pieces * chunks
    me = lax.axis_index('sp')

    barrier = pltpu.get_barrier_semaphore()

    def greet(i, c):
        pl.semaphore_signal(barrier, inc=1, device_id={'sp': lax.rem(me + i, n)}, device_id_type=MESH_ID)
        return c

    def piece_of(p):
        hf = p // 6
        kind = lax.rem(lax.rem(p, 6) // 2 + 1, 3)
        hh = lax.rem(p, 2)
        return hf, kind, hh

    def w_copy(s):
        _, kind, hh = piece_of(s // chunks)
        c = lax.rem(s, chunks)
        slot = lax.rem(s, 4)
        return pltpu.make_async_copy(
            w_ref.at[pl.ds(pl.multiple_of(c * k_tile, k_tile), k_tile), kind, pl.ds(pl.multiple_of(hh * group, group), group)],
            wbuf.at[slot], w_sem.at[slot])

    def x_copy(hf):
        return pltpu.make_async_copy(x_ref.at[pl.ds(pl.multiple_of(hf * half_tok, half_tok), half_tok)], xb, x_sem)

    def a_copy(hf):
        return pltpu.make_async_copy(ab, a_out.at[pl.ds(pl.multiple_of(hf * half_tok, half_tok), half_tok)], a_sem)

    def l_copy(p):
        hf, kind, hh = piece_of(p)
        slot = lax.rem(p, 2)
        return pltpu.make_async_copy(
            sb.at[slot],
            snd.at[kind, pl.ds(pl.multiple_of(hh * group, group), group), pl.ds(hf * half_rows, half_rows)],
            l_sem.at[slot])

    def own_copy(p):
        hf, kind, hh = piece_of(p)
        slot = lax.rem(p, 2)
        return pltpu.make_async_copy(
            sb.at[slot, lax.rem(me, group)],
            rc.at[kind, pl.ds(hf * half_rows, half_rows), me],
            o_sem.at[slot])

    def mine(p):
        return piece_of(p)[2] == me // group

    def send(kind, head, pair):
        two = pl.ds(2 * pair, 2)
        return pltpu.make_async_remote_copy(
            src_ref=snd.at[kind, head, two], dst_ref=rc.at[kind, two, me],
            send_sem=snd_sem.at[pair], recv_sem=rcv_sem.at[pair],
            device_id={'sp': head}, device_id_type=MESH_ID)

    def c_send(dest, pair):
        two = pl.ds(2 * pair, 2)
        return pltpu.make_async_remote_copy(
            src_ref=c_snd.at[dest, two], dst_ref=c_rc.at[me, two],
            send_sem=cs_sem, recv_sem=cr_sem, device_id={'sp': dest}, device_id_type=MESH_ID)

    def layer_norm(hf):
        x_copy(hf).wait()
        tile = 16

        def body(i, c):
            at = pl.ds(pl.multiple_of(i * tile, tile), tile)
            x = xb[at, :].astype(F32)
            mean = jnp.mean(x, axis=-1, keepdims=True)
            cent = x - mean
            var = jnp.mean(jnp.square(cent), axis=-1, keepdims=True)
            ab[at, :] = (cent * lax.rsqrt(var + LN_EPS) * g_ref[...] + be_ref[...]).astype(BF16)
            return c

        lax.fori_loop(0, half_tok // tile, body, 0)
        a_copy(hf).start()

    def relayout(s, wb):
        slot = lax.rem(s, 4)
        sub = min(64, k_tile)
        for part in range(k_tile // sub):
            lo = part * sub
            tile = jnp.swapaxes(wbuf[slot, lo:lo + sub], 0, 1)
            for head in range(group):
                wb[lo:lo + sub, head * dim:(head + 1) * dim] = tile[head]

    def multiply(c, wb):
        lhs = ab[:, pl.ds(pl.multiple_of(c * k_tile, k_tile), k_tile)]
        wide = min(256, group * dim)
        for t in range(group * dim // wide):
            cols = slice(t * wide, (t + 1) * wide)
            acc[:, cols] += jnp.dot(lhs, wb[:, cols], preferred_element_type=F32)

    def epilogue(p):
        hf, kind, hh = piece_of(p)
        slot = lax.rem(p, 2)
        toks = pl.ds(pl.multiple_of(hf * half_tok, half_tok), half_tok)

        def biased(h):
            cols = pl.ds(pl.multiple_of(h * dim, dim), dim)
            x = acc[:, cols] + bias_ref[kind * heads + hh * group + h]
            acc[:, cols] = jnp.zeros((half_tok, dim), F32)
            return x.astype(BF16)

        @pl.when(kind < 2)
        def _():
            def body(h, c):
                x = biased(h).astype(F32)
                lane = lax.broadcasted_iota(jnp.int32, x.shape, 1)
                first = lax.rem(lane, dim // 2) < dim // 4
                pair = jnp.where(first, pltpu.roll(x, dim - dim // 4, 1), pltpu.roll(x, dim // 4, 1))
                x = (x * cos_ref[toks, :] + pair * sin_ref[toks, :]).astype(BF16)
                sb[slot, h] = x.reshape(half_rows, chunk, dim)
                return c

            lax.fori_loop(0, group, body, 0)

        @pl.when(kind == 2)
        def _():
            def body(h, c):
                sb[slot, h] = biased(h).reshape(half_rows, chunk, dim)
                return c

            lax.fori_loop(0, group, body, 0)

    def spread(i, count):
        quarter = count // 4
        return lax.rem(i, 4) * quarter + lax.rem(i // 4 + lax.rem(i, 4), quarter)

    def flush(p):
        hf, kind, hh = piece_of(p)
        l_copy(p).wait()

        @pl.when(mine(p))
        def _():
            own_copy(p).wait()

        def body(i, c):
            head = hh * group + lax.rem(spread(i, group) + me, group)

            @pl.when(head != me)
            def _():
                send(kind, head, 2 * hf).start()

            return c

        lax.fori_loop(0, group, body, 0)

        @pl.when(lax.rem(p, 6) == 5)
        def _():
            def late(i, c):
                which = i // heads
                head = lax.rem(spread(lax.rem(i, heads), heads) + me, heads)

                @pl.when(head != me)
                def _():
                    send(lax.rem(which + 1, 3), head, 2 * hf + 1).start()

                return c

            lax.fori_loop(0, 3 * heads, late, 0)

    x_copy(0).start()
    for s in range(3):
        w_copy(s).start()
    lax.fori_loop(1, n, greet, 0)
    acc[...] = jnp.zeros_like(acc)
    w_copy(0).wait()
    relayout(0, wb0)
    layer_norm(0)
    x_copy(1).start()
    pl.semaphore_wait(barrier, n - 1)

    def project(p, c):
        @pl.when(p == 6)
        def _():
            a_copy(0).wait()
            layer_norm(1)

        def steps(i, c):
            s = p * chunks + 2 * i
            w_copy(s + 1).wait()

            @pl.when(s + 2 < total)
            def _():
                w_copy(s + 2).wait()

            @pl.when(s + 3 < total)
            def _():
                w_copy(s + 3).start()

            @pl.when(s + 4 < total)
            def _():
                w_copy(s + 4).start()

            @pl.when((i == 1) & (p > 0))
            def _():
                flush(p - 1)

            relayout(s + 1, wb1)
            multiply(2 * i, wb0)
            relayout(s + 2, wb0)
            multiply(2 * i + 1, wb1)
            return c

        lax.fori_loop(0, chunks // 2, steps, 0)
        epilogue(p)
        l_copy(p).start()

        @pl.when(mine(p))
        def _():
            own_copy(p).start()

        return c

    lax.fori_loop(0, pieces, project, 0)
    flush(pieces - 1)
    a_copy(1).wait()

    coef = math.log2(math.e) / math.sqrt(dim)
    per = q_blk // chunk
    kn = k_blk // chunk
    ratio = q_blk // k_blk

    def row_copies(b, slot):
        return [pltpu.make_async_copy(rc.at[kind, b], buf.at[slot], row_sem.at[kind, slot])
                for kind, buf in ((0, qb), (1, kb), (2, vb))]

    def ctx_copies(b, slot):
        return [pltpu.make_async_copy(cb.at[slot], c_snd.at[:, b], c_sem.at[0, slot]),
                pltpu.make_async_copy(cb.at[slot, me], c_rc.at[me, b], c_sem.at[1, slot])]

    def attend_row(b, slot):
        ctx = ctx_ref[b]
        step_v = min(512, seq)
        for c in range(seq // step_v):
            m = step_v // chunk
            vt[:, c * step_v:(c + 1) * step_v] = vb[slot, c * m:(c + 1) * m].reshape(step_v, dim).T

        def q_loop(qi, _):
            q0 = qi * q_blk
            q_tile = qb[slot, pl.ds(qi * per, per)].reshape(q_blk, dim)

            def scores(j, s_slot, masked):
                k_tile_ = kb[slot, pl.ds(j * kn, kn)].reshape(k_blk, dim)
                s = lax.dot_general(k_tile_, q_tile, (((1,), (1,)), ((), ())), preferred_element_type=F32)
                if masked:
                    kpos = j * k_blk + lax.broadcasted_iota(jnp.int32, s.shape, 0)
                    lim = jnp.maximum(ctx, q0 + 1 + lax.broadcasted_iota(jnp.int32, (1, q_blk), 1))
                    s = jnp.where(kpos < lim, s, -jnp.inf)
                s_buf[s_slot] = s
                m_old = m_run[...]
                m_new = jnp.maximum(m_old, jnp.max(s, axis=0, keepdims=True) * coef)
                m_run[...] = m_new
                m_buf[s_slot] = m_new
                a_buf[s_slot] = jnp.exp2(m_old - m_new)

            def probs(s_slot):
                p = jnp.exp2(s_buf[s_slot] * coef - m_buf[s_slot])
                scale = a_buf[s_slot]
                l_s[...] = l_s[...] * scale + jnp.sum(p.reshape(k_blk // 8, 8, q_blk), axis=0)
                p_buf[s_slot] = p.astype(BF16)
                a_val[s_slot] = scale

            def values(j, s_slot):
                v_tile = vt[:, pl.ds(pl.multiple_of(j * k_blk, k_blk), k_blk)]
                acc_s[...] = acc_s[...] * a_val[s_slot] + jnp.dot(v_tile, p_buf[s_slot], preferred_element_type=F32)

            def pair(i, masked):
                values(2 * i, 0)
                probs(1)
                scores(2 * i + 2, 0, masked)
                values(2 * i + 1, 1)
                probs(0)
                scores(2 * i + 3, 1, masked)

            m_run[...] = jnp.full(m_run.shape, -jnp.inf, F32)
            l_s[...] = jnp.zeros_like(l_s)
            acc_s[...] = jnp.zeros_like(acc_s)
            scores(0, 0, False)
            scores(1, 1, False)
            probs(0)
            pairs = (jnp.maximum(high, q0 + q_blk) + 2 * k_blk - 1) // (2 * k_blk)
            full = jnp.maximum(low, q0) // (2 * k_blk) - 1
            lax.fori_loop(0, full, lambda i, c: (pair(i, False), c)[1], 0)
            lax.fori_loop(full, pairs - 1, lambda i, c: (pair(i, True), c)[1], 0)
            values(2 * pairs - 2, 0)
            probs(1)
            values(2 * pairs - 1, 1)
            inv = 1.0 / jnp.sum(l_s[...], axis=0, keepdims=True)
            cb[slot, pl.ds(qi * per, per)] = (acc_s[...] * inv).T.astype(BF16).reshape(per, chunk, dim)
            return 0

        lax.fori_loop(0, seq // q_blk, q_loop, 0)

    def attend_pair(pair, c):
        peers = pl.ds(0, n - 1)
        got = rc.at[:, pl.ds(2 * pair, 2), peers]
        pltpu.make_async_copy(got, got, rcv_sem.at[pair]).wait()
        for r in range(2):
            for copy in row_copies(2 * pair + r, r):
                copy.start()

        def one(r, c):
            for copy in row_copies(2 * pair + r, r):
                copy.wait()
            attend_row(2 * pair + r, r)
            for copy in ctx_copies(2 * pair + r, r):
                copy.start()
            return c

        lax.fori_loop(0, 2, one, 0)
        for r in range(2):
            for copy in ctx_copies(2 * pair + r, r):
                copy.wait()

        def out(i, c):
            dest = lax.rem(spread(i, n) + me, n)

            @pl.when(dest != me)
            def _():
                c_send(dest, pair).start()

            return c

        lax.fori_loop(0, n, out, 0)
        return c

    lax.fori_loop(0, rows // 2, attend_pair, 0)

    for pair in range(rows // 2):
        gone = snd.at[:, pl.ds(0, n - 1), pl.ds(2 * pair, 2)]
        pltpu.make_async_copy(gone, gone, snd_sem.at[pair]).wait()
    gone = c_snd.at[pl.ds(0, n - 1)]
    pltpu.make_async_copy(gone, gone, cs_sem).wait()
    got = c_rc.at[pl.ds(0, n - 1)]
    pltpu.make_async_copy(got, got, cr_sem).wait()


def exchange(n, ctx_len, x, gamma, beta, w_rows, bias, cos_t, sin_t, rows, chunk, k_tile=512, q_blk=512, k_blk=512, low=CTX_LOW, high=CTX_HIGH):
    tokens, depth = x.shape
    _, kinds, heads, dim = w_rows.shape
    half_rows, group = split_sizes(rows, heads)
    half_tok = half_rows * chunk
    seq = n * chunk
    any_spec = pl.BlockSpec(memory_space=pl.ANY)
    vmem = pl.BlockSpec(memory_space=pltpu.VMEM)
    smem = pl.BlockSpec(memory_space=pltpu.SMEM)
    dma = pltpu.SemaphoreType.DMA
    cfg = (n, depth, k_tile, q_blk, k_blk, low, high)
    return pl.pallas_call(
        functools.partial(exchange_kernel, cfg),
        in_specs=[smem, any_spec, vmem, vmem, any_spec, vmem, vmem, vmem],
        out_specs=[any_spec] * 5,
        out_shape=[
            jax.ShapeDtypeStruct((tokens, depth), BF16),
            jax.ShapeDtypeStruct((kinds, heads, rows, chunk, dim), BF16),
            jax.ShapeDtypeStruct((kinds, rows, n, chunk, dim), BF16),
            jax.ShapeDtypeStruct((n, rows, chunk, dim), BF16),
            jax.ShapeDtypeStruct((heads, rows, chunk, dim), BF16),
        ],
        scratch_shapes=[
            pltpu.VMEM((half_tok, depth), BF16),
            pltpu.VMEM((half_tok, depth), BF16),
            pltpu.VMEM((4, k_tile, group, dim), BF16),
            pltpu.VMEM((k_tile, group * dim), BF16),
            pltpu.VMEM((k_tile, group * dim), BF16),
            pltpu.VMEM((half_tok, group * dim), F32),
            pltpu.VMEM((2, group, half_rows, chunk, dim), BF16),
            pltpu.VMEM((2, n, chunk, dim), BF16),
            pltpu.VMEM((2, n, chunk, dim), BF16),
            pltpu.VMEM((2, n, chunk, dim), BF16),
            pltpu.VMEM((2, n, chunk, dim), BF16),
            pltpu.VMEM((dim, seq), BF16),
            pltpu.VMEM((2, k_blk, q_blk), F32),
            pltpu.VMEM((2, k_blk, q_blk), BF16),
            pltpu.VMEM((1, q_blk), F32),
            pltpu.VMEM((2, 1, q_blk), F32),
            pltpu.VMEM((2, 1, q_blk), F32),
            pltpu.VMEM((2, 1, q_blk), F32),
            pltpu.VMEM((8, q_blk), F32),
            pltpu.VMEM((dim, q_blk), F32),
            dma, dma, dma((4,)), dma((2,)), dma((2,)), dma((rows // 2,)), dma((rows // 2,)), dma((3, 2)), dma((2, 2)), dma, dma,
        ],
        compiler_params=pltpu.CompilerParams(vmem_limit_bytes=VMEM_CAP, collective_id=0, has_side_effects=True),
        cost_estimate=pl.CostEstimate(flops=2 * tokens * depth * kinds * heads * dim, bytes_accessed=4 * depth * kinds * heads * dim, transcendentals=0),
        name="exchange",
    )(ctx_len, x, gamma, beta, w_rows, bias, cos_t, sin_t)


def dense_kernel(c_ref, w_ref, b_ref, a_hbm, kv_hbm, o_ref, ko_hbm, vo_hbm, lhs, acc, a_buf, kv_buf, a_sem, in_sem, out_sem):
    heads_blk, tokens, dim = c_ref.shape
    half, step = pl.program_id(0), pl.program_id(1)
    steps = pl.num_programs(1)
    rows = kv_hbm.shape[1]
    turn = half * steps + step
    wide = w_ref.shape[1]

    def a_copy(i):
        return pltpu.make_async_copy(a_hbm.at[:, pl.ds(pl.multiple_of(i * wide, wide), wide)], a_buf, a_sem)

    def in_copy(i):
        slot = lax.rem(i, 2)
        return pltpu.make_async_copy(kv_hbm.at[pl.ds(1, 2), i], kv_buf.at[slot], in_sem.at[slot])

    def out_copies(i):
        slot = lax.rem(i, 2)
        return [pltpu.make_async_copy(kv_buf.at[slot, 0], ko_hbm.at[i], out_sem.at[0, slot]),
                pltpu.make_async_copy(kv_buf.at[slot, 1], vo_hbm.at[i], out_sem.at[1, slot])]

    @pl.when(step == 0)
    def _():
        a_copy(half).start()

    @pl.when(turn == 0)
    def _():
        in_copy(0).start()

    in_copy(turn).wait()
    for copy in out_copies(turn):
        copy.start()

    @pl.when(turn > 0)
    def _():
        for copy in out_copies(turn - 1):
            copy.wait()

    @pl.when(turn + 1 < rows)
    def _():
        in_copy(turn + 1).start()

    @pl.when(turn + 1 == rows)
    def _():
        for copy in out_copies(turn):
            copy.wait()

    depth_blk = heads_blk * dim
    base = pl.multiple_of(step * depth_blk, depth_blk)

    @pl.when(half == 0)
    def _():
        for h in range(heads_blk):
            lhs[:, pl.ds(base + h * dim, dim)] = c_ref[h]

    @pl.when(step == 0)
    def _():
        acc[...] = jnp.zeros_like(acc)

    left = lhs[:, pl.ds(base, depth_blk)]
    for t in range(wide // 256):
        cols = slice(t * 256, (t + 1) * 256)
        acc[:, cols] += jnp.dot(left, w_ref[:, cols], preferred_element_type=F32)

    @pl.when(step == steps - 1)
    def _():
        a_copy(half).wait()
        o_ref[...] = (a_buf[...].astype(F32) * ALPHA + (acc[...] + b_ref[...].astype(F32))).astype(BF16)


def dense(context, w_dense, bias, normed, kv):
    heads, tokens, dim = context.shape
    depth, width = w_dense.shape
    kinds, rows, seq, _ = kv.shape
    steps = 4
    any_spec = pl.BlockSpec(memory_space=pl.ANY)
    wide = width // 2
    return pl.pallas_call(
        dense_kernel,
        grid=(2, steps),
        in_specs=[
            pl.BlockSpec((heads // steps, tokens, dim), lambda i, k: (lax.select(i == 0, k, steps - 1), 0, 0)),
            pl.BlockSpec((depth // steps, wide), lambda i, k: (k, i)),
            pl.BlockSpec((1, wide), lambda i, k: (0, i)),
            any_spec,
            any_spec,
        ],
        out_specs=[pl.BlockSpec((tokens, wide), lambda i, k: (0, i)), any_spec, any_spec],
        out_shape=[
            jax.ShapeDtypeStruct((tokens, width), BF16),
            jax.ShapeDtypeStruct((rows, seq, dim), BF16),
            jax.ShapeDtypeStruct((rows, seq, dim), BF16),
        ],
        scratch_shapes=[
            pltpu.VMEM((tokens, depth), BF16),
            pltpu.VMEM((tokens, wide), F32),
            pltpu.VMEM((tokens, wide), BF16),
            pltpu.VMEM((2, 2, seq, dim), BF16),
            pltpu.SemaphoreType.DMA,
            pltpu.SemaphoreType.DMA((2,)),
            pltpu.SemaphoreType.DMA((2, 2)),
        ],
        compiler_params=pltpu.CompilerParams(vmem_limit_bytes=VMEM_CAP),
        cost_estimate=pl.CostEstimate(flops=2 * tokens * depth * width, bytes_accessed=2 * depth * width, transcendentals=0),
        name="dense",
    )(context, w_dense, bias.reshape(1, width), normed, kv)


def solution(mesh):
    seq_spec = P('dp', 'sp', None)
    row_spec = P('dp', 'sp')
    head_spec = P('dp', None, 'sp', None)
    rep = P()
    devices = mesh.shape['sp']

    def local_block(hidden, pos_ids, block_ids, ctx_len, ln_gamma, ln_beta, w_qkv, b_qkv, w_dense, b_dense):
        rows, chunk, width = hidden.shape
        depth, heads, kinds, dim = w_qkv.shape
        seq = chunk * devices
        tokens = rows * chunk
        cos_t, sin_t = rotary_tables(pos_ids, block_ids, dim)
        w_rows = jnp.transpose(w_qkv, (0, 2, 1, 3))
        bias = jnp.transpose(b_qkv, (1, 0, 2)).reshape(kinds * heads, 1, dim).astype(F32)
        gamma = ln_gamma.astype(F32).reshape(1, width)
        beta = ln_beta.astype(F32).reshape(1, width)
        normed, _, recv, _, context = exchange(devices, ctx_len, hidden.reshape(tokens, width), gamma, beta, w_rows, bias, cos_t, sin_t, rows, chunk)
        out, keys, values = dense(context.reshape(heads, tokens, dim), w_dense, b_dense, normed, recv.reshape(kinds, rows, seq, dim))
        return out.reshape(rows, chunk, width), keys.reshape(rows, seq, 1, dim), values.reshape(rows, seq, 1, dim)

    return jax.shard_map(local_block, mesh=mesh, in_specs=(seq_spec, row_spec, row_spec, P('dp'), rep, rep, rep, rep, rep, rep), out_specs=(seq_spec, head_spec, head_spec), check_vma=False)
```

```python
import functools
import math

import jax
import jax.numpy as jnp
from jax import lax
from jax.experimental import pallas as pl
from jax.experimental.pallas import tpu as pltpu
from jax.sharding import PartitionSpec as P

ALPHA = math.sqrt(56.0)
ROPE_BASE = 10000.0
LN_EPS = 1e-5
CTX_LOW = 1024
CTX_HIGH = 3072
F32 = jnp.float32
BF16 = jnp.bfloat16
VMEM_CAP = 60000 * 1024
MESH_ID = pl.DeviceIdType.MESH


def rotary_tables(pos_ids, block_ids, dim):
    half = dim // 2
    quarter = half // 2
    inv_freq = ROPE_BASE ** (-jnp.arange(0, half, 2).astype(F32) / half)
    lane = lax.broadcasted_iota(jnp.int32, (1, dim), 1)
    ids = jnp.where(lane < half, pos_ids.reshape(-1, 1), block_ids.reshape(-1, 1))
    ang = ids.astype(F32) * jnp.concatenate([inv_freq] * 4).reshape(1, dim)
    sign = jnp.where(lax.rem(lane, half) < quarter, -1.0, 1.0)
    return jnp.cos(ang), jnp.sin(ang) * sign


def split_sizes(rows, heads):
    return rows // 2, heads // 2


def exchange_kernel(cfg, ctx_ref, x_ref, g_ref, be_ref, w_ref, bias_ref, cos_ref, sin_ref, wd_ref, bd_ref,
                    a_out, snd, rc, c_snd, c_rc, half_out,
                    xb, ab, wbuf, wb0, wb1, acc, sb, qb, kb, vb, cb, vt, s_buf, m_buf, a_buf, l_s, acc_s,
                    x_sem, a_sem, w_sem, l_sem, o_sem, snd_sem, rcv_sem, row_sem, c_sem, cs_sem, cr_sem, lhs_sem):
    n, depth, k_tile, q_blk, k_blk, low, high = cfg
    _, heads, rows, chunk, dim = snd.shape
    half_rows, group = split_sizes(rows, heads)
    half_tok = half_rows * chunk
    seq = n * chunk
    pieces = 12
    chunks = depth // k_tile
    total = pieces * chunks
    me = lax.axis_index('sp')

    barrier = pltpu.get_barrier_semaphore()

    def greet(i, c):
        pl.semaphore_signal(barrier, inc=1, device_id={'sp': lax.rem(me + i, n)}, device_id_type=MESH_ID)
        return c

    def piece_of(p):
        hf = p // 6
        kind = lax.rem(lax.rem(p, 6) // 2 + 1, 3)
        hh = lax.rem(p, 2)
        return hf, kind, hh

    def w_copy(s):
        _, kind, hh = piece_of(s // chunks)
        c = lax.rem(s, chunks)
        slot = lax.rem(s, 4)
        return pltpu.make_async_copy(
            w_ref.at[pl.ds(pl.multiple_of(c * k_tile, k_tile), k_tile), kind, pl.ds(pl.multiple_of(hh * group, group), group)],
            wbuf.at[slot], w_sem.at[slot])

    def x_copy(hf):
        return pltpu.make_async_copy(x_ref.at[pl.ds(pl.multiple_of(hf * half_tok, half_tok), half_tok)], xb, x_sem)

    def a_copy(hf):
        return pltpu.make_async_copy(ab, a_out.at[pl.ds(pl.multiple_of(hf * half_tok, half_tok), half_tok)], a_sem)

    def l_copy(p):
        hf, kind, hh = piece_of(p)
        slot = lax.rem(p, 2)
        return pltpu.make_async_copy(
            sb.at[slot],
            snd.at[kind, pl.ds(pl.multiple_of(hh * group, group), group), pl.ds(hf * half_rows, half_rows)],
            l_sem.at[slot])

    def own_copy(p):
        hf, kind, hh = piece_of(p)
        slot = lax.rem(p, 2)
        return pltpu.make_async_copy(
            sb.at[slot, lax.rem(me, group)],
            rc.at[kind, pl.ds(hf * half_rows, half_rows), me],
            o_sem.at[slot])

    def mine(p):
        return piece_of(p)[2] == me // group

    def send(kind, head, hf):
        def start(at, group_id):
            pltpu.make_async_remote_copy(
                src_ref=snd.at[kind, head, at], dst_ref=rc.at[kind, at, me],
                send_sem=snd_sem.at[group_id], recv_sem=rcv_sem.at[group_id],
                device_id={'sp': head}, device_id_type=MESH_ID).start()

        @pl.when(hf == 0)
        def _():
            start(pl.ds(0, half_rows), 0)

        @pl.when(hf == 1)
        def _():
            start(pl.ds(half_rows, half_rows - 2), 1)

    def send_row(head, row, group_id):
        pltpu.make_async_remote_copy(
            src_ref=snd.at[:, head, row], dst_ref=rc.at[:, row, me],
            send_sem=snd_sem.at[group_id], recv_sem=rcv_sem.at[group_id],
            device_id={'sp': head}, device_id_type=MESH_ID).start()

    def c_send(dest, first, count, sem):
        at = pl.ds(pl.multiple_of(first * chunk, chunk), count * chunk)
        return pltpu.make_async_remote_copy(
            src_ref=c_snd.at[dest, at], dst_ref=c_rc.at[me, at],
            send_sem=cs_sem, recv_sem=cr_sem.at[sem], device_id={'sp': dest}, device_id_type=MESH_ID)

    def layer_norm(hf):
        x_copy(hf).wait()
        sub = 16
        tile = min(64, half_tok)
        lanes = [slice(c * 128, (c + 1) * 128) for c in range(depth // 128)]

        def body(i, c):
            ats = [pl.ds(pl.multiple_of(i * tile + u * sub, sub), sub) for u in range(tile // sub)]
            means, scales = [], []
            for at in ats:
                total = sum(xb[at, cols].astype(F32) for cols in lanes)
                means.append(jnp.sum(total, axis=-1, keepdims=True) * (1.0 / depth))
            for at, mean in zip(ats, means):
                total = sum(jnp.square(xb[at, cols].astype(F32) - mean) for cols in lanes)
                scales.append(lax.rsqrt(jnp.sum(total, axis=-1, keepdims=True) * (1.0 / depth) + LN_EPS))
            for cols in lanes:
                gain = g_ref[cols].astype(F32).reshape(1, 128)
                shift = be_ref[cols].astype(F32).reshape(1, 128)
                for at, mean, scale in zip(ats, means, scales):
                    ab[at, cols] = ((xb[at, cols].astype(F32) - mean) * scale * gain + shift).astype(BF16)
            return c

        lax.fori_loop(0, half_tok // tile, body, 0)
        a_copy(hf).start()

    def relayout(s, wb):
        slot = lax.rem(s, 4)
        sub = min(64, k_tile)
        for part in range(k_tile // sub):
            lo = part * sub
            tile = jnp.swapaxes(wbuf[slot, lo:lo + sub], 0, 1)
            for head in range(group):
                wb[lo:lo + sub, head * dim:(head + 1) * dim] = tile[head]

    def multiply(c, wb):
        lhs = ab[:, pl.ds(pl.multiple_of(c * k_tile, k_tile), k_tile)]
        wide = min(256, group * dim)
        for t in range(group * dim // wide):
            cols = slice(t * wide, (t + 1) * wide)
            acc[:, cols] += jnp.dot(lhs, wb[:, cols], preferred_element_type=F32)

    def epilogue(p):
        hf, kind, hh = piece_of(p)
        slot = lax.rem(p, 2)
        toks = pl.ds(pl.multiple_of(hf * half_tok, half_tok), half_tok)
        turn = min(4, group)
        bias = bias_ref[kind, pl.ds(pl.multiple_of(hh * group, group), group), :].astype(F32)
        fill = jnp.zeros((half_tok, dim), F32)
        lane = lax.broadcasted_iota(jnp.int32, (1, dim), 1)
        first = lax.rem(lane, dim // 2) < dim // 4

        def biased(h, row):
            cols = pl.ds(pl.multiple_of(h * dim, dim), dim)
            x = (acc[:, cols] + row).astype(BF16)
            acc[:, cols] = fill
            return x

        def rows_of(t):
            return [bias[t * turn + u:t * turn + u + 1, :] for u in range(turn)]

        for t in range(group // turn):
            @pl.when(kind < 2)
            def _():
                for u, row in enumerate(rows_of(t)):
                    h = t * turn + u
                    x = biased(h, row).astype(F32)
                    pair = jnp.where(first, pltpu.roll(x, dim - dim // 4, 1), pltpu.roll(x, dim // 4, 1))
                    x = (x * cos_ref[toks, :] + pair * sin_ref[toks, :]).astype(BF16)
                    sb[slot, h] = x.reshape(half_rows, chunk, dim)

            @pl.when(kind == 2)
            def _():
                for u, row in enumerate(rows_of(t)):
                    h = t * turn + u
                    sb[slot, h] = biased(h, row).reshape(half_rows, chunk, dim)

    def spread(i, count):
        quarter = count // 4
        return lax.rem(i, 4) * quarter + lax.rem(i // 4 + lax.rem(i, 4), quarter)

    def flush(p):
        hf, kind, hh = piece_of(p)
        l_copy(p).wait()

        @pl.when(mine(p))
        def _():
            own_copy(p).wait()

        def body(i, c):
            head = hh * group + lax.rem(spread(i, group) + me, group)

            @pl.when(head != me)
            def _():
                send(kind, head, hf)

            return c

        lax.fori_loop(0, group, body, 0)

        @pl.when(p == pieces - 1)
        def _():
            for r in range(2):
                def late(i, c):
                    head = lax.rem(spread(i, heads) + me, heads)

                    @pl.when(head != me)
                    def _():
                        send_row(head, rows - 2 + r, 2 + r)

                    return c

                lax.fori_loop(0, heads, late, 0)

    x_copy(0).start()
    for s in range(3):
        w_copy(s).start()
    lax.fori_loop(1, n, greet, 0)
    acc[...] = jnp.zeros_like(acc)
    w_copy(0).wait()
    relayout(0, wb0)
    layer_norm(0)
    x_copy(1).start()
    pl.semaphore_wait(barrier, n - 1)

    def project(p, c):
        @pl.when(p == 6)
        def _():
            a_copy(0).wait()
            layer_norm(1)

        def steps(i, c):
            s = p * chunks + 2 * i
            w_copy(s + 1).wait()

            @pl.when(s + 2 < total)
            def _():
                w_copy(s + 2).wait()

            @pl.when(s + 3 < total)
            def _():
                w_copy(s + 3).start()

            @pl.when(s + 4 < total)
            def _():
                w_copy(s + 4).start()

            @pl.when((i == 1) & (p > 0))
            def _():
                flush(p - 1)

            relayout(s + 1, wb1)
            multiply(2 * i, wb0)
            relayout(s + 2, wb0)
            multiply(2 * i + 1, wb1)
            return c

        lax.fori_loop(0, chunks // 2, steps, 0)
        epilogue(p)
        l_copy(p).start()

        @pl.when(mine(p))
        def _():
            own_copy(p).start()

        return c

    lax.fori_loop(0, pieces, project, 0)
    flush(pieces - 1)
    a_copy(1).wait()

    coef = math.log2(math.e) / math.sqrt(dim)
    per = q_blk // chunk
    kn = k_blk // chunk
    ratio = q_blk // k_blk

    def row_copies(b):
        slot = lax.rem(b, 2)
        return [pltpu.make_async_copy(rc.at[kind, b], buf.at[slot], row_sem.at[kind, slot])
                for kind, buf in ((0, qb), (1, kb), (2, vb))]

    def ctx_copies(b):
        slot = lax.rem(b, 2)
        at = pl.ds(pl.multiple_of(b * chunk, chunk), chunk)
        return [pltpu.make_async_copy(cb.at[slot], c_snd.at[:, at], c_sem.at[0, slot]),
                pltpu.make_async_copy(cb.at[slot, me], c_rc.at[me, at], c_sem.at[1, slot])]

    def attend_row(b):
        slot = lax.rem(b, 2)
        ctx = ctx_ref[b]
        step_v = min(512, seq)
        for c in range(seq // step_v):
            m = step_v // chunk
            vt[:, c * step_v:(c + 1) * step_v] = vb[slot, c * m:(c + 1) * m].reshape(step_v, dim).T
        blocks = seq // q_blk

        def scores(qi, j, s_slot, masked, prev):
            k_rows = kb[slot, pl.ds(j * kn, kn)].reshape(k_blk, dim)
            q_rows = qb[slot, pl.ds(qi * per, per)].reshape(q_blk, dim)
            s = lax.dot_general(k_rows, q_rows, (((1,), (1,)), ((), ())), preferred_element_type=F32)
            if masked:
                kpos = j * k_blk + lax.broadcasted_iota(jnp.int32, s.shape, 0)
                lim = jnp.maximum(ctx, qi * q_blk + 1 + lax.broadcasted_iota(jnp.int32, (1, q_blk), 1))
                s = jnp.where(kpos < lim, s, -jnp.inf)
            s_buf[s_slot] = s
            top = jnp.max(s, axis=0, keepdims=True) * coef
            if prev is None:
                m_buf[s_slot] = top
                a_buf[s_slot] = jnp.zeros_like(top)
            else:
                m_old = m_buf[prev]
                m_new = jnp.maximum(m_old, top)
                m_buf[s_slot] = m_new
                a_buf[s_slot] = jnp.exp2(m_old - m_new)

        def values(j, s_slot):
            v_cols = vt[:, pl.ds(pl.multiple_of(j * k_blk, k_blk), k_blk)]
            scale = a_buf[s_slot]
            p = jnp.exp2(s_buf[s_slot] * coef - m_buf[s_slot])
            l_s[...] = l_s[...] * scale + jnp.sum(p.reshape(k_blk // 8, 8, q_blk), axis=0)
            acc_s[...] = acc_s[...] * scale + jnp.dot(v_cols, p.astype(BF16), preferred_element_type=F32)

        def q_loop(qi, _):
            q0 = qi * q_blk
            l_s[...] = jnp.zeros_like(l_s)
            acc_s[...] = jnp.zeros_like(acc_s)

            def pair(i, masked):
                scores(qi, 2 * i + 1, 1, masked, 0)
                values(2 * i, 0)
                scores(qi, 2 * i + 2, 0, masked, 1)
                values(2 * i + 1, 1)

            last = (jnp.maximum(high, q0 + q_blk) + 2 * k_blk - 1) // (2 * k_blk) - 1
            full = jnp.minimum((jnp.maximum(low, q0) // k_blk - 1) // 2, last)
            lax.fori_loop(0, full, lambda i, c: (pair(i, False), c)[1], 0)
            lax.fori_loop(full, last, lambda i, c: (pair(i, True), c)[1], 0)
            scores(qi, 2 * last + 1, 1, True, 0)
            values(2 * last, 0)
            scores(jnp.minimum(qi + 1, blocks - 1), 0, 0, False, None)
            values(2 * last + 1, 1)
            inv = 1.0 / jnp.sum(l_s[...], axis=0, keepdims=True)
            cb[slot, pl.ds(qi * per, per)] = (acc_s[...] * inv).T.astype(BF16).reshape(per, chunk, dim)
            return 0

        scores(0, 0, 0, False, None)
        lax.fori_loop(0, blocks, q_loop, 0)

    def arrived(at, group_id):
        got = rc.at[:, at, pl.ds(0, n - 1)]
        pltpu.make_async_copy(got, got, rcv_sem.at[group_id]).wait()

    def give(b, first, count, sem):
        for r in range(count):
            for copy in ctx_copies(b - count + 1 + r):
                copy.wait()

        def out(i, c):
            dest = lax.rem(spread(i, n) + me, n)

            @pl.when(dest != me)
            def _():
                c_send(dest, first, count, sem).start()

            return c

        lax.fori_loop(0, n, out, 0)

    starts = ((0, pl.ds(0, half_rows)), (half_rows, pl.ds(half_rows, half_rows - 2)), (rows - 2, pl.ds(rows - 2, 1)), (rows - 1, pl.ds(rows - 1, 1)))

    def attend(b, c):
        for group_id, (row, at) in enumerate(starts):
            @pl.when(b == row)
            def _():
                arrived(at, group_id)
                for copy in row_copies(b):
                    copy.start()

        @pl.when((b < half_rows - 1) | ((b >= half_rows) & (b < rows - 3)))
        def _():
            for copy in row_copies(b + 1):
                copy.start()

        for copy in row_copies(b):
            copy.wait()
        attend_row(b)
        for copy in ctx_copies(b):
            copy.start()

        @pl.when((lax.rem(b, 2) == 1) & (b < half_rows))
        def _():
            give(b, b - 1, 2, 0)

        @pl.when(b == rows - 3)
        def _():
            give(b, b - 1, 2, 1)

        @pl.when(b >= rows - 2)
        def _():
            give(b, b, 1, 1)

        return c

    lax.fori_loop(0, rows, attend, 0)

    steps = depth // k_tile
    wide = group * dim

    def wd_copy(i, buf, slot):
        return pltpu.make_async_copy(
            wd_ref.at[pl.ds(pl.multiple_of(lax.rem(i, steps) * k_tile, k_tile), k_tile), pl.ds(pl.multiple_of(i // steps * wide, wide), wide)],
            buf, w_sem.at[slot])

    def lhs_copy(h):
        return pltpu.make_async_copy(c_rc.at[h, pl.ds(0, half_tok)], ab.at[:, pl.ds(pl.multiple_of(h * dim, dim), dim)], lhs_sem)

    wd_copy(0, wb0, 0).start()
    a_back = pltpu.make_async_copy(a_out.at[pl.ds(0, half_tok)], xb, x_sem)
    a_back.start()
    got = c_rc.at[pl.ds(0, n - 1), pl.ds(0, half_tok)]
    pltpu.make_async_copy(got, got, cr_sem.at[0]).wait()
    lax.fori_loop(0, heads, lambda h, c: (lhs_copy(h).start(), c)[1], 0)
    lax.fori_loop(0, heads, lambda h, c: (lhs_copy(h).wait(), c)[1], 0)
    a_back.wait()

    def dense_half(t, c):
        def two(i, c):
            s = t * steps + 2 * i
            wd_copy(s + 1, wb1, 1).start()
            wd_copy(s, wb0, 0).wait()
            multiply(2 * i, wb0)

            @pl.when(s + 2 < 2 * steps)
            def _():
                wd_copy(s + 2, wb0, 0).start()

            wd_copy(s + 1, wb1, 1).wait()
            multiply(2 * i + 1, wb1)
            return c

        lax.fori_loop(0, steps // 2, two, 0)
        for u in range(wide // 256):
            cols = pl.ds(pl.multiple_of(t * wide + u * 256, 256), 256)
            part = slice(u * 256, (u + 1) * 256)
            shift = bd_ref[:, cols].astype(F32)
            xb[:, cols] = (xb[:, cols].astype(F32) * ALPHA + (acc[:, part] + shift)).astype(BF16)
            acc[:, part] = jnp.zeros((half_tok, 256), F32)
        return c

    lax.fori_loop(0, depth // wide, dense_half, 0)
    done = pltpu.make_async_copy(xb, half_out, x_sem)
    done.start()

    for group_id, (_, at) in enumerate(starts):
        gone = snd.at[:, pl.ds(0, n - 1), at]
        pltpu.make_async_copy(gone, gone, snd_sem.at[group_id]).wait()
    gone = c_snd.at[pl.ds(0, n - 1)]
    pltpu.make_async_copy(gone, gone, cs_sem).wait()
    got = c_rc.at[pl.ds(0, n - 1), pl.ds(half_tok, half_tok)]
    pltpu.make_async_copy(got, got, cr_sem.at[1]).wait()
    done.wait()


def exchange(n, ctx_len, x, gamma, beta, w_rows, bias, cos_t, sin_t, w_dense, b_dense, rows, chunk, k_tile=512, q_blk=512, k_blk=512, low=CTX_LOW, high=CTX_HIGH):
    tokens, depth = x.shape
    _, kinds, heads, dim = w_rows.shape
    half_rows, group = split_sizes(rows, heads)
    half_tok = half_rows * chunk
    seq = n * chunk
    any_spec = pl.BlockSpec(memory_space=pl.ANY)
    vmem = pl.BlockSpec(memory_space=pltpu.VMEM)
    smem = pl.BlockSpec(memory_space=pltpu.SMEM)
    dma = pltpu.SemaphoreType.DMA
    cfg = (n, depth, k_tile, q_blk, k_blk, low, high)
    return pl.pallas_call(
        functools.partial(exchange_kernel, cfg),
        in_specs=[smem, any_spec, vmem, vmem, any_spec, vmem, vmem, vmem, any_spec, vmem],
        out_specs=[any_spec] * 6,
        out_shape=[
            jax.ShapeDtypeStruct((tokens, depth), BF16),
            jax.ShapeDtypeStruct((kinds, heads, rows, chunk, dim), BF16),
            jax.ShapeDtypeStruct((kinds, rows, n, chunk, dim), BF16),
            jax.ShapeDtypeStruct((n, tokens, dim), BF16),
            jax.ShapeDtypeStruct((heads, tokens, dim), BF16),
            jax.ShapeDtypeStruct((half_tok, depth), BF16),
        ],
        scratch_shapes=[
            pltpu.VMEM((half_tok, depth), BF16),
            pltpu.VMEM((half_tok, depth), BF16),
            pltpu.VMEM((4, k_tile, group, dim), BF16),
            pltpu.VMEM((k_tile, group * dim), BF16),
            pltpu.VMEM((k_tile, group * dim), BF16),
            pltpu.VMEM((half_tok, group * dim), F32),
            pltpu.VMEM((2, group, half_rows, chunk, dim), BF16),
            pltpu.VMEM((2, n, chunk, dim), BF16),
            pltpu.VMEM((2, n, chunk, dim), BF16),
            pltpu.VMEM((2, n, chunk, dim), BF16),
            pltpu.VMEM((2, n, chunk, dim), BF16),
            pltpu.VMEM((dim, seq), BF16),
            pltpu.VMEM((2, k_blk, q_blk), F32),
            pltpu.VMEM((2, 1, q_blk), F32),
            pltpu.VMEM((2, 1, q_blk), F32),
            pltpu.VMEM((8, q_blk), F32),
            pltpu.VMEM((dim, q_blk), F32),
            dma, dma, dma((4,)), dma((2,)), dma((2,)), dma((4,)), dma((4,)), dma((3, 2)), dma((2, 2)), dma, dma((2,)), dma,
        ],
        compiler_params=pltpu.CompilerParams(vmem_limit_bytes=VMEM_CAP, collective_id=0, has_side_effects=True),
        cost_estimate=pl.CostEstimate(flops=2 * tokens * depth * kinds * heads * dim, bytes_accessed=4 * depth * kinds * heads * dim, transcendentals=0),
        name="exchange",
    )(ctx_len, x, gamma, beta, w_rows, bias, cos_t, sin_t, w_dense, b_dense)


def dense_kernel(c_ref, w_ref, b_ref, a_hbm, kv_hbm, half_hbm, o_hbm, ko_hbm, vo_hbm, lhs, acc, a_buf, kv_buf, h_buf, a_sem, in_sem, out_sem, o_sem):
    heads_blk, tokens, dim = c_ref.shape
    side, step = pl.program_id(0), pl.program_id(1)
    steps = pl.num_programs(1)
    turns = 2 * steps
    turn = side * steps + step
    wide = w_ref.shape[1]
    rest = pl.ds(tokens, tokens)
    share = tokens // turns

    def cols_of(i):
        return pl.ds(pl.multiple_of(i * wide, wide), wide)

    def a_copy(i):
        return pltpu.make_async_copy(a_hbm.at[rest, cols_of(i)], a_buf.at[i], a_sem.at[i])

    def o_copy(i):
        return pltpu.make_async_copy(a_buf.at[i], o_hbm.at[rest, cols_of(i)], o_sem.at[i])

    def part(i):
        return pl.ds(pl.multiple_of(i * share, share), share)

    def in_copies(i):
        slot = lax.rem(i, 2)
        return [pltpu.make_async_copy(kv_hbm.at[pl.ds(1, 2), i], kv_buf.at[slot], in_sem.at[0, slot]),
                pltpu.make_async_copy(half_hbm.at[part(i)], h_buf.at[slot], in_sem.at[1, slot])]

    def out_copies(i):
        slot = lax.rem(i, 2)
        return [pltpu.make_async_copy(kv_buf.at[slot, 0], ko_hbm.at[i], out_sem.at[0, slot]),
                pltpu.make_async_copy(kv_buf.at[slot, 1], vo_hbm.at[i], out_sem.at[1, slot]),
                pltpu.make_async_copy(h_buf.at[slot], o_hbm.at[part(i)], out_sem.at[2, slot])]

    def start(copies):
        for copy in copies:
            copy.start()

    def wait(copies):
        for copy in copies:
            copy.wait()

    @pl.when(turn == 0)
    def _():
        start(in_copies(0))
        start([a_copy(0), a_copy(1)])

    wait(in_copies(turn))
    start(out_copies(turn))

    @pl.when(turn > 0)
    def _():
        wait(out_copies(turn - 1))

    @pl.when(turn + 1 < turns)
    def _():
        start(in_copies(turn + 1))

    depth_blk = heads_blk * dim
    base = pl.multiple_of(step * depth_blk, depth_blk)

    @pl.when(side == 0)
    def _():
        for h in range(heads_blk):
            lhs[:, pl.ds(base + h * dim, dim)] = c_ref[h]

    left = lhs[:, pl.ds(base, depth_blk)]

    def product(first):
        for t in range(wide // 256):
            cols = slice(t * 256, (t + 1) * 256)
            prod = jnp.dot(left, w_ref[:, cols], preferred_element_type=F32)
            acc[:, cols] = prod if first else acc[:, cols] + prod

    @pl.when(step == 0)
    def _():
        product(True)

    @pl.when(step > 0)
    def _():
        product(False)

    @pl.when(step == steps - 1)
    def _():
        a_copy(side).wait()
        a_buf[side] = (a_buf[side].astype(F32) * ALPHA + (acc[...] + b_ref[...].astype(F32))).astype(BF16)
        o_copy(side).start()

    @pl.when(turn == turns - 1)
    def _():
        wait(out_copies(turn))
        wait([o_copy(0), o_copy(1)])


def dense(context, w_dense, bias, normed, kv, half_out):
    heads, tokens, dim = context.shape
    depth, width = w_dense.shape
    kinds, rows, seq, _ = kv.shape
    half_tok = tokens // 2
    steps = rows // 2
    any_spec = pl.BlockSpec(memory_space=pl.ANY)
    wide = width // 2
    dma = pltpu.SemaphoreType.DMA
    return pl.pallas_call(
        dense_kernel,
        grid=(2, steps),
        in_specs=[
            pl.BlockSpec((heads // steps, half_tok, dim), lambda i, k: (lax.select(i == 0, k, steps - 1), 1, 0)),
            pl.BlockSpec((depth // steps, wide), lambda i, k: (k, i)),
            pl.BlockSpec((1, wide), lambda i, k: (0, i)),
            any_spec,
            any_spec,
            any_spec,
        ],
        out_specs=[any_spec] * 3,
        out_shape=[
            jax.ShapeDtypeStruct((tokens, width), BF16),
            jax.ShapeDtypeStruct((rows, seq, dim), BF16),
            jax.ShapeDtypeStruct((rows, seq, dim), BF16),
        ],
        scratch_shapes=[
            pltpu.VMEM((half_tok, depth), BF16),
            pltpu.VMEM((half_tok, wide), F32),
            pltpu.VMEM((2, half_tok, wide), BF16),
            pltpu.VMEM((2, 2, seq, dim), BF16),
            pltpu.VMEM((2, half_tok // (2 * steps), width), BF16),
            dma((2,)), dma((2, 2)), dma((3, 2)), dma((2,)),
        ],
        compiler_params=pltpu.CompilerParams(vmem_limit_bytes=VMEM_CAP),
        cost_estimate=pl.CostEstimate(flops=tokens * depth * width, bytes_accessed=2 * depth * width, transcendentals=0),
        name="dense",
    )(context, w_dense, bias, normed, kv, half_out)


def solution(mesh):
    seq_spec = P('dp', 'sp', None)
    row_spec = P('dp', 'sp')
    head_spec = P('dp', None, 'sp', None)
    rep = P()
    devices = mesh.shape['sp']

    def local_block(hidden, pos_ids, block_ids, ctx_len, ln_gamma, ln_beta, w_qkv, b_qkv, w_dense, b_dense):
        rows, chunk, width = hidden.shape
        depth, heads, kinds, dim = w_qkv.shape
        seq = chunk * devices
        tokens = rows * chunk
        cos_t, sin_t = rotary_tables(pos_ids, block_ids, dim)
        w_rows = jnp.transpose(w_qkv, (0, 2, 1, 3))
        bias = jnp.transpose(b_qkv, (1, 0, 2))
        b_row = b_dense.reshape(1, width)
        normed, _, recv, _, context, half_out = exchange(
            devices, ctx_len, hidden.reshape(tokens, width), ln_gamma, ln_beta, w_rows, bias, cos_t, sin_t, w_dense, b_row, rows, chunk)
        out, keys, values = dense(context, w_dense, b_row, normed, recv.reshape(kinds, rows, seq, dim), half_out)
        return out.reshape(rows, chunk, width), keys.reshape(rows, seq, 1, dim), values.reshape(rows, seq, 1, dim)

    return jax.shard_map(local_block, mesh=mesh, in_specs=(seq_spec, row_spec, row_spec, P('dp'), rep, rep, rep, rep, rep, rep), out_specs=(seq_spec, head_spec, head_spec), check_vma=False)
```

```python
import functools
import math

import jax
import jax.numpy as jnp
from jax import lax
from jax.experimental import pallas as pl
from jax.experimental.pallas import tpu as pltpu
from jax.sharding import PartitionSpec as P

ALPHA = math.sqrt(56.0)
ROPE_BASE = 10000.0
LN_EPS = 1e-5
CTX_LOW = 1024
CTX_HIGH = 3072
F32 = jnp.float32
BF16 = jnp.bfloat16
VMEM_CAP = 60000 * 1024
MESH_ID = pl.DeviceIdType.MESH


def rotary_freq(dim):
    half = dim // 2
    lane = lax.rem(lax.broadcasted_iota(jnp.int32, (1, dim), 1), half // 2)
    return ROPE_BASE ** (-(2 * lane).astype(F32) / half)


def split_sizes(rows, heads):
    return rows // 2, heads // 2


def exchange_kernel(cfg, ctx_ref, x_ref, g_ref, be_ref, w_ref, bias_ref, pos_ref, blk_ref, freq_ref, wd_ref, bd_ref,
                    a_out, snd, rc, c_snd, c_rc, half_out,
                    xb, ab, wbuf, wb0, wb1, acc, sb, qb, kb, vb, cb, vt, s_buf, m_buf, a_buf, l_s, acc_s, cos_ref, sin_ref, bd_row,
                    x_sem, a_sem, w_sem, l_sem, o_sem, snd_sem, rcv_sem, row_sem, c_sem, cs_sem, cr_sem, lhs_sem):
    n, depth, k_tile, q_blk, k_blk, low, high = cfg
    _, heads, rows, chunk, dim = snd.shape
    half_rows, group = split_sizes(rows, heads)
    half_tok = half_rows * chunk
    seq = n * chunk
    pieces = 12
    chunks = depth // k_tile
    total = pieces * chunks
    me = lax.axis_index('sp')

    barrier = pltpu.get_barrier_semaphore()

    def greet(i, c):
        pl.semaphore_signal(barrier, inc=1, device_id={'sp': lax.rem(me + i, n)}, device_id_type=MESH_ID)
        return c

    def piece_of(p):
        hf = p // 6
        kind = 2 - lax.rem(p, 6) // 2
        hh = lax.rem(p, 2)
        return hf, kind, hh

    def w_copy(s):
        _, kind, hh = piece_of(s // chunks)
        c = lax.rem(s, chunks)
        slot = lax.rem(s, 4)
        return pltpu.make_async_copy(
            w_ref.at[pl.ds(pl.multiple_of(c * k_tile, k_tile), k_tile), kind, pl.ds(pl.multiple_of(hh * group, group), group)],
            wbuf.at[slot], w_sem.at[slot])

    def x_copy(hf):
        return pltpu.make_async_copy(x_ref.at[pl.ds(pl.multiple_of(hf * half_tok, half_tok), half_tok)], xb, x_sem)

    def a_copy(hf):
        return pltpu.make_async_copy(ab, a_out.at[pl.ds(pl.multiple_of(hf * half_tok, half_tok), half_tok)], a_sem)

    def l_copy(p):
        hf, kind, hh = piece_of(p)
        slot = lax.rem(p, 2)
        return pltpu.make_async_copy(
            sb.at[slot],
            snd.at[kind, pl.ds(pl.multiple_of(hh * group, group), group), pl.ds(hf * half_rows, half_rows)],
            l_sem.at[slot])

    def own_copy(p):
        hf, kind, hh = piece_of(p)
        slot = lax.rem(p, 2)
        return pltpu.make_async_copy(
            sb.at[slot, lax.rem(me, group)],
            rc.at[kind, pl.ds(hf * half_rows, half_rows), me],
            o_sem.at[slot])

    def mine(p):
        return piece_of(p)[2] == me // group

    def send(kind, head, hf):
        def start(at, group_id):
            pltpu.make_async_remote_copy(
                src_ref=snd.at[kind, head, at], dst_ref=rc.at[kind, at, me],
                send_sem=snd_sem.at[group_id], recv_sem=rcv_sem.at[group_id],
                device_id={'sp': head}, device_id_type=MESH_ID).start()

        @pl.when(hf == 0)
        def _():
            start(pl.ds(0, half_rows), 0)

        @pl.when(hf == 1)
        def _():
            start(pl.ds(half_rows, half_rows - 2), 1)

    def send_row(head, row, group_id):
        pltpu.make_async_remote_copy(
            src_ref=snd.at[:, head, row], dst_ref=rc.at[:, row, me],
            send_sem=snd_sem.at[group_id], recv_sem=rcv_sem.at[group_id],
            device_id={'sp': head}, device_id_type=MESH_ID).start()

    def c_send(dest, first, count, sem):
        at = pl.ds(pl.multiple_of(first * chunk, chunk), count * chunk)
        return pltpu.make_async_remote_copy(
            src_ref=c_snd.at[dest, at], dst_ref=c_rc.at[me, at],
            send_sem=cs_sem, recv_sem=cr_sem.at[sem], device_id={'sp': dest}, device_id_type=MESH_ID)

    def layer_norm(hf):
        x_copy(hf).wait()
        sub = 16
        tile = min(64, half_tok)
        lanes = [slice(c * 128, (c + 1) * 128) for c in range(depth // 128)]

        def body(i, c):
            ats = [pl.ds(pl.multiple_of(i * tile + u * sub, sub), sub) for u in range(tile // sub)]
            means, scales = [], []
            for at in ats:
                total = sum(xb[at, cols].astype(F32) for cols in lanes)
                means.append(jnp.sum(total, axis=-1, keepdims=True) * (1.0 / depth))
            for at, mean in zip(ats, means):
                total = sum(jnp.square(xb[at, cols].astype(F32) - mean) for cols in lanes)
                scales.append(lax.rsqrt(jnp.sum(total, axis=-1, keepdims=True) * (1.0 / depth) + LN_EPS))
            for cols in lanes:
                gain = g_ref[cols].astype(F32).reshape(1, 128)
                shift = be_ref[cols].astype(F32).reshape(1, 128)
                for at, mean, scale in zip(ats, means, scales):
                    ab[at, cols] = ((xb[at, cols].astype(F32) - mean) * scale * gain + shift).astype(BF16)
            return c

        lax.fori_loop(0, half_tok // tile, body, 0)

    def tables():
        lane = lax.broadcasted_iota(jnp.int32, (1, dim), 1)

        def body(r, c):
            at = pl.ds(pl.multiple_of(r * chunk, chunk), chunk)
            pos = jnp.broadcast_to(pos_ref[pl.ds(r, 1), :].astype(F32), (dim, chunk)).T
            blk = jnp.broadcast_to(blk_ref[pl.ds(r, 1), :].astype(F32), (dim, chunk)).T
            ang = jnp.where(lane < dim // 2, pos, blk) * freq_ref[...]
            sin = jnp.sin(ang)
            cos_ref[at, :] = jnp.cos(ang)
            sin_ref[at, :] = jnp.where(lax.rem(lane, dim // 2) < dim // 4, -sin, sin)
            return c

        lax.fori_loop(0, rows, body, 0)

    def relayout(s, wb):
        slot = lax.rem(s, 4)
        sub = min(64, k_tile)
        for part in range(k_tile // sub):
            lo = part * sub
            tile = jnp.swapaxes(wbuf[slot, lo:lo + sub], 0, 1)
            for head in range(group):
                wb[lo:lo + sub, head * dim:(head + 1) * dim] = tile[head]

    def multiply(c, wb):
        lhs = ab[:, pl.ds(pl.multiple_of(c * k_tile, k_tile), k_tile)]
        wide = min(256, group * dim)
        for t in range(group * dim // wide):
            cols = slice(t * wide, (t + 1) * wide)
            acc[:, cols] += jnp.dot(lhs, wb[:, cols], preferred_element_type=F32)

    def epilogue(p):
        hf, kind, hh = piece_of(p)
        slot = lax.rem(p, 2)
        toks = pl.ds(pl.multiple_of(hf * half_tok, half_tok), half_tok)
        turn = min(4, group)
        bias = bias_ref[kind, pl.ds(pl.multiple_of(hh * group, group), group), :].astype(F32)
        fill = jnp.zeros((half_tok, dim), F32)
        lane = lax.broadcasted_iota(jnp.int32, (1, dim), 1)
        first = lax.rem(lane, dim // 2) < dim // 4

        def biased(h, row):
            cols = pl.ds(pl.multiple_of(h * dim, dim), dim)
            x = (acc[:, cols] + row).astype(BF16)
            acc[:, cols] = fill
            return x

        def rows_of(t):
            return [bias[t * turn + u:t * turn + u + 1, :] for u in range(turn)]

        for t in range(group // turn):
            @pl.when(kind < 2)
            def _():
                for u, row in enumerate(rows_of(t)):
                    h = t * turn + u
                    x = biased(h, row).astype(F32)
                    pair = jnp.where(first, pltpu.roll(x, dim - dim // 4, 1), pltpu.roll(x, dim // 4, 1))
                    x = (x * cos_ref[toks, :] + pair * sin_ref[toks, :]).astype(BF16)
                    sb[slot, h] = x.reshape(half_rows, chunk, dim)

            @pl.when(kind == 2)
            def _():
                for u, row in enumerate(rows_of(t)):
                    h = t * turn + u
                    sb[slot, h] = biased(h, row).reshape(half_rows, chunk, dim)

    def spread(i, count):
        quarter = count // 4
        return lax.rem(i, 4) * quarter + lax.rem(i // 4 + lax.rem(i, 4), quarter)

    def landed(p):
        l_copy(p).wait()

        @pl.when(mine(p))
        def _():
            own_copy(p).wait()

    def flush(p, count):
        hf, kind, hh = piece_of(p)
        landed(p)
        base = hh * group
        if count == 2:
            landed(p - 1)
            base = 0

        def body(i, c):
            head = base + lax.rem(spread(i, count * group) + me, count * group)

            @pl.when(head != me)
            def _():
                send(kind, head, hf)

            return c

        lax.fori_loop(0, count * group, body, 0)

    def flush_rows():
        for r in range(2):
            def late(i, c):
                head = lax.rem(spread(i, heads) + me, heads)

                @pl.when(head != me)
                def _():
                    send_row(head, rows - 2 + r, 2 + r)

                return c

            lax.fori_loop(0, heads, late, 0)

    x_copy(0).start()
    for s in range(3):
        w_copy(s).start()
    lax.fori_loop(1, n, greet, 0)
    acc[...] = jnp.zeros_like(acc)
    w_copy(0).wait()
    relayout(0, wb0)
    with jax.named_scope('ln0'):
        layer_norm(0)
    with jax.named_scope('barrier_wait'):
        pl.semaphore_wait(barrier, n - 1)

    def project(p, c):
        @pl.when(p == 6)
        def _():
            with jax.named_scope('ln1'):
                a_copy(0).wait()
                layer_norm(1)
                a_copy(1).start()

        @pl.when(p == 1)
        def _():
            a_copy(0).start()
            x_copy(1).start()
            bd_row[...] = bd_ref[...].astype(F32).reshape(1, -1)
            with jax.named_scope('tables'):
                tables()

        def steps(i, c):
            s = p * chunks + 2 * i
            w_copy(s + 1).wait()

            @pl.when(s + 2 < total)
            def _():
                w_copy(s + 2).wait()

            @pl.when(s + 3 < total)
            def _():
                w_copy(s + 3).start()

            @pl.when(s + 4 < total)
            def _():
                w_copy(s + 4).start()

            @pl.when((i == 1) & (p == 2))
            def _():
                with jax.named_scope('flush'):
                    flush(p - 1, 1)

            @pl.when((i == 1) & (p > 2) & (lax.rem(p, 2) == 0))
            def _():
                with jax.named_scope('flush'):
                    flush(p - 1, 2)

            relayout(s + 1, wb1)
            multiply(2 * i, wb0)
            relayout(s + 2, wb0)
            multiply(2 * i + 1, wb1)
            return c

        lax.fori_loop(0, chunks // 2, steps, 0)
        with jax.named_scope('epi'):
            epilogue(p)
        l_copy(p).start()

        @pl.when(mine(p))
        def _():
            own_copy(p).start()

        @pl.when(p == 0)
        def _():
            with jax.named_scope('flush0'):
                flush(p, 1)

        return c

    lax.fori_loop(0, pieces, project, 0)
    with jax.named_scope('lastflush'):
        flush(pieces - 1, 2)
        flush_rows()
    a_copy(1).wait()

    coef = math.log2(math.e) / math.sqrt(dim)
    per = q_blk // chunk
    kn = k_blk // chunk
    ratio = q_blk // k_blk

    def row_copies(b):
        slot = lax.rem(b, 2)
        return [pltpu.make_async_copy(rc.at[kind, b], buf.at[slot], row_sem.at[kind, slot])
                for kind, buf in ((0, qb), (1, kb), (2, vb))]

    def ctx_copies(b):
        slot = lax.rem(b, 2)
        at = pl.ds(pl.multiple_of(b * chunk, chunk), chunk)
        return [pltpu.make_async_copy(cb.at[slot], c_snd.at[:, at], c_sem.at[0, slot]),
                pltpu.make_async_copy(cb.at[slot, me], c_rc.at[me, at], c_sem.at[1, slot])]

    def attend_row(b):
        slot = lax.rem(b, 2)
        ctx = ctx_ref[b]
        step_v = min(512, seq)
        for c in range(seq // step_v):
            m = step_v // chunk
            vt[:, c * step_v:(c + 1) * step_v] = vb[slot, c * m:(c + 1) * m].reshape(step_v, dim).T
        blocks = seq // q_blk

        def scores(qi, j, s_slot, masked, prev):
            k_rows = kb[slot, pl.ds(j * kn, kn)].reshape(k_blk, dim)
            q_rows = qb[slot, pl.ds(qi * per, per)].reshape(q_blk, dim)
            s = lax.dot_general(k_rows, q_rows, (((1,), (1,)), ((), ())), preferred_element_type=F32)
            if masked:
                kpos = j * k_blk + lax.broadcasted_iota(jnp.int32, s.shape, 0)
                lim = jnp.maximum(ctx, qi * q_blk + 1 + lax.broadcasted_iota(jnp.int32, (1, q_blk), 1))
                s = jnp.where(kpos < lim, s, -jnp.inf)
            s_buf[s_slot] = s
            top = jnp.max(s, axis=0, keepdims=True) * coef
            if prev is None:
                m_buf[s_slot] = top
                a_buf[s_slot] = jnp.zeros_like(top)
            else:
                m_old = m_buf[prev]
                m_new = jnp.maximum(m_old, top)
                m_buf[s_slot] = m_new
                a_buf[s_slot] = jnp.exp2(m_old - m_new)

        def values(j, s_slot):
            v_cols = vt[:, pl.ds(pl.multiple_of(j * k_blk, k_blk), k_blk)]
            scale = a_buf[s_slot]
            p = jnp.exp2(s_buf[s_slot] * coef - m_buf[s_slot])
            l_s[...] = l_s[...] * scale + jnp.sum(p.reshape(k_blk // 8, 8, q_blk), axis=0)
            acc_s[...] = acc_s[...] * scale + jnp.dot(v_cols, p.astype(BF16), preferred_element_type=F32)

        def q_loop(qi, _):
            q0 = qi * q_blk
            l_s[...] = jnp.zeros_like(l_s)
            acc_s[...] = jnp.zeros_like(acc_s)

            def pair(i, masked):
                scores(qi, 2 * i + 1, 1, masked, 0)
                values(2 * i, 0)
                scores(qi, 2 * i + 2, 0, masked, 1)
                values(2 * i + 1, 1)

            last = (jnp.maximum(high, q0 + q_blk) + 2 * k_blk - 1) // (2 * k_blk) - 1
            full = jnp.minimum((jnp.maximum(low, q0) // k_blk - 1) // 2, last)
            lax.fori_loop(0, full, lambda i, c: (pair(i, False), c)[1], 0)
            lax.fori_loop(full, last, lambda i, c: (pair(i, True), c)[1], 0)
            scores(qi, 2 * last + 1, 1, True, 0)
            values(2 * last, 0)
            scores(jnp.minimum(qi + 1, blocks - 1), 0, 0, False, None)
            values(2 * last + 1, 1)
            inv = 1.0 / jnp.sum(l_s[...], axis=0, keepdims=True)
            cb[slot, pl.ds(qi * per, per)] = (acc_s[...] * inv).T.astype(BF16).reshape(per, chunk, dim)
            return 0

        scores(0, 0, 0, False, None)
        lax.fori_loop(0, blocks, q_loop, 0)

    def arrived(at, group_id):
        got = rc.at[:, at, pl.ds(0, n - 1)]
        pltpu.make_async_copy(got, got, rcv_sem.at[group_id]).wait()

    def give(b, first, count, sem):
        with jax.named_scope('ctxwait'):
            for r in range(count):
                for copy in ctx_copies(b - count + 1 + r):
                    copy.wait()

        def out(i, c):
            dest = lax.rem(spread(i, n) + me, n)

            @pl.when(dest != me)
            def _():
                c_send(dest, first, count, sem).start()

            return c

        lax.fori_loop(0, n, out, 0)

    starts = ((0, pl.ds(0, half_rows)), (half_rows, pl.ds(half_rows, half_rows - 2)), (rows - 2, pl.ds(rows - 2, 1)), (rows - 1, pl.ds(rows - 1, 1)))

    def attend(b, c):
        for group_id, (row, at) in enumerate(starts):
            @pl.when(b == row)
            def _():
                with jax.named_scope(f'arr{group_id}'):
                    arrived(at, group_id)
                for copy in row_copies(b):
                    copy.start()

        @pl.when((b < half_rows - 1) | ((b >= half_rows) & (b < rows - 3)))
        def _():
            for copy in row_copies(b + 1):
                copy.start()

        with jax.named_scope('rowwait'):
            for copy in row_copies(b):
                copy.wait()
        with jax.named_scope('row'):
            attend_row(b)
        for copy in ctx_copies(b):
            copy.start()

        @pl.when((lax.rem(b, 2) == 1) & (b < half_rows))
        def _():
            give(b, b - 1, 2, 0)

        @pl.when(b == rows - 3)
        def _():
            give(b, b - 1, 2, 1)

        @pl.when(b >= rows - 2)
        def _():
            give(b, b, 1, 1)

        return c

    lax.fori_loop(0, rows, attend, 0)

    steps = depth // k_tile
    wide = group * dim

    def wd_copy(i, buf, slot):
        return pltpu.make_async_copy(
            wd_ref.at[pl.ds(pl.multiple_of(lax.rem(i, steps) * k_tile, k_tile), k_tile), pl.ds(pl.multiple_of(i // steps * wide, wide), wide)],
            buf, w_sem.at[slot])

    def lhs_copy(h):
        return pltpu.make_async_copy(c_rc.at[h, pl.ds(0, half_tok)], ab.at[:, pl.ds(pl.multiple_of(h * dim, dim), dim)], lhs_sem)

    wd_copy(0, wb0, 0).start()
    a_back = pltpu.make_async_copy(a_out.at[pl.ds(0, half_tok)], xb, x_sem)
    a_back.start()
    got = c_rc.at[pl.ds(0, n - 1), pl.ds(0, half_tok)]
    with jax.named_scope('cr0'):
        pltpu.make_async_copy(got, got, cr_sem.at[0]).wait()
    lax.fori_loop(0, heads, lambda h, c: (lhs_copy(h).start(), c)[1], 0)
    with jax.named_scope('lhswait'):
        lax.fori_loop(0, heads, lambda h, c: (lhs_copy(h).wait(), c)[1], 0)
        a_back.wait()

    def dense_half(t, c):
        def two(i, c):
            s = t * steps + 2 * i
            wd_copy(s + 1, wb1, 1).start()
            wd_copy(s, wb0, 0).wait()
            multiply(2 * i, wb0)

            @pl.when(s + 2 < 2 * steps)
            def _():
                wd_copy(s + 2, wb0, 0).start()

            wd_copy(s + 1, wb1, 1).wait()
            multiply(2 * i + 1, wb1)
            return c

        lax.fori_loop(0, steps // 2, two, 0)
        for u in range(wide // 256):
            cols = pl.ds(pl.multiple_of(t * wide + u * 256, 256), 256)
            part = slice(u * 256, (u + 1) * 256)
            shift = bd_row[:, cols]
            xb[:, cols] = (xb[:, cols].astype(F32) * ALPHA + (acc[:, part] + shift)).astype(BF16)
            acc[:, part] = jnp.zeros((half_tok, 256), F32)
        return c

    with jax.named_scope('dense'):
        lax.fori_loop(0, depth // wide, dense_half, 0)
    done = pltpu.make_async_copy(xb, half_out, x_sem)
    done.start()

    for group_id, (_, at) in enumerate(starts):
        gone = snd.at[:, pl.ds(0, n - 1), at]
        with jax.named_scope(f'drainsnd{group_id}'):
            pltpu.make_async_copy(gone, gone, snd_sem.at[group_id]).wait()
    gone = c_snd.at[pl.ds(0, n - 1)]
    with jax.named_scope('draincs'):
        pltpu.make_async_copy(gone, gone, cs_sem).wait()
    got = c_rc.at[pl.ds(0, n - 1), pl.ds(half_tok, half_tok)]
    with jax.named_scope('draincr'):
        pltpu.make_async_copy(got, got, cr_sem.at[1]).wait()
    done.wait()


def exchange(n, ctx_len, x, gamma, beta, w_rows, bias, pos_ids, block_ids, freq, w_dense, b_dense, rows, chunk, k_tile=512, q_blk=512, k_blk=512, low=CTX_LOW, high=CTX_HIGH):
    tokens, depth = x.shape
    _, kinds, heads, dim = w_rows.shape
    half_rows, group = split_sizes(rows, heads)
    half_tok = half_rows * chunk
    seq = n * chunk
    any_spec = pl.BlockSpec(memory_space=pl.ANY)
    vmem = pl.BlockSpec(memory_space=pltpu.VMEM)
    smem = pl.BlockSpec(memory_space=pltpu.SMEM)
    dma = pltpu.SemaphoreType.DMA
    cfg = (n, depth, k_tile, q_blk, k_blk, low, high)
    return pl.pallas_call(
        functools.partial(exchange_kernel, cfg),
        in_specs=[smem, any_spec, vmem, vmem, any_spec, vmem, vmem, vmem, vmem, any_spec, vmem],
        out_specs=[any_spec] * 6,
        out_shape=[
            jax.ShapeDtypeStruct((tokens, depth), BF16),
            jax.ShapeDtypeStruct((kinds, heads, rows, chunk, dim), BF16),
            jax.ShapeDtypeStruct((kinds, rows, n, chunk, dim), BF16),
            jax.ShapeDtypeStruct((n, tokens, dim), BF16),
            jax.ShapeDtypeStruct((heads, tokens, dim), BF16),
            jax.ShapeDtypeStruct((half_tok, depth), BF16),
        ],
        scratch_shapes=[
            pltpu.VMEM((half_tok, depth), BF16),
            pltpu.VMEM((half_tok, depth), BF16),
            pltpu.VMEM((4, k_tile, group, dim), BF16),
            pltpu.VMEM((k_tile, group * dim), BF16),
            pltpu.VMEM((k_tile, group * dim), BF16),
            pltpu.VMEM((half_tok, group * dim), F32),
            pltpu.VMEM((2, group, half_rows, chunk, dim), BF16),
            pltpu.VMEM((2, n, chunk, dim), BF16),
            pltpu.VMEM((2, n, chunk, dim), BF16),
            pltpu.VMEM((2, n, chunk, dim), BF16),
            pltpu.VMEM((2, n, chunk, dim), BF16),
            pltpu.VMEM((dim, seq), BF16),
            pltpu.VMEM((2, k_blk, q_blk), F32),
            pltpu.VMEM((2, 1, q_blk), F32),
            pltpu.VMEM((2, 1, q_blk), F32),
            pltpu.VMEM((8, q_blk), F32),
            pltpu.VMEM((dim, q_blk), F32),
            pltpu.VMEM((tokens, dim), F32),
            pltpu.VMEM((tokens, dim), F32),
            pltpu.VMEM((1, depth), F32),
            dma, dma, dma((4,)), dma((2,)), dma((2,)), dma((4,)), dma((4,)), dma((3, 2)), dma((2, 2)), dma, dma((2,)), dma,
        ],
        compiler_params=pltpu.CompilerParams(vmem_limit_bytes=VMEM_CAP, collective_id=0, has_side_effects=True),
        cost_estimate=pl.CostEstimate(flops=2 * tokens * depth * kinds * heads * dim, bytes_accessed=4 * depth * kinds * heads * dim, transcendentals=0),
        name="exchange",
    )(ctx_len, x, gamma, beta, w_rows, bias, pos_ids, block_ids, freq, w_dense, b_dense)


def dense_kernel(c_ref, w_ref, b_ref, a_hbm, kv_hbm, half_hbm, o_hbm, ko_hbm, vo_hbm, lhs, acc, a_buf, kv_buf, h_buf, a_sem, in_sem, out_sem, o_sem):
    heads_blk, tokens, dim = c_ref.shape
    side, step = pl.program_id(0), pl.program_id(1)
    steps = pl.num_programs(1)
    turns = 2 * steps
    turn = side * steps + step
    wide = w_ref.shape[1]
    rest = pl.ds(tokens, tokens)
    share = tokens // turns

    def cols_of(i):
        return pl.ds(pl.multiple_of(i * wide, wide), wide)

    def a_copy(i):
        return pltpu.make_async_copy(a_hbm.at[rest, cols_of(i)], a_buf.at[i], a_sem.at[i])

    def o_copy(i):
        return pltpu.make_async_copy(a_buf.at[i], o_hbm.at[rest, cols_of(i)], o_sem.at[i])

    def part(i):
        return pl.ds(pl.multiple_of(i * share, share), share)

    def in_copies(i):
        slot = lax.rem(i, 2)
        return [pltpu.make_async_copy(kv_hbm.at[pl.ds(1, 2), i], kv_buf.at[slot], in_sem.at[0, slot]),
                pltpu.make_async_copy(half_hbm.at[part(i)], h_buf.at[slot], in_sem.at[1, slot])]

    def out_copies(i):
        slot = lax.rem(i, 2)
        return [pltpu.make_async_copy(kv_buf.at[slot, 0], ko_hbm.at[i], out_sem.at[0, slot]),
                pltpu.make_async_copy(kv_buf.at[slot, 1], vo_hbm.at[i], out_sem.at[1, slot]),
                pltpu.make_async_copy(h_buf.at[slot], o_hbm.at[part(i)], out_sem.at[2, slot])]

    def start(copies):
        for copy in copies:
            copy.start()

    def wait(copies):
        for copy in copies:
            copy.wait()

    @pl.when(turn == 0)
    def _():
        start(in_copies(0))
        start([a_copy(0), a_copy(1)])

    wait(in_copies(turn))
    start(out_copies(turn))

    @pl.when(turn > 0)
    def _():
        wait(out_copies(turn - 1))

    @pl.when(turn + 1 < turns)
    def _():
        start(in_copies(turn + 1))

    depth_blk = heads_blk * dim
    base = pl.multiple_of(step * depth_blk, depth_blk)

    @pl.when(side == 0)
    def _():
        for h in range(heads_blk):
            lhs[:, pl.ds(base + h * dim, dim)] = c_ref[h]

    left = lhs[:, pl.ds(base, depth_blk)]

    def product(first):
        for t in range(wide // 256):
            cols = slice(t * 256, (t + 1) * 256)
            prod = jnp.dot(left, w_ref[:, cols], preferred_element_type=F32)
            acc[:, cols] = prod if first else acc[:, cols] + prod

    @pl.when(step == 0)
    def _():
        product(True)

    @pl.when(step > 0)
    def _():
        product(False)

    @pl.when(step == steps - 1)
    def _():
        a_copy(side).wait()
        a_buf[side] = (a_buf[side].astype(F32) * ALPHA + (acc[...] + b_ref[...].astype(F32).reshape(1, -1))).astype(BF16)
        o_copy(side).start()

    @pl.when(turn == turns - 1)
    def _():
        wait(out_copies(turn))
        wait([o_copy(0), o_copy(1)])


def dense(context, w_dense, bias, normed, kv, half_out):
    heads, tokens, dim = context.shape
    depth, width = w_dense.shape
    kinds, rows, seq, _ = kv.shape
    half_tok = tokens // 2
    steps = rows // 2
    any_spec = pl.BlockSpec(memory_space=pl.ANY)
    wide = width // 2
    dma = pltpu.SemaphoreType.DMA
    return pl.pallas_call(
        dense_kernel,
        grid=(2, steps),
        in_specs=[
            pl.BlockSpec((heads // steps, half_tok, dim), lambda i, k: (lax.select(i == 0, k, steps - 1), 1, 0)),
            pl.BlockSpec((depth // steps, wide), lambda i, k: (k, i)),
            pl.BlockSpec((wide,), lambda i, k: (i,)),
            any_spec,
            any_spec,
            any_spec,
        ],
        out_specs=[any_spec] * 3,
        out_shape=[
            jax.ShapeDtypeStruct((tokens, width), BF16),
            jax.ShapeDtypeStruct((rows, seq, dim), BF16),
            jax.ShapeDtypeStruct((rows, seq, dim), BF16),
        ],
        scratch_shapes=[
            pltpu.VMEM((half_tok, depth), BF16),
            pltpu.VMEM((half_tok, wide), F32),
            pltpu.VMEM((2, half_tok, wide), BF16),
            pltpu.VMEM((2, 2, seq, dim), BF16),
            pltpu.VMEM((2, half_tok // (2 * steps), width), BF16),
            dma((2,)), dma((2, 2)), dma((3, 2)), dma((2,)),
        ],
        compiler_params=pltpu.CompilerParams(vmem_limit_bytes=VMEM_CAP),
        cost_estimate=pl.CostEstimate(flops=tokens * depth * width, bytes_accessed=2 * depth * width, transcendentals=0),
        name="dense",
    )(context, w_dense, bias, normed, kv, half_out)


def solution(mesh):
    seq_spec = P('dp', 'sp', None)
    row_spec = P('dp', 'sp')
    head_spec = P('dp', None, 'sp', None)
    rep = P()
    devices = mesh.shape['sp']

    def local_block(hidden, pos_ids, block_ids, ctx_len, ln_gamma, ln_beta, w_qkv, b_qkv, w_dense, b_dense):
        rows, chunk, width = hidden.shape
        depth, heads, kinds, dim = w_qkv.shape
        seq = chunk * devices
        tokens = rows * chunk
        w_rows = jnp.transpose(w_qkv, (0, 2, 1, 3))
        bias = jnp.transpose(b_qkv, (1, 0, 2))
        normed, _, recv, _, context, half_out = exchange(
            devices, ctx_len, hidden.reshape(tokens, width), ln_gamma, ln_beta, w_rows, bias, pos_ids, block_ids, rotary_freq(dim), w_dense, b_dense, rows, chunk)
        out, keys, values = dense(context, w_dense, b_dense, normed, recv.reshape(kinds, rows, seq, dim), half_out)
        return out.reshape(rows, chunk, width), keys.reshape(rows, seq, 1, dim), values.reshape(rows, seq, 1, dim)

    return jax.shard_map(local_block, mesh=mesh, in_specs=(seq_spec, row_spec, row_spec, P('dp'), rep, rep, rep, rep, rep, rep), out_specs=(seq_spec, head_spec, head_spec), check_vma=False)
```

```python
import functools
import math

import jax
import jax.numpy as jnp
from jax import lax
from jax.experimental import pallas as pl
from jax.experimental.pallas import tpu as pltpu
from jax.sharding import PartitionSpec as P

ALPHA = math.sqrt(56.0)
ROPE_BASE = 10000.0
LN_EPS = 1e-5
CTX_LOW = 1024
CTX_HIGH = 3072
F32 = jnp.float32
BF16 = jnp.bfloat16
VMEM_CAP = 60000 * 1024
MESH_ID = pl.DeviceIdType.MESH


def rotary_freq(dim):
    half = dim // 2
    lane = lax.rem(lax.broadcasted_iota(jnp.int32, (1, dim), 1), half // 2)
    return ROPE_BASE ** (-(2 * lane).astype(F32) / half)


def split_sizes(rows, heads):
    return rows // 2, heads // 2


def exchange_kernel(cfg, ctx_ref, x_ref, g_ref, be_ref, w_ref, bias_ref, pos_ref, blk_ref, freq_ref, wd_ref, bd_ref,
                    a_out, snd, rc, c_snd, c_rc, half_out,
                    xb, ab, wbuf, wb0, wb1, acc, sb, qb, kb, vb, cb, vt, s_buf, m_buf, a_buf, l_s, acc_s, cos_ref, sin_ref, bd_row,
                    x_sem, a_sem, w_sem, l_sem, o_sem, snd_sem, rcv_sem, row_sem, c_sem, cs_sem, cr_sem, lhs_sem):
    n, depth, k_tile, q_blk, k_blk, low, high = cfg
    _, heads, rows, chunk, dim = snd.shape
    half_rows, group = split_sizes(rows, heads)
    half_tok = half_rows * chunk
    seq = n * chunk
    pieces = 12
    chunks = depth // k_tile
    total = pieces * chunks
    me = lax.axis_index('sp')

    barrier = pltpu.get_barrier_semaphore()

    def greet(i, c):
        pl.semaphore_signal(barrier, inc=1, device_id={'sp': lax.rem(me + i, n)}, device_id_type=MESH_ID)
        return c

    def piece_of(p):
        hf = p // 6
        kind = 2 - lax.rem(p, 6) // 2
        hh = lax.rem(p, 2)
        return hf, kind, hh

    def w_copy(s):
        _, kind, hh = piece_of(s // chunks)
        c = lax.rem(s, chunks)
        slot = lax.rem(s, 4)
        return pltpu.make_async_copy(
            w_ref.at[pl.ds(pl.multiple_of(c * k_tile, k_tile), k_tile), kind, pl.ds(pl.multiple_of(hh * group, group), group)],
            wbuf.at[slot], w_sem.at[slot])

    def x_copy(hf):
        return pltpu.make_async_copy(x_ref.at[pl.ds(pl.multiple_of(hf * half_tok, half_tok), half_tok)], xb, x_sem)

    def a_copy(hf):
        return pltpu.make_async_copy(ab, a_out.at[pl.ds(pl.multiple_of(hf * half_tok, half_tok), half_tok)], a_sem)

    def l_copy(p):
        hf, kind, hh = piece_of(p)
        slot = lax.rem(p, 2)
        return pltpu.make_async_copy(
            sb.at[slot],
            snd.at[kind, pl.ds(pl.multiple_of(hh * group, group), group), pl.ds(hf * half_rows, half_rows)],
            l_sem.at[slot])

    def own_copy(p):
        hf, kind, hh = piece_of(p)
        slot = lax.rem(p, 2)
        return pltpu.make_async_copy(
            sb.at[slot, lax.rem(me, group)],
            rc.at[kind, pl.ds(hf * half_rows, half_rows), me],
            o_sem.at[slot])

    def mine(p):
        return piece_of(p)[2] == me // group

    def send(kind, head, hf):
        def start(at, group_id):
            pltpu.make_async_remote_copy(
                src_ref=snd.at[kind, head, at], dst_ref=rc.at[kind, at, me],
                send_sem=snd_sem.at[group_id], recv_sem=rcv_sem.at[group_id],
                device_id={'sp': head}, device_id_type=MESH_ID).start()

        @pl.when(hf == 0)
        def _():
            start(pl.ds(0, half_rows), 0)

        @pl.when(hf == 1)
        def _():
            start(pl.ds(half_rows, half_rows - 2), 1)

    def send_row(head, row, group_id):
        pltpu.make_async_remote_copy(
            src_ref=snd.at[:, head, row], dst_ref=rc.at[:, row, me],
            send_sem=snd_sem.at[group_id], recv_sem=rcv_sem.at[group_id],
            device_id={'sp': head}, device_id_type=MESH_ID).start()

    def c_send(dest, first, count, sem):
        at = pl.ds(pl.multiple_of(first * chunk, chunk), count * chunk)
        return pltpu.make_async_remote_copy(
            src_ref=c_snd.at[dest, at], dst_ref=c_rc.at[me, at],
            send_sem=cs_sem, recv_sem=cr_sem.at[sem], device_id={'sp': dest}, device_id_type=MESH_ID)

    def layer_norm(hf):
        x_copy(hf).wait()
        sub = 16
        tile = min(64, half_tok)
        lanes = [slice(c * 128, (c + 1) * 128) for c in range(depth // 128)]

        def body(i, c):
            ats = [pl.ds(pl.multiple_of(i * tile + u * sub, sub), sub) for u in range(tile // sub)]
            means, scales = [], []
            for at in ats:
                total = sum(xb[at, cols].astype(F32) for cols in lanes)
                means.append(jnp.sum(total, axis=-1, keepdims=True) * (1.0 / depth))
            for at, mean in zip(ats, means):
                total = sum(jnp.square(xb[at, cols].astype(F32) - mean) for cols in lanes)
                scales.append(lax.rsqrt(jnp.sum(total, axis=-1, keepdims=True) * (1.0 / depth) + LN_EPS))
            for cols in lanes:
                gain = g_ref[cols].astype(F32).reshape(1, 128)
                shift = be_ref[cols].astype(F32).reshape(1, 128)
                for at, mean, scale in zip(ats, means, scales):
                    ab[at, cols] = ((xb[at, cols].astype(F32) - mean) * scale * gain + shift).astype(BF16)
            return c

        lax.fori_loop(0, half_tok // tile, body, 0)

    def tables():
        lane = lax.broadcasted_iota(jnp.int32, (1, dim), 1)

        def body(r, c):
            at = pl.ds(pl.multiple_of(r * chunk, chunk), chunk)
            pos = jnp.broadcast_to(pos_ref[pl.ds(r, 1), :].astype(F32), (dim, chunk)).T
            blk = jnp.broadcast_to(blk_ref[pl.ds(r, 1), :].astype(F32), (dim, chunk)).T
            ang = jnp.where(lane < dim // 2, pos, blk) * freq_ref[...]
            sin = jnp.sin(ang)
            cos_ref[at, :] = jnp.cos(ang)
            sin_ref[at, :] = jnp.where(lax.rem(lane, dim // 2) < dim // 4, -sin, sin)
            return c

        lax.fori_loop(0, rows, body, 0)

    def relayout(s, wb):
        slot = lax.rem(s, 4)
        sub = min(64, k_tile)
        for part in range(k_tile // sub):
            lo = part * sub
            tile = jnp.swapaxes(wbuf[slot, lo:lo + sub], 0, 1)
            for head in range(group):
                wb[lo:lo + sub, head * dim:(head + 1) * dim] = tile[head]

    def multiply(c, wb):
        lhs = ab[:, pl.ds(pl.multiple_of(c * k_tile, k_tile), k_tile)]
        wide = min(256, group * dim)
        for t in range(group * dim // wide):
            cols = slice(t * wide, (t + 1) * wide)
            acc[:, cols] += jnp.dot(lhs, wb[:, cols], preferred_element_type=F32)

    def epilogue(p):
        hf, kind, hh = piece_of(p)
        slot = lax.rem(p, 2)
        toks = pl.ds(pl.multiple_of(hf * half_tok, half_tok), half_tok)
        turn = min(4, group)
        bias = bias_ref[kind, pl.ds(pl.multiple_of(hh * group, group), group), :].astype(F32)
        fill = jnp.zeros((half_tok, dim), F32)
        lane = lax.broadcasted_iota(jnp.int32, (1, dim), 1)
        first = lax.rem(lane, dim // 2) < dim // 4

        def biased(h, row):
            cols = pl.ds(pl.multiple_of(h * dim, dim), dim)
            x = (acc[:, cols] + row).astype(BF16)
            acc[:, cols] = fill
            return x

        def rows_of(t):
            return [bias[t * turn + u:t * turn + u + 1, :] for u in range(turn)]

        for t in range(group // turn):
            @pl.when(kind < 2)
            def _():
                for u, row in enumerate(rows_of(t)):
                    h = t * turn + u
                    x = biased(h, row).astype(F32)
                    pair = jnp.where(first, pltpu.roll(x, dim - dim // 4, 1), pltpu.roll(x, dim // 4, 1))
                    x = (x * cos_ref[toks, :] + pair * sin_ref[toks, :]).astype(BF16)
                    sb[slot, h] = x.reshape(half_rows, chunk, dim)

            @pl.when(kind == 2)
            def _():
                for u, row in enumerate(rows_of(t)):
                    h = t * turn + u
                    sb[slot, h] = biased(h, row).reshape(half_rows, chunk, dim)

    side = math.isqrt(n // 2)

    def peer(i):
        t = i // 2
        dx = lax.rem(t, side)
        dy = lax.rem(t // side + t, side)
        y = lax.rem(me // (2 * side) + dy, side)
        x = lax.rem(me // 2 + dx, side)
        return (y * side + x) * 2 + lax.rem(me + i, 2)

    def landed(p):
        l_copy(p).wait()

        @pl.when(mine(p))
        def _():
            own_copy(p).wait()

    def flush(p, count):
        hf, kind, hh = piece_of(p)
        landed(p)
        if count == 2:
            landed(p - 1)

        def body(i, c):
            head = peer(i)
            due = head // group == hh if count == 1 else True

            @pl.when((head != me) & due)
            def _():
                send(kind, head, hf)

            return c

        lax.fori_loop(0, heads, body, 0)

    def flush_rows():
        for r in range(2):
            def late(i, c):
                head = peer(i)

                @pl.when(head != me)
                def _():
                    send_row(head, rows - 2 + r, 2 + r)

                return c

            lax.fori_loop(0, heads, late, 0)

    x_copy(0).start()
    for s in range(3):
        w_copy(s).start()
    lax.fori_loop(1, n, greet, 0)
    acc[...] = jnp.zeros_like(acc)
    w_copy(0).wait()
    relayout(0, wb0)
    with jax.named_scope('ln0'):
        layer_norm(0)
    with jax.named_scope('barrier_wait'):
        pl.semaphore_wait(barrier, n - 1)

    def project(p, c):
        @pl.when(p == 6)
        def _():
            with jax.named_scope('ln1'):
                a_copy(0).wait()
                layer_norm(1)
                a_copy(1).start()

        @pl.when(p == 1)
        def _():
            a_copy(0).start()
            x_copy(1).start()
            bd_row[...] = bd_ref[...].astype(F32).reshape(1, -1)
            with jax.named_scope('tables'):
                tables()

        def steps(i, c):
            s = p * chunks + 2 * i
            w_copy(s + 1).wait()

            @pl.when(s + 2 < total)
            def _():
                w_copy(s + 2).wait()

            @pl.when(s + 3 < total)
            def _():
                w_copy(s + 3).start()

            @pl.when(s + 4 < total)
            def _():
                w_copy(s + 4).start()

            @pl.when((i == 1) & (p == 2))
            def _():
                with jax.named_scope('flush'):
                    flush(p - 1, 1)

            @pl.when((i == 1) & (p > 2) & (lax.rem(p, 2) == 0))
            def _():
                with jax.named_scope('flush'):
                    flush(p - 1, 2)

            relayout(s + 1, wb1)
            multiply(2 * i, wb0)
            relayout(s + 2, wb0)
            multiply(2 * i + 1, wb1)
            return c

        lax.fori_loop(0, chunks // 2, steps, 0)
        with jax.named_scope('epi'):
            epilogue(p)
        l_copy(p).start()

        @pl.when(mine(p))
        def _():
            own_copy(p).start()

        @pl.when(p == 0)
        def _():
            with jax.named_scope('flush0'):
                flush(p, 1)

        return c

    lax.fori_loop(0, pieces, project, 0)
    with jax.named_scope('lastflush'):
        flush(pieces - 1, 2)
        flush_rows()
    a_copy(1).wait()

    coef = math.log2(math.e) / math.sqrt(dim)
    per = q_blk // chunk
    kn = k_blk // chunk
    ratio = q_blk // k_blk

    def row_copies(b):
        slot = lax.rem(b, 2)
        return [pltpu.make_async_copy(rc.at[kind, b], buf.at[slot], row_sem.at[kind, slot])
                for kind, buf in ((0, qb), (1, kb), (2, vb))]

    def ctx_copies(b):
        slot = lax.rem(b, 2)
        at = pl.ds(pl.multiple_of(b * chunk, chunk), chunk)
        return [pltpu.make_async_copy(cb.at[slot], c_snd.at[:, at], c_sem.at[0, slot]),
                pltpu.make_async_copy(cb.at[slot, me], c_rc.at[me, at], c_sem.at[1, slot])]

    def attend_row(b):
        slot = lax.rem(b, 2)
        ctx = ctx_ref[b]
        step_v = min(512, seq)
        for c in range(seq // step_v):
            m = step_v // chunk
            vt[:, c * step_v:(c + 1) * step_v] = vb[slot, c * m:(c + 1) * m].reshape(step_v, dim).T
        blocks = seq // q_blk

        def scores(qi, j, s_slot, masked, prev):
            k_rows = kb[slot, pl.ds(j * kn, kn)].reshape(k_blk, dim)
            q_rows = qb[slot, pl.ds(qi * per, per)].reshape(q_blk, dim)
            s = lax.dot_general(k_rows, q_rows, (((1,), (1,)), ((), ())), preferred_element_type=F32)
            if masked:
                kpos = j * k_blk + lax.broadcasted_iota(jnp.int32, s.shape, 0)
                lim = jnp.maximum(ctx, qi * q_blk + 1 + lax.broadcasted_iota(jnp.int32, (1, q_blk), 1))
                s = jnp.where(kpos < lim, s, -jnp.inf)
            s_buf[s_slot] = s
            top = jnp.max(s, axis=0, keepdims=True) * coef
            if prev is None:
                m_buf[s_slot] = top
                a_buf[s_slot] = jnp.zeros_like(top)
            else:
                m_old = m_buf[prev]
                m_new = jnp.maximum(m_old, top)
                m_buf[s_slot] = m_new
                a_buf[s_slot] = jnp.exp2(m_old - m_new)

        def values(j, s_slot):
            v_cols = vt[:, pl.ds(pl.multiple_of(j * k_blk, k_blk), k_blk)]
            scale = a_buf[s_slot]
            p = jnp.exp2(s_buf[s_slot] * coef - m_buf[s_slot])
            l_s[...] = l_s[...] * scale + jnp.sum(p.reshape(k_blk // 8, 8, q_blk), axis=0)
            acc_s[...] = acc_s[...] * scale + jnp.dot(v_cols, p.astype(BF16), preferred_element_type=F32)

        def q_loop(qi, _):
            q0 = qi * q_blk
            l_s[...] = jnp.zeros_like(l_s)
            acc_s[...] = jnp.zeros_like(acc_s)

            def pair(i, masked):
                scores(qi, 2 * i + 1, 1, masked, 0)
                values(2 * i, 0)
                scores(qi, 2 * i + 2, 0, masked, 1)
                values(2 * i + 1, 1)

            last = (jnp.maximum(high, q0 + q_blk) + 2 * k_blk - 1) // (2 * k_blk) - 1
            full = jnp.minimum((jnp.maximum(low, q0) // k_blk - 1) // 2, last)
            lax.fori_loop(0, full, lambda i, c: (pair(i, False), c)[1], 0)
            lax.fori_loop(full, last, lambda i, c: (pair(i, True), c)[1], 0)
            scores(qi, 2 * last + 1, 1, True, 0)
            values(2 * last, 0)
            scores(jnp.minimum(qi + 1, blocks - 1), 0, 0, False, None)
            values(2 * last + 1, 1)
            inv = 1.0 / jnp.sum(l_s[...], axis=0, keepdims=True)
            cb[slot, pl.ds(qi * per, per)] = (acc_s[...] * inv).T.astype(BF16).reshape(per, chunk, dim)
            return 0

        scores(0, 0, 0, False, None)
        lax.fori_loop(0, blocks, q_loop, 0)

    def arrived(at, group_id):
        got = rc.at[:, at, pl.ds(0, n - 1)]
        pltpu.make_async_copy(got, got, rcv_sem.at[group_id]).wait()

    def give(b, first, count, sem):
        with jax.named_scope('ctxwait'):
            for r in range(count):
                for copy in ctx_copies(b - count + 1 + r):
                    copy.wait()

        def out(i, c):
            dest = peer(i)

            @pl.when(dest != me)
            def _():
                c_send(dest, first, count, sem).start()

            return c

        lax.fori_loop(0, n, out, 0)

    starts = ((0, pl.ds(0, half_rows)), (half_rows, pl.ds(half_rows, half_rows - 2)), (rows - 2, pl.ds(rows - 2, 1)), (rows - 1, pl.ds(rows - 1, 1)))

    def attend(b, c):
        for group_id, (row, at) in enumerate(starts):
            @pl.when(b == row)
            def _():
                with jax.named_scope(f'arr{group_id}'):
                    arrived(at, group_id)
                for copy in row_copies(b):
                    copy.start()

        @pl.when((b < half_rows - 1) | ((b >= half_rows) & (b < rows - 3)))
        def _():
            for copy in row_copies(b + 1):
                copy.start()

        with jax.named_scope('rowwait'):
            for copy in row_copies(b):
                copy.wait()
        with jax.named_scope('row'):
            attend_row(b)
        for copy in ctx_copies(b):
            copy.start()

        @pl.when((lax.rem(b, 2) == 1) & (b < half_rows))
        def _():
            give(b, b - 1, 2, 0)

        @pl.when(b == rows - 3)
        def _():
            give(b, b - 1, 2, 1)

        @pl.when(b >= rows - 2)
        def _():
            give(b, b, 1, 1)

        return c

    lax.fori_loop(0, rows, attend, 0)

    steps = depth // k_tile
    wide = group * dim

    def wd_copy(i, buf, slot):
        return pltpu.make_async_copy(
            wd_ref.at[pl.ds(pl.multiple_of(lax.rem(i, steps) * k_tile, k_tile), k_tile), pl.ds(pl.multiple_of(i // steps * wide, wide), wide)],
            buf, w_sem.at[slot])

    def lhs_copy(h):
        return pltpu.make_async_copy(c_rc.at[h, pl.ds(0, half_tok)], ab.at[:, pl.ds(pl.multiple_of(h * dim, dim), dim)], lhs_sem)

    wd_copy(0, wb0, 0).start()
    a_back = pltpu.make_async_copy(a_out.at[pl.ds(0, half_tok)], xb, x_sem)
    a_back.start()
    got = c_rc.at[pl.ds(0, n - 1), pl.ds(0, half_tok)]
    with jax.named_scope('cr0'):
        pltpu.make_async_copy(got, got, cr_sem.at[0]).wait()
    lax.fori_loop(0, heads, lambda h, c: (lhs_copy(h).start(), c)[1], 0)
    with jax.named_scope('lhswait'):
        lax.fori_loop(0, heads, lambda h, c: (lhs_copy(h).wait(), c)[1], 0)
        a_back.wait()

    def dense_half(t, c):
        def two(i, c):
            s = t * steps + 2 * i
            wd_copy(s + 1, wb1, 1).start()
            wd_copy(s, wb0, 0).wait()
            multiply(2 * i, wb0)

            @pl.when(s + 2 < 2 * steps)
            def _():
                wd_copy(s + 2, wb0, 0).start()

            wd_copy(s + 1, wb1, 1).wait()
            multiply(2 * i + 1, wb1)
            return c

        lax.fori_loop(0, steps // 2, two, 0)
        for u in range(wide // 256):
            cols = pl.ds(pl.multiple_of(t * wide + u * 256, 256), 256)
            part = slice(u * 256, (u + 1) * 256)
            shift = bd_row[:, cols]
            xb[:, cols] = (xb[:, cols].astype(F32) * ALPHA + (acc[:, part] + shift)).astype(BF16)
            acc[:, part] = jnp.zeros((half_tok, 256), F32)
        return c

    with jax.named_scope('dense'):
        lax.fori_loop(0, depth // wide, dense_half, 0)
    done = pltpu.make_async_copy(xb, half_out, x_sem)
    done.start()

    for group_id, (_, at) in enumerate(starts):
        gone = snd.at[:, pl.ds(0, n - 1), at]
        with jax.named_scope(f'drainsnd{group_id}'):
            pltpu.make_async_copy(gone, gone, snd_sem.at[group_id]).wait()
    gone = c_snd.at[pl.ds(0, n - 1)]
    with jax.named_scope('draincs'):
        pltpu.make_async_copy(gone, gone, cs_sem).wait()
    got = c_rc.at[pl.ds(0, n - 1), pl.ds(half_tok, half_tok)]
    with jax.named_scope('draincr'):
        pltpu.make_async_copy(got, got, cr_sem.at[1]).wait()
    done.wait()


def exchange(n, ctx_len, x, gamma, beta, w_rows, bias, pos_ids, block_ids, freq, w_dense, b_dense, rows, chunk, k_tile=512, q_blk=512, k_blk=512, low=CTX_LOW, high=CTX_HIGH):
    tokens, depth = x.shape
    _, kinds, heads, dim = w_rows.shape
    half_rows, group = split_sizes(rows, heads)
    half_tok = half_rows * chunk
    seq = n * chunk
    any_spec = pl.BlockSpec(memory_space=pl.ANY)
    vmem = pl.BlockSpec(memory_space=pltpu.VMEM)
    smem = pl.BlockSpec(memory_space=pltpu.SMEM)
    dma = pltpu.SemaphoreType.DMA
    cfg = (n, depth, k_tile, q_blk, k_blk, low, high)
    return pl.pallas_call(
        functools.partial(exchange_kernel, cfg),
        in_specs=[smem, any_spec, vmem, vmem, any_spec, vmem, vmem, vmem, vmem, any_spec, vmem],
        out_specs=[any_spec] * 6,
        out_shape=[
            jax.ShapeDtypeStruct((tokens, depth), BF16),
            jax.ShapeDtypeStruct((kinds, heads, rows, chunk, dim), BF16),
            jax.ShapeDtypeStruct((kinds, rows, n, chunk, dim), BF16),
            jax.ShapeDtypeStruct((n, tokens, dim), BF16),
            jax.ShapeDtypeStruct((heads, tokens, dim), BF16),
            jax.ShapeDtypeStruct((half_tok, depth), BF16),
        ],
        scratch_shapes=[
            pltpu.VMEM((half_tok, depth), BF16),
            pltpu.VMEM((half_tok, depth), BF16),
            pltpu.VMEM((4, k_tile, group, dim), BF16),
            pltpu.VMEM((k_tile, group * dim), BF16),
            pltpu.VMEM((k_tile, group * dim), BF16),
            pltpu.VMEM((half_tok, group * dim), F32),
            pltpu.VMEM((2, group, half_rows, chunk, dim), BF16),
            pltpu.VMEM((2, n, chunk, dim), BF16),
            pltpu.VMEM((2, n, chunk, dim), BF16),
            pltpu.VMEM((2, n, chunk, dim), BF16),
            pltpu.VMEM((2, n, chunk, dim), BF16),
            pltpu.VMEM((dim, seq), BF16),
            pltpu.VMEM((2, k_blk, q_blk), F32),
            pltpu.VMEM((2, 1, q_blk), F32),
            pltpu.VMEM((2, 1, q_blk), F32),
            pltpu.VMEM((8, q_blk), F32),
            pltpu.VMEM((dim, q_blk), F32),
            pltpu.VMEM((tokens, dim), F32),
            pltpu.VMEM((tokens, dim), F32),
            pltpu.VMEM((1, depth), F32),
            dma, dma, dma((4,)), dma((2,)), dma((2,)), dma((4,)), dma((4,)), dma((3, 2)), dma((2, 2)), dma, dma((2,)), dma,
        ],
        compiler_params=pltpu.CompilerParams(vmem_limit_bytes=VMEM_CAP, collective_id=0, has_side_effects=True),
        cost_estimate=pl.CostEstimate(flops=2 * tokens * depth * kinds * heads * dim, bytes_accessed=4 * depth * kinds * heads * dim, transcendentals=0),
        name="exchange",
    )(ctx_len, x, gamma, beta, w_rows, bias, pos_ids, block_ids, freq, w_dense, b_dense)


def dense_kernel(c_ref, w_ref, b_ref, a_hbm, kv_hbm, half_hbm, o_hbm, ko_hbm, vo_hbm, lhs, acc, a_buf, kv_buf, h_buf, a_sem, in_sem, out_sem, o_sem):
    heads_blk, tokens, dim = c_ref.shape
    side, step = pl.program_id(0), pl.program_id(1)
    steps = pl.num_programs(1)
    turns = 2 * steps
    turn = side * steps + step
    wide = w_ref.shape[1]
    rest = pl.ds(tokens, tokens)
    share = tokens // turns

    def cols_of(i):
        return pl.ds(pl.multiple_of(i * wide, wide), wide)

    def a_copy(i):
        return pltpu.make_async_copy(a_hbm.at[rest, cols_of(i)], a_buf.at[i], a_sem.at[i])

    def o_copy(i):
        return pltpu.make_async_copy(a_buf.at[i], o_hbm.at[rest, cols_of(i)], o_sem.at[i])

    def part(i):
        return pl.ds(pl.multiple_of(i * share, share), share)

    def in_copies(i):
        slot = lax.rem(i, 2)
        return [pltpu.make_async_copy(kv_hbm.at[pl.ds(1, 2), i], kv_buf.at[slot], in_sem.at[0, slot]),
                pltpu.make_async_copy(half_hbm.at[part(i)], h_buf.at[slot], in_sem.at[1, slot])]

    def out_copies(i):
        slot = lax.rem(i, 2)
        return [pltpu.make_async_copy(kv_buf.at[slot, 0], ko_hbm.at[i], out_sem.at[0, slot]),
                pltpu.make_async_copy(kv_buf.at[slot, 1], vo_hbm.at[i], out_sem.at[1, slot]),
                pltpu.make_async_copy(h_buf.at[slot], o_hbm.at[part(i)], out_sem.at[2, slot])]

    def start(copies):
        for copy in copies:
            copy.start()

    def wait(copies):
        for copy in copies:
            copy.wait()

    @pl.when(turn == 0)
    def _():
        start(in_copies(0))
        start([a_copy(0), a_copy(1)])

    wait(in_copies(turn))
    start(out_copies(turn))

    @pl.when(turn > 0)
    def _():
        wait(out_copies(turn - 1))

    @pl.when(turn + 1 < turns)
    def _():
        start(in_copies(turn + 1))

    depth_blk = heads_blk * dim
    base = pl.multiple_of(step * depth_blk, depth_blk)

    @pl.when(side == 0)
    def _():
        for h in range(heads_blk):
            lhs[:, pl.ds(base + h * dim, dim)] = c_ref[h]

    left = lhs[:, pl.ds(base, depth_blk)]

    def product(first):
        for t in range(wide // 256):
            cols = slice(t * 256, (t + 1) * 256)
            prod = jnp.dot(left, w_ref[:, cols], preferred_element_type=F32)
            acc[:, cols] = prod if first else acc[:, cols] + prod

    @pl.when(step == 0)
    def _():
        product(True)

    @pl.when(step > 0)
    def _():
        product(False)

    @pl.when(step == steps - 1)
    def _():
        a_copy(side).wait()
        a_buf[side] = (a_buf[side].astype(F32) * ALPHA + (acc[...] + b_ref[...].astype(F32).reshape(1, -1))).astype(BF16)
        o_copy(side).start()

    @pl.when(turn == turns - 1)
    def _():
        wait(out_copies(turn))
        wait([o_copy(0), o_copy(1)])


def dense(context, w_dense, bias, normed, kv, half_out):
    heads, tokens, dim = context.shape
    depth, width = w_dense.shape
    kinds, rows, seq, _ = kv.shape
    half_tok = tokens // 2
    steps = rows // 2
    any_spec = pl.BlockSpec(memory_space=pl.ANY)
    wide = width // 2
    dma = pltpu.SemaphoreType.DMA
    return pl.pallas_call(
        dense_kernel,
        grid=(2, steps),
        in_specs=[
            pl.BlockSpec((heads // steps, half_tok, dim), lambda i, k: (lax.select(i == 0, k, steps - 1), 1, 0)),
            pl.BlockSpec((depth // steps, wide), lambda i, k: (k, i)),
            pl.BlockSpec((wide,), lambda i, k: (i,)),
            any_spec,
            any_spec,
            any_spec,
        ],
        out_specs=[any_spec] * 3,
        out_shape=[
            jax.ShapeDtypeStruct((tokens, width), BF16),
            jax.ShapeDtypeStruct((rows, seq, dim), BF16),
            jax.ShapeDtypeStruct((rows, seq, dim), BF16),
        ],
        scratch_shapes=[
            pltpu.VMEM((half_tok, depth), BF16),
            pltpu.VMEM((half_tok, wide), F32),
            pltpu.VMEM((2, half_tok, wide), BF16),
            pltpu.VMEM((2, 2, seq, dim), BF16),
            pltpu.VMEM((2, half_tok // (2 * steps), width), BF16),
            dma((2,)), dma((2, 2)), dma((3, 2)), dma((2,)),
        ],
        compiler_params=pltpu.CompilerParams(vmem_limit_bytes=VMEM_CAP),
        cost_estimate=pl.CostEstimate(flops=tokens * depth * width, bytes_accessed=2 * depth * width, transcendentals=0),
        name="dense",
    )(context, w_dense, bias, normed, kv, half_out)


def solution(mesh):
    seq_spec = P('dp', 'sp', None)
    row_spec = P('dp', 'sp')
    head_spec = P('dp', None, 'sp', None)
    rep = P()
    devices = mesh.shape['sp']

    def local_block(hidden, pos_ids, block_ids, ctx_len, ln_gamma, ln_beta, w_qkv, b_qkv, w_dense, b_dense):
        rows, chunk, width = hidden.shape
        depth, heads, kinds, dim = w_qkv.shape
        seq = chunk * devices
        tokens = rows * chunk
        w_rows = jnp.transpose(w_qkv, (0, 2, 1, 3))
        bias = jnp.transpose(b_qkv, (1, 0, 2))
        normed, _, recv, _, context, half_out = exchange(
            devices, ctx_len, hidden.reshape(tokens, width), ln_gamma, ln_beta, w_rows, bias, pos_ids, block_ids, rotary_freq(dim), w_dense, b_dense, rows, chunk)
        out, keys, values = dense(context, w_dense, b_dense, normed, recv.reshape(kinds, rows, seq, dim), half_out)
        return out.reshape(rows, chunk, width), keys.reshape(rows, seq, 1, dim), values.reshape(rows, seq, 1, dim)

    return jax.shard_map(local_block, mesh=mesh, in_specs=(seq_spec, row_spec, row_spec, P('dp'), rep, rep, rep, rep, rep, rep), out_specs=(seq_spec, head_spec, head_spec), check_vma=False)
```

```python
import functools
import math

import jax
import jax.numpy as jnp
from jax import lax
from jax.experimental import pallas as pl
from jax.experimental.pallas import tpu as pltpu
from jax.sharding import PartitionSpec as P

ALPHA = math.sqrt(56.0)
ROPE_BASE = 10000.0
LN_EPS = 1e-5
CTX_LOW = 1024
CTX_HIGH = 3072
F32 = jnp.float32
BF16 = jnp.bfloat16
VMEM_CAP = 60000 * 1024
MESH_ID = pl.DeviceIdType.MESH


SHIFT_PAIRS = (((1, 0), (3, 2)), ((1, 1), (3, 3)), ((3, 0), (1, 2)), ((0, 1), (2, 3)),
               ((1, 3), (3, 1)), ((0, 3), (2, 1)), ((2, 0), (0, 2)), ((2, 2), (0, 0)))


def shift_codes(side):
    if side == 4:
        pairs = SHIFT_PAIRS
    else:
        shifts = [(i % side, i // side) for i in range(side * side)]
        pairs = tuple(zip(shifts[0::2], shifts[1::2]))
    return len(pairs), [sum(pair[k // 2][k % 2] * side ** u for u, pair in enumerate(pairs)) for k in range(4)]


def rotary_freq(dim):
    half = dim // 2
    lane = lax.rem(lax.broadcasted_iota(jnp.int32, (1, dim), 1), half // 2)
    return ROPE_BASE ** (-(2 * lane).astype(F32) / half)


def split_sizes(rows, heads):
    return rows // 2, heads // 2


def exchange_kernel(cfg, ctx_ref, x_ref, g_ref, be_ref, w_ref, bias_ref, pos_ref, blk_ref, freq_ref, wd_ref, bd_ref,
                    a_out, snd, rc, c_snd, c_rc, half_out,
                    xb, ab, wbuf, wb0, wb1, acc, sb, qb, kb, vb, cb, vt, s_buf, m_buf, a_buf, l_s, acc_s, cos_ref, sin_ref, bd_row,
                    x_sem, a_sem, w_sem, l_sem, o_sem, snd_sem, rcv_sem, row_sem, c_sem, cs_sem, cr_sem, lhs_sem):
    n, depth, k_tile, q_blk, k_blk, low, high = cfg
    _, heads, rows, chunk, dim = snd.shape
    half_rows, group = split_sizes(rows, heads)
    half_tok = half_rows * chunk
    seq = n * chunk
    pieces = 12
    chunks = depth // k_tile
    total = pieces * chunks
    me = lax.axis_index('sp')

    barrier = pltpu.get_barrier_semaphore()

    def greet(i, c):
        pl.semaphore_signal(barrier, inc=1, device_id={'sp': lax.rem(me + i, n)}, device_id_type=MESH_ID)
        return c

    def piece_of(p):
        hf = p // 6
        kind = 2 - lax.rem(p, 6) // 2
        hh = lax.rem(p, 2)
        return hf, kind, hh

    def w_copy(s):
        _, kind, hh = piece_of(s // chunks)
        c = lax.rem(s, chunks)
        slot = lax.rem(s, 4)
        return pltpu.make_async_copy(
            w_ref.at[pl.ds(pl.multiple_of(c * k_tile, k_tile), k_tile), kind, pl.ds(pl.multiple_of(hh * group, group), group)],
            wbuf.at[slot], w_sem.at[slot])

    def x_copy(hf):
        return pltpu.make_async_copy(x_ref.at[pl.ds(pl.multiple_of(hf * half_tok, half_tok), half_tok)], xb, x_sem)

    def a_copy(hf):
        return pltpu.make_async_copy(ab, a_out.at[pl.ds(pl.multiple_of(hf * half_tok, half_tok), half_tok)], a_sem)

    def l_copy(p):
        hf, kind, hh = piece_of(p)
        slot = lax.rem(p, 2)
        return pltpu.make_async_copy(
            sb.at[slot],
            snd.at[kind, pl.ds(pl.multiple_of(hh * group, group), group), pl.ds(hf * half_rows, half_rows)],
            l_sem.at[slot])

    def own_copy(p):
        hf, kind, hh = piece_of(p)
        slot = lax.rem(p, 2)
        return pltpu.make_async_copy(
            sb.at[slot, lax.rem(me, group)],
            rc.at[kind, pl.ds(hf * half_rows, half_rows), me],
            o_sem.at[slot])

    def mine(p):
        return piece_of(p)[2] == me // group

    def send(kind, head, hf):
        def start(at, group_id):
            pltpu.make_async_remote_copy(
                src_ref=snd.at[kind, head, at], dst_ref=rc.at[kind, at, me],
                send_sem=snd_sem.at[group_id], recv_sem=rcv_sem.at[group_id],
                device_id={'sp': head}, device_id_type=MESH_ID).start()

        @pl.when(hf == 0)
        def _():
            start(pl.ds(0, half_rows), 0)

        @pl.when(hf == 1)
        def _():
            start(pl.ds(half_rows, half_rows - 2), 1)

    def send_row(head, row, group_id):
        pltpu.make_async_remote_copy(
            src_ref=snd.at[:, head, row], dst_ref=rc.at[:, row, me],
            send_sem=snd_sem.at[group_id], recv_sem=rcv_sem.at[group_id],
            device_id={'sp': head}, device_id_type=MESH_ID).start()

    def c_send(dest, first, count, sem):
        at = pl.ds(pl.multiple_of(first * chunk, chunk), count * chunk)
        return pltpu.make_async_remote_copy(
            src_ref=c_snd.at[dest, at], dst_ref=c_rc.at[me, at],
            send_sem=cs_sem, recv_sem=cr_sem.at[sem], device_id={'sp': dest}, device_id_type=MESH_ID)

    def layer_norm(hf):
        x_copy(hf).wait()
        sub = 16
        tile = min(64, half_tok)
        lanes = [slice(c * 128, (c + 1) * 128) for c in range(depth // 128)]

        def body(i, c):
            ats = [pl.ds(pl.multiple_of(i * tile + u * sub, sub), sub) for u in range(tile // sub)]
            means, scales = [], []
            for at in ats:
                total = sum(xb[at, cols].astype(F32) for cols in lanes)
                means.append(jnp.sum(total, axis=-1, keepdims=True) * (1.0 / depth))
            for at, mean in zip(ats, means):
                total = sum(jnp.square(xb[at, cols].astype(F32) - mean) for cols in lanes)
                scales.append(lax.rsqrt(jnp.sum(total, axis=-1, keepdims=True) * (1.0 / depth) + LN_EPS))
            for cols in lanes:
                gain = g_ref[cols].astype(F32).reshape(1, 128)
                shift = be_ref[cols].astype(F32).reshape(1, 128)
                for at, mean, scale in zip(ats, means, scales):
                    ab[at, cols] = ((xb[at, cols].astype(F32) - mean) * scale * gain + shift).astype(BF16)
            return c

        lax.fori_loop(0, half_tok // tile, body, 0)

    def tables():
        lane = lax.broadcasted_iota(jnp.int32, (1, dim), 1)

        def body(r, c):
            at = pl.ds(pl.multiple_of(r * chunk, chunk), chunk)
            pos = jnp.broadcast_to(pos_ref[pl.ds(r, 1), :].astype(F32), (dim, chunk)).T
            blk = jnp.broadcast_to(blk_ref[pl.ds(r, 1), :].astype(F32), (dim, chunk)).T
            ang = jnp.where(lane < dim // 2, pos, blk) * freq_ref[...]
            sin = jnp.sin(ang)
            cos_ref[at, :] = jnp.cos(ang)
            sin_ref[at, :] = jnp.where(lax.rem(lane, dim // 2) < dim // 4, -sin, sin)
            return c

        lax.fori_loop(0, rows, body, 0)

    def relayout(s, wb):
        slot = lax.rem(s, 4)
        sub = min(64, k_tile)
        for part in range(k_tile // sub):
            lo = part * sub
            tile = jnp.swapaxes(wbuf[slot, lo:lo + sub], 0, 1)
            for head in range(group):
                wb[lo:lo + sub, head * dim:(head + 1) * dim] = tile[head]

    def multiply(c, wb):
        lhs = ab[:, pl.ds(pl.multiple_of(c * k_tile, k_tile), k_tile)]
        wide = min(256, group * dim)
        for t in range(group * dim // wide):
            cols = slice(t * wide, (t + 1) * wide)
            acc[:, cols] += jnp.dot(lhs, wb[:, cols], preferred_element_type=F32)

    def epilogue(p):
        hf, kind, hh = piece_of(p)
        slot = lax.rem(p, 2)
        toks = pl.ds(pl.multiple_of(hf * half_tok, half_tok), half_tok)
        turn = min(4, group)
        bias = bias_ref[kind, pl.ds(pl.multiple_of(hh * group, group), group), :].astype(F32)
        fill = jnp.zeros((half_tok, dim), F32)
        lane = lax.broadcasted_iota(jnp.int32, (1, dim), 1)
        first = lax.rem(lane, dim // 2) < dim // 4

        def biased(h, row):
            cols = pl.ds(pl.multiple_of(h * dim, dim), dim)
            x = (acc[:, cols] + row).astype(BF16)
            acc[:, cols] = fill
            return x

        def rows_of(t):
            return [bias[t * turn + u:t * turn + u + 1, :] for u in range(turn)]

        for t in range(group // turn):
            @pl.when(kind < 2)
            def _():
                for u, row in enumerate(rows_of(t)):
                    h = t * turn + u
                    x = biased(h, row).astype(F32)
                    pair = jnp.where(first, pltpu.roll(x, dim - dim // 4, 1), pltpu.roll(x, dim // 4, 1))
                    x = (x * cos_ref[toks, :] + pair * sin_ref[toks, :]).astype(BF16)
                    sb[slot, h] = x.reshape(half_rows, chunk, dim)

            @pl.when(kind == 2)
            def _():
                for u, row in enumerate(rows_of(t)):
                    h = t * turn + u
                    sb[slot, h] = biased(h, row).reshape(half_rows, chunk, dim)

    side = math.isqrt(n // 2)
    pair_count, codes = shift_codes(side)

    def for_peers(act):
        core = lax.rem(me, 2)

        def one(u, rest):
            digit = [lax.rem(code, side) for code in rest]
            for r in range(4):
                second = lax.rem(r // 2 + core, 2)
                dx = digit[0] + second * (digit[2] - digit[0])
                dy = digit[1] + second * (digit[3] - digit[1])
                y = lax.rem(me // (2 * side) + dy, side)
                x = lax.rem(me // 2 + dx, side)
                peer = (y * side + x) * 2 + lax.rem(me + r, 2)

                @pl.when(peer != me)
                def _():
                    act(peer)

            return tuple(code // side for code in rest)

        lax.fori_loop(0, pair_count, one, tuple(jnp.int32(code) for code in codes))

    def landed(p):
        l_copy(p).wait()

        @pl.when(mine(p))
        def _():
            own_copy(p).wait()

    def flush(p, count):
        hf, kind, hh = piece_of(p)
        landed(p)
        if count == 2:
            landed(p - 1)

        def act(head):
            if count == 2:
                send(kind, head, hf)
            else:
                @pl.when(head // group == hh)
                def _():
                    send(kind, head, hf)

        for_peers(act)

    def flush_rows():
        for r in range(2):
            for_peers(lambda head: send_row(head, rows - 2 + r, 2 + r))

    x_copy(0).start()
    for s in range(3):
        w_copy(s).start()
    lax.fori_loop(1, n, greet, 0)
    acc[...] = jnp.zeros_like(acc)
    w_copy(0).wait()
    relayout(0, wb0)
    with jax.named_scope('ln0'):
        layer_norm(0)
    with jax.named_scope('barrier_wait'):
        pl.semaphore_wait(barrier, n - 1)

    def project(p, c):
        @pl.when(p == 6)
        def _():
            with jax.named_scope('ln1'):
                a_copy(0).wait()
                layer_norm(1)
                a_copy(1).start()

        @pl.when(p == 1)
        def _():
            a_copy(0).start()
            x_copy(1).start()
            bd_row[...] = bd_ref[...].astype(F32).reshape(1, -1)
            with jax.named_scope('tables'):
                tables()

        def steps(i, c):
            s = p * chunks + 2 * i
            w_copy(s + 1).wait()

            @pl.when(s + 2 < total)
            def _():
                w_copy(s + 2).wait()

            @pl.when(s + 3 < total)
            def _():
                w_copy(s + 3).start()

            @pl.when(s + 4 < total)
            def _():
                w_copy(s + 4).start()

            @pl.when((i == 1) & (p == 2))
            def _():
                with jax.named_scope('flush'):
                    flush(p - 1, 1)

            @pl.when((i == 1) & (p > 2) & (lax.rem(p, 2) == 0))
            def _():
                with jax.named_scope('flush'):
                    flush(p - 1, 2)

            relayout(s + 1, wb1)
            multiply(2 * i, wb0)
            relayout(s + 2, wb0)
            multiply(2 * i + 1, wb1)
            return c

        lax.fori_loop(0, chunks // 2, steps, 0)
        with jax.named_scope('epi'):
            epilogue(p)
        l_copy(p).start()

        @pl.when(mine(p))
        def _():
            own_copy(p).start()

        @pl.when(p == 0)
        def _():
            with jax.named_scope('flush0'):
                flush(p, 1)

        return c

    lax.fori_loop(0, pieces, project, 0)
    with jax.named_scope('lastflush'):
        flush(pieces - 1, 2)
        flush_rows()
    a_copy(1).wait()

    coef = math.log2(math.e) / math.sqrt(dim)
    per = q_blk // chunk
    kn = k_blk // chunk
    ratio = q_blk // k_blk

    def row_copies(b):
        slot = lax.rem(b, 2)
        return [pltpu.make_async_copy(rc.at[kind, b], buf.at[slot], row_sem.at[kind, slot])
                for kind, buf in ((0, qb), (1, kb), (2, vb))]

    def ctx_copies(b):
        slot = lax.rem(b, 2)
        at = pl.ds(pl.multiple_of(b * chunk, chunk), chunk)
        return [pltpu.make_async_copy(cb.at[slot], c_snd.at[:, at], c_sem.at[0, slot]),
                pltpu.make_async_copy(cb.at[slot, me], c_rc.at[me, at], c_sem.at[1, slot])]

    def attend_row(b):
        slot = lax.rem(b, 2)
        ctx = ctx_ref[b]
        step_v = min(512, seq)
        for c in range(seq // step_v):
            m = step_v // chunk
            vt[:, c * step_v:(c + 1) * step_v] = vb[slot, c * m:(c + 1) * m].reshape(step_v, dim).T
        blocks = seq // q_blk

        def scores(qi, j, s_slot, masked, prev):
            k_rows = kb[slot, pl.ds(j * kn, kn)].reshape(k_blk, dim)
            q_rows = qb[slot, pl.ds(qi * per, per)].reshape(q_blk, dim)
            s = lax.dot_general(k_rows, q_rows, (((1,), (1,)), ((), ())), preferred_element_type=F32)
            if masked:
                kpos = j * k_blk + lax.broadcasted_iota(jnp.int32, s.shape, 0)
                lim = jnp.maximum(ctx, qi * q_blk + 1 + lax.broadcasted_iota(jnp.int32, (1, q_blk), 1))
                s = jnp.where(kpos < lim, s, -jnp.inf)
            s_buf[s_slot] = s
            top = jnp.max(s, axis=0, keepdims=True) * coef
            if prev is None:
                m_buf[s_slot] = top
                a_buf[s_slot] = jnp.zeros_like(top)
            else:
                m_old = m_buf[prev]
                m_new = jnp.maximum(m_old, top)
                m_buf[s_slot] = m_new
                a_buf[s_slot] = jnp.exp2(m_old - m_new)

        def values(j, s_slot):
            v_cols = vt[:, pl.ds(pl.multiple_of(j * k_blk, k_blk), k_blk)]
            scale = a_buf[s_slot]
            p = jnp.exp2(s_buf[s_slot] * coef - m_buf[s_slot])
            l_s[...] = l_s[...] * scale + jnp.sum(p.reshape(k_blk // 8, 8, q_blk), axis=0)
            acc_s[...] = acc_s[...] * scale + jnp.dot(v_cols, p.astype(BF16), preferred_element_type=F32)

        def q_loop(qi, _):
            q0 = qi * q_blk
            l_s[...] = jnp.zeros_like(l_s)
            acc_s[...] = jnp.zeros_like(acc_s)

            def pair(i, masked):
                scores(qi, 2 * i + 1, 1, masked, 0)
                values(2 * i, 0)
                scores(qi, 2 * i + 2, 0, masked, 1)
                values(2 * i + 1, 1)

            last = (jnp.maximum(high, q0 + q_blk) + 2 * k_blk - 1) // (2 * k_blk) - 1
            full = jnp.minimum((jnp.maximum(low, q0) // k_blk - 1) // 2, last)
            lax.fori_loop(0, full, lambda i, c: (pair(i, False), c)[1], 0)
            lax.fori_loop(full, last, lambda i, c: (pair(i, True), c)[1], 0)
            scores(qi, 2 * last + 1, 1, True, 0)
            values(2 * last, 0)
            scores(jnp.minimum(qi + 1, blocks - 1), 0, 0, False, None)
            values(2 * last + 1, 1)
            inv = 1.0 / jnp.sum(l_s[...], axis=0, keepdims=True)
            cb[slot, pl.ds(qi * per, per)] = (acc_s[...] * inv).T.astype(BF16).reshape(per, chunk, dim)
            return 0

        scores(0, 0, 0, False, None)
        lax.fori_loop(0, blocks, q_loop, 0)

    def arrived(at, group_id):
        got = rc.at[:, at, pl.ds(0, n - 1)]
        pltpu.make_async_copy(got, got, rcv_sem.at[group_id]).wait()

    def give(b, first, count, sem):
        with jax.named_scope('ctxwait'):
            for r in range(count):
                for copy in ctx_copies(b - count + 1 + r):
                    copy.wait()

        for_peers(lambda dest: c_send(dest, first, count, sem).start())

    starts = ((0, pl.ds(0, half_rows)), (half_rows, pl.ds(half_rows, half_rows - 2)), (rows - 2, pl.ds(rows - 2, 1)), (rows - 1, pl.ds(rows - 1, 1)))

    def attend(b, c):
        for group_id, (row, at) in enumerate(starts):
            @pl.when(b == row)
            def _():
                with jax.named_scope(f'arr{group_id}'):
                    arrived(at, group_id)
                for copy in row_copies(b):
                    copy.start()

        @pl.when((b < half_rows - 1) | ((b >= half_rows) & (b < rows - 3)))
        def _():
            for copy in row_copies(b + 1):
                copy.start()

        with jax.named_scope('rowwait'):
            for copy in row_copies(b):
                copy.wait()
        with jax.named_scope('row'):
            attend_row(b)
        for copy in ctx_copies(b):
            copy.start()

        @pl.when((lax.rem(b, 2) == 1) & (b < half_rows))
        def _():
            give(b, b - 1, 2, 0)

        @pl.when(b == rows - 3)
        def _():
            give(b, b - 1, 2, 1)

        @pl.when(b >= rows - 2)
        def _():
            give(b, b, 1, 1)

        return c

    lax.fori_loop(0, rows, attend, 0)

    steps = depth // k_tile
    wide = group * dim

    def wd_copy(i, buf, slot):
        return pltpu.make_async_copy(
            wd_ref.at[pl.ds(pl.multiple_of(lax.rem(i, steps) * k_tile, k_tile), k_tile), pl.ds(pl.multiple_of(i // steps * wide, wide), wide)],
            buf, w_sem.at[slot])

    def lhs_copy(h):
        return pltpu.make_async_copy(c_rc.at[h, pl.ds(0, half_tok)], ab.at[:, pl.ds(pl.multiple_of(h * dim, dim), dim)], lhs_sem)

    wd_copy(0, wb0, 0).start()
    a_back = pltpu.make_async_copy(a_out.at[pl.ds(0, half_tok)], xb, x_sem)
    a_back.start()
    got = c_rc.at[pl.ds(0, n - 1), pl.ds(0, half_tok)]
    with jax.named_scope('cr0'):
        pltpu.make_async_copy(got, got, cr_sem.at[0]).wait()
    lax.fori_loop(0, heads, lambda h, c: (lhs_copy(h).start(), c)[1], 0)
    with jax.named_scope('lhswait'):
        lax.fori_loop(0, heads, lambda h, c: (lhs_copy(h).wait(), c)[1], 0)
        a_back.wait()

    def dense_half(t, c):
        def two(i, c):
            s = t * steps + 2 * i
            wd_copy(s + 1, wb1, 1).start()
            wd_copy(s, wb0, 0).wait()
            multiply(2 * i, wb0)

            @pl.when(s + 2 < 2 * steps)
            def _():
                wd_copy(s + 2, wb0, 0).start()

            wd_copy(s + 1, wb1, 1).wait()
            multiply(2 * i + 1, wb1)
            return c

        lax.fori_loop(0, steps // 2, two, 0)
        for u in range(wide // 256):
            cols = pl.ds(pl.multiple_of(t * wide + u * 256, 256), 256)
            part = slice(u * 256, (u + 1) * 256)
            shift = bd_row[:, cols]
            xb[:, cols] = (xb[:, cols].astype(F32) * ALPHA + (acc[:, part] + shift)).astype(BF16)
            acc[:, part] = jnp.zeros((half_tok, 256), F32)
        return c

    with jax.named_scope('dense'):
        lax.fori_loop(0, depth // wide, dense_half, 0)
    done = pltpu.make_async_copy(xb, half_out, x_sem)
    done.start()

    for group_id, (_, at) in enumerate(starts):
        gone = snd.at[:, pl.ds(0, n - 1), at]
        with jax.named_scope(f'drainsnd{group_id}'):
            pltpu.make_async_copy(gone, gone, snd_sem.at[group_id]).wait()
    gone = c_snd.at[pl.ds(0, n - 1)]
    with jax.named_scope('draincs'):
        pltpu.make_async_copy(gone, gone, cs_sem).wait()
    got = c_rc.at[pl.ds(0, n - 1), pl.ds(half_tok, half_tok)]
    with jax.named_scope('draincr'):
        pltpu.make_async_copy(got, got, cr_sem.at[1]).wait()
    done.wait()


def exchange(n, ctx_len, x, gamma, beta, w_rows, bias, pos_ids, block_ids, freq, w_dense, b_dense, rows, chunk, k_tile=512, q_blk=512, k_blk=512, low=CTX_LOW, high=CTX_HIGH):
    tokens, depth = x.shape
    _, kinds, heads, dim = w_rows.shape
    half_rows, group = split_sizes(rows, heads)
    half_tok = half_rows * chunk
    seq = n * chunk
    any_spec = pl.BlockSpec(memory_space=pl.ANY)
    vmem = pl.BlockSpec(memory_space=pltpu.VMEM)
    smem = pl.BlockSpec(memory_space=pltpu.SMEM)
    dma = pltpu.SemaphoreType.DMA
    cfg = (n, depth, k_tile, q_blk, k_blk, low, high)
    return pl.pallas_call(
        functools.partial(exchange_kernel, cfg),
        in_specs=[smem, any_spec, vmem, vmem, any_spec, vmem, vmem, vmem, vmem, any_spec, vmem],
        out_specs=[any_spec] * 6,
        out_shape=[
            jax.ShapeDtypeStruct((tokens, depth), BF16),
            jax.ShapeDtypeStruct((kinds, heads, rows, chunk, dim), BF16),
            jax.ShapeDtypeStruct((kinds, rows, n, chunk, dim), BF16),
            jax.ShapeDtypeStruct((n, tokens, dim), BF16),
            jax.ShapeDtypeStruct((heads, tokens, dim), BF16),
            jax.ShapeDtypeStruct((half_tok, depth), BF16),
        ],
        scratch_shapes=[
            pltpu.VMEM((half_tok, depth), BF16),
            pltpu.VMEM((half_tok, depth), BF16),
            pltpu.VMEM((4, k_tile, group, dim), BF16),
            pltpu.VMEM((k_tile, group * dim), BF16),
            pltpu.VMEM((k_tile, group * dim), BF16),
            pltpu.VMEM((half_tok, group * dim), F32),
            pltpu.VMEM((2, group, half_rows, chunk, dim), BF16),
            pltpu.VMEM((2, n, chunk, dim), BF16),
            pltpu.VMEM((2, n, chunk, dim), BF16),
            pltpu.VMEM((2, n, chunk, dim), BF16),
            pltpu.VMEM((2, n, chunk, dim), BF16),
            pltpu.VMEM((dim, seq), BF16),
            pltpu.VMEM((2, k_blk, q_blk), F32),
            pltpu.VMEM((2, 1, q_blk), F32),
            pltpu.VMEM((2, 1, q_blk), F32),
            pltpu.VMEM((8, q_blk), F32),
            pltpu.VMEM((dim, q_blk), F32),
            pltpu.VMEM((tokens, dim), F32),
            pltpu.VMEM((tokens, dim), F32),
            pltpu.VMEM((1, depth), F32),
            dma, dma, dma((4,)), dma((2,)), dma((2,)), dma((4,)), dma((4,)), dma((3, 2)), dma((2, 2)), dma, dma((2,)), dma,
        ],
        compiler_params=pltpu.CompilerParams(vmem_limit_bytes=VMEM_CAP, collective_id=0, has_side_effects=True),
        cost_estimate=pl.CostEstimate(flops=2 * tokens * depth * kinds * heads * dim, bytes_accessed=4 * depth * kinds * heads * dim, transcendentals=0),
        name="exchange",
    )(ctx_len, x, gamma, beta, w_rows, bias, pos_ids, block_ids, freq, w_dense, b_dense)


def dense_kernel(c_ref, w_ref, b_ref, a_hbm, kv_hbm, half_hbm, o_hbm, ko_hbm, vo_hbm, lhs, acc, a_buf, kv_buf, h_buf, a_sem, in_sem, out_sem, o_sem):
    heads_blk, tokens, dim = c_ref.shape
    side, step = pl.program_id(0), pl.program_id(1)
    steps = pl.num_programs(1)
    turns = 2 * steps
    turn = side * steps + step
    wide = w_ref.shape[1]
    rest = pl.ds(tokens, tokens)
    share = tokens // turns

    def cols_of(i):
        return pl.ds(pl.multiple_of(i * wide, wide), wide)

    def a_copy(i):
        return pltpu.make_async_copy(a_hbm.at[rest, cols_of(i)], a_buf.at[i], a_sem.at[i])

    def o_copy(i):
        return pltpu.make_async_copy(a_buf.at[i], o_hbm.at[rest, cols_of(i)], o_sem.at[i])

    def part(i):
        return pl.ds(pl.multiple_of(i * share, share), share)

    def in_copies(i):
        slot = lax.rem(i, 2)
        return [pltpu.make_async_copy(kv_hbm.at[pl.ds(1, 2), i], kv_buf.at[slot], in_sem.at[0, slot]),
                pltpu.make_async_copy(half_hbm.at[part(i)], h_buf.at[slot], in_sem.at[1, slot])]

    def out_copies(i):
        slot = lax.rem(i, 2)
        return [pltpu.make_async_copy(kv_buf.at[slot, 0], ko_hbm.at[i], out_sem.at[0, slot]),
                pltpu.make_async_copy(kv_buf.at[slot, 1], vo_hbm.at[i], out_sem.at[1, slot]),
                pltpu.make_async_copy(h_buf.at[slot], o_hbm.at[part(i)], out_sem.at[2, slot])]

    def start(copies):
        for copy in copies:
            copy.start()

    def wait(copies):
        for copy in copies:
            copy.wait()

    @pl.when(turn == 0)
    def _():
        start(in_copies(0))
        start([a_copy(0), a_copy(1)])

    wait(in_copies(turn))
    start(out_copies(turn))

    @pl.when(turn > 0)
    def _():
        wait(out_copies(turn - 1))

    @pl.when(turn + 1 < turns)
    def _():
        start(in_copies(turn + 1))

    depth_blk = heads_blk * dim
    base = pl.multiple_of(step * depth_blk, depth_blk)

    @pl.when(side == 0)
    def _():
        for h in range(heads_blk):
            lhs[:, pl.ds(base + h * dim, dim)] = c_ref[h]

    left = lhs[:, pl.ds(base, depth_blk)]

    def product(first):
        for t in range(wide // 256):
            cols = slice(t * 256, (t + 1) * 256)
            prod = jnp.dot(left, w_ref[:, cols], preferred_element_type=F32)
            acc[:, cols] = prod if first else acc[:, cols] + prod

    @pl.when(step == 0)
    def _():
        product(True)

    @pl.when(step > 0)
    def _():
        product(False)

    @pl.when(step == steps - 1)
    def _():
        a_copy(side).wait()
        a_buf[side] = (a_buf[side].astype(F32) * ALPHA + (acc[...] + b_ref[...].astype(F32).reshape(1, -1))).astype(BF16)
        o_copy(side).start()

    @pl.when(turn == turns - 1)
    def _():
        wait(out_copies(turn))
        wait([o_copy(0), o_copy(1)])


def dense(context, w_dense, bias, normed, kv, half_out):
    heads, tokens, dim = context.shape
    depth, width = w_dense.shape
    kinds, rows, seq, _ = kv.shape
    half_tok = tokens // 2
    steps = rows // 2
    any_spec = pl.BlockSpec(memory_space=pl.ANY)
    wide = width // 2
    dma = pltpu.SemaphoreType.DMA
    return pl.pallas_call(
        dense_kernel,
        grid=(2, steps),
        in_specs=[
            pl.BlockSpec((heads // steps, half_tok, dim), lambda i, k: (lax.select(i == 0, k, steps - 1), 1, 0)),
            pl.BlockSpec((depth // steps, wide), lambda i, k: (k, i)),
            pl.BlockSpec((wide,), lambda i, k: (i,)),
            any_spec,
            any_spec,
            any_spec,
        ],
        out_specs=[any_spec] * 3,
        out_shape=[
            jax.ShapeDtypeStruct((tokens, width), BF16),
            jax.ShapeDtypeStruct((rows, seq, dim), BF16),
            jax.ShapeDtypeStruct((rows, seq, dim), BF16),
        ],
        scratch_shapes=[
            pltpu.VMEM((half_tok, depth), BF16),
            pltpu.VMEM((half_tok, wide), F32),
            pltpu.VMEM((2, half_tok, wide), BF16),
            pltpu.VMEM((2, 2, seq, dim), BF16),
            pltpu.VMEM((2, half_tok // (2 * steps), width), BF16),
            dma((2,)), dma((2, 2)), dma((3, 2)), dma((2,)),
        ],
        compiler_params=pltpu.CompilerParams(vmem_limit_bytes=VMEM_CAP),
        cost_estimate=pl.CostEstimate(flops=tokens * depth * width, bytes_accessed=2 * depth * width, transcendentals=0),
        name="dense",
    )(context, w_dense, bias, normed, kv, half_out)


def solution(mesh):
    seq_spec = P('dp', 'sp', None)
    row_spec = P('dp', 'sp')
    head_spec = P('dp', None, 'sp', None)
    rep = P()
    devices = mesh.shape['sp']

    def local_block(hidden, pos_ids, block_ids, ctx_len, ln_gamma, ln_beta, w_qkv, b_qkv, w_dense, b_dense):
        rows, chunk, width = hidden.shape
        depth, heads, kinds, dim = w_qkv.shape
        seq = chunk * devices
        tokens = rows * chunk
        w_rows = jnp.transpose(w_qkv, (0, 2, 1, 3))
        bias = jnp.transpose(b_qkv, (1, 0, 2))
        normed, _, recv, _, context, half_out = exchange(
            devices, ctx_len, hidden.reshape(tokens, width), ln_gamma, ln_beta, w_rows, bias, pos_ids, block_ids, rotary_freq(dim), w_dense, b_dense, rows, chunk)
        out, keys, values = dense(context, w_dense, b_dense, normed, recv.reshape(kinds, rows, seq, dim), half_out)
        return out.reshape(rows, chunk, width), keys.reshape(rows, seq, 1, dim), values.reshape(rows, seq, 1, dim)

    return jax.shard_map(local_block, mesh=mesh, in_specs=(seq_spec, row_spec, row_spec, P('dp'), rep, rep, rep, rep, rep, rep), out_specs=(seq_spec, head_spec, head_spec), check_vma=False)
```

```python
import functools
import math

import jax
import jax.numpy as jnp
from jax import lax
from jax.experimental import pallas as pl
from jax.experimental.pallas import tpu as pltpu
from jax.sharding import PartitionSpec as P

ALPHA = math.sqrt(56.0)
ROPE_BASE = 10000.0
LN_EPS = 1e-5
CTX_LOW = 1024
CTX_HIGH = 3072
F32 = jnp.float32
BF16 = jnp.bfloat16
VMEM_CAP = 60000 * 1024
MESH_ID = pl.DeviceIdType.MESH


SHIFT_PAIRS = (((1, 0), (3, 2)), ((1, 1), (3, 3)), ((3, 0), (1, 2)), ((0, 1), (2, 3)),
               ((1, 3), (3, 1)), ((0, 3), (2, 1)), ((2, 0), (0, 2)), ((2, 2), (0, 0)))


def shift_codes(side):
    if side == 4:
        pairs = SHIFT_PAIRS
    else:
        shifts = [(i % side, i // side) for i in range(side * side)]
        pairs = tuple(zip(shifts[0::2], shifts[1::2]))
    return len(pairs), [sum(pair[k // 2][k % 2] * side ** u for u, pair in enumerate(pairs)) for k in range(4)]


def rotary_freq(dim):
    half = dim // 2
    lane = lax.rem(lax.broadcasted_iota(jnp.int32, (1, dim), 1), half // 2)
    return ROPE_BASE ** (-(2 * lane).astype(F32) / half)


def split_sizes(rows, heads):
    return rows // 2, heads // 2


def exchange_kernel(cfg, ctx_ref, x_ref, g_ref, be_ref, w_ref, bias_ref, pos_ref, blk_ref, freq_ref, wd_ref, bd_ref,
                    a_out, snd, rc, c_snd, c_rc, half_out,
                    xb, ab, wbuf, wb0, wb1, acc, sb, qb, kb, vb, cb, vt, s_buf, m_buf, a_buf, l_s, acc_s, cos_ref, sin_ref, bd_row,
                    x_sem, a_sem, w_sem, l_sem, o_sem, snd_sem, rcv_sem, row_sem, c_sem, cs_sem, cr_sem, lhs_sem):
    n, depth, k_tile, q_blk, k_blk, low, high = cfg
    _, heads, rows, chunk, dim = snd.shape
    half_rows, group = split_sizes(rows, heads)
    half_tok = half_rows * chunk
    seq = n * chunk
    pieces = 12
    chunks = depth // k_tile
    total = pieces * chunks
    me = lax.axis_index('sp')

    barrier = pltpu.get_barrier_semaphore()

    def greet(i, c):
        pl.semaphore_signal(barrier, inc=1, device_id={'sp': lax.rem(me + i, n)}, device_id_type=MESH_ID)
        return c

    def piece_of(p):
        hf = p // 6
        kind = 2 - lax.rem(p, 6) // 2
        hh = lax.rem(p, 2)
        return hf, kind, hh

    def w_copy(s):
        _, kind, hh = piece_of(s // chunks)
        c = lax.rem(s, chunks)
        slot = lax.rem(s, 4)
        return pltpu.make_async_copy(
            w_ref.at[pl.ds(pl.multiple_of(c * k_tile, k_tile), k_tile), kind, pl.ds(pl.multiple_of(hh * group, group), group)],
            wbuf.at[slot], w_sem.at[slot])

    def x_copy(hf):
        return pltpu.make_async_copy(x_ref.at[pl.ds(pl.multiple_of(hf * half_tok, half_tok), half_tok)], xb, x_sem)

    def a_copy(hf):
        return pltpu.make_async_copy(ab, a_out.at[pl.ds(pl.multiple_of(hf * half_tok, half_tok), half_tok)], a_sem)

    def l_copy(p):
        hf, kind, hh = piece_of(p)
        slot = lax.rem(p, 2)
        return pltpu.make_async_copy(
            sb.at[slot],
            snd.at[kind, pl.ds(pl.multiple_of(hh * group, group), group), pl.ds(hf * half_rows, half_rows)],
            l_sem.at[slot])

    def own_copy(p):
        hf, kind, hh = piece_of(p)
        slot = lax.rem(p, 2)
        return pltpu.make_async_copy(
            sb.at[slot, lax.rem(me, group)],
            rc.at[kind, pl.ds(hf * half_rows, half_rows), me],
            o_sem.at[slot])

    def mine(p):
        return piece_of(p)[2] == me // group

    def send(kind, head, hf):
        def start(at, group_id):
            pltpu.make_async_remote_copy(
                src_ref=snd.at[kind, head, at], dst_ref=rc.at[kind, at, me],
                send_sem=snd_sem.at[group_id], recv_sem=rcv_sem.at[group_id],
                device_id={'sp': head}, device_id_type=MESH_ID).start()

        @pl.when(hf == 0)
        def _():
            start(pl.ds(0, half_rows), 0)

        @pl.when(hf == 1)
        def _():
            start(pl.ds(half_rows, half_rows - 2), 1)

    def send_row(head, row, group_id):
        pltpu.make_async_remote_copy(
            src_ref=snd.at[:, head, row], dst_ref=rc.at[:, row, me],
            send_sem=snd_sem.at[group_id], recv_sem=rcv_sem.at[group_id],
            device_id={'sp': head}, device_id_type=MESH_ID).start()

    def c_send(dest, first, count, sem):
        at = pl.ds(pl.multiple_of(first * chunk, chunk), count * chunk)
        return pltpu.make_async_remote_copy(
            src_ref=c_snd.at[dest, at], dst_ref=c_rc.at[me, at],
            send_sem=cs_sem, recv_sem=cr_sem.at[sem], device_id={'sp': dest}, device_id_type=MESH_ID)

    def layer_norm(hf):
        x_copy(hf).wait()
        sub = 16
        tile = min(64, half_tok)
        lanes = [slice(c * 128, (c + 1) * 128) for c in range(depth // 128)]

        def body(i, c):
            ats = [pl.ds(pl.multiple_of(i * tile + u * sub, sub), sub) for u in range(tile // sub)]
            means, scales = [], []
            for at in ats:
                total = sum(xb[at, cols].astype(F32) for cols in lanes)
                means.append(jnp.sum(total, axis=-1, keepdims=True) * (1.0 / depth))
            for at, mean in zip(ats, means):
                total = sum(jnp.square(xb[at, cols].astype(F32) - mean) for cols in lanes)
                scales.append(lax.rsqrt(jnp.sum(total, axis=-1, keepdims=True) * (1.0 / depth) + LN_EPS))
            for cols in lanes:
                gain = g_ref[cols].astype(F32).reshape(1, 128)
                shift = be_ref[cols].astype(F32).reshape(1, 128)
                for at, mean, scale in zip(ats, means, scales):
                    ab[at, cols] = ((xb[at, cols].astype(F32) - mean) * scale * gain + shift).astype(BF16)
            return c

        lax.fori_loop(0, half_tok // tile, body, 0)

    def tables():
        lane = lax.broadcasted_iota(jnp.int32, (1, dim), 1)

        def body(r, c):
            at = pl.ds(pl.multiple_of(r * chunk, chunk), chunk)
            pos = jnp.broadcast_to(pos_ref[pl.ds(r, 1), :].astype(F32), (dim, chunk)).T
            blk = jnp.broadcast_to(blk_ref[pl.ds(r, 1), :].astype(F32), (dim, chunk)).T
            ang = jnp.where(lane < dim // 2, pos, blk) * freq_ref[...]
            sin = jnp.sin(ang)
            cos_ref[at, :] = jnp.cos(ang)
            sin_ref[at, :] = jnp.where(lax.rem(lane, dim // 2) < dim // 4, -sin, sin)
            return c

        lax.fori_loop(0, rows, body, 0)

    def relayout(s, wb):
        slot = lax.rem(s, 4)
        sub = min(64, k_tile)
        for part in range(k_tile // sub):
            lo = part * sub
            tile = jnp.swapaxes(wbuf[slot, lo:lo + sub], 0, 1)
            for head in range(group):
                wb[lo:lo + sub, head * dim:(head + 1) * dim] = tile[head]

    def multiply(c, wb):
        lhs = ab[:, pl.ds(pl.multiple_of(c * k_tile, k_tile), k_tile)]
        wide = min(256, group * dim)
        for t in range(group * dim // wide):
            cols = slice(t * wide, (t + 1) * wide)
            acc[:, cols] += jnp.dot(lhs, wb[:, cols], preferred_element_type=F32)

    def epilogue(p):
        hf, kind, hh = piece_of(p)
        slot = lax.rem(p, 2)
        toks = pl.ds(pl.multiple_of(hf * half_tok, half_tok), half_tok)
        turn = min(4, group)
        bias = bias_ref[kind, pl.ds(pl.multiple_of(hh * group, group), group), :].astype(F32)
        fill = jnp.zeros((half_tok, dim), F32)
        lane = lax.broadcasted_iota(jnp.int32, (1, dim), 1)
        first = lax.rem(lane, dim // 2) < dim // 4

        def biased(h, row):
            cols = pl.ds(pl.multiple_of(h * dim, dim), dim)
            x = (acc[:, cols] + row).astype(BF16)
            acc[:, cols] = fill
            return x

        def rows_of(t):
            return [bias[t * turn + u:t * turn + u + 1, :] for u in range(turn)]

        for t in range(group // turn):
            @pl.when(kind < 2)
            def _():
                for u, row in enumerate(rows_of(t)):
                    h = t * turn + u
                    x = biased(h, row).astype(F32)
                    pair = jnp.where(first, pltpu.roll(x, dim - dim // 4, 1), pltpu.roll(x, dim // 4, 1))
                    x = (x * cos_ref[toks, :] + pair * sin_ref[toks, :]).astype(BF16)
                    sb[slot, h] = x.reshape(half_rows, chunk, dim)

            @pl.when(kind == 2)
            def _():
                for u, row in enumerate(rows_of(t)):
                    h = t * turn + u
                    sb[slot, h] = biased(h, row).reshape(half_rows, chunk, dim)

    side = math.isqrt(n // 2)
    pair_count, codes = shift_codes(side)

    def for_peers(act):
        core = lax.rem(me, 2)

        def sweep(flip, c):
            def one(u, rest):
                digit = [lax.rem(code, side) for code in rest]
                for r in range(2):
                    second = lax.rem(r + core, 2)
                    dx = digit[0] + second * (digit[2] - digit[0])
                    dy = digit[1] + second * (digit[3] - digit[1])
                    y = lax.rem(me // (2 * side) + dy, side)
                    x = lax.rem(me // 2 + dx, side)
                    peer = (y * side + x) * 2 + lax.rem(me + flip, 2)

                    @pl.when(peer != me)
                    def _():
                        act(peer)

                return tuple(code // side for code in rest)

            lax.fori_loop(0, pair_count, one, tuple(jnp.int32(code) for code in codes))
            return c

        lax.fori_loop(0, 2, sweep, 0)

    def landed(p):
        l_copy(p).wait()

        @pl.when(mine(p))
        def _():
            own_copy(p).wait()

    def flush(p, count):
        hf, kind, hh = piece_of(p)
        landed(p)
        if count == 2:
            landed(p - 1)

        def act(head):
            if count == 2:
                send(kind, head, hf)
            else:
                @pl.when(head // group == hh)
                def _():
                    send(kind, head, hf)

        for_peers(act)

    def flush_rows():
        for r in range(2):
            for_peers(lambda head: send_row(head, rows - 2 + r, 2 + r))

    x_copy(0).start()
    for s in range(3):
        w_copy(s).start()
    lax.fori_loop(1, n, greet, 0)
    acc[...] = jnp.zeros_like(acc)
    w_copy(0).wait()
    relayout(0, wb0)
    with jax.named_scope('ln0'):
        layer_norm(0)
    with jax.named_scope('barrier_wait'):
        pl.semaphore_wait(barrier, n - 1)

    def project(p, c):
        @pl.when(p == 6)
        def _():
            with jax.named_scope('ln1'):
                a_copy(0).wait()
                layer_norm(1)
                a_copy(1).start()

        @pl.when(p == 1)
        def _():
            a_copy(0).start()
            x_copy(1).start()
            bd_row[...] = bd_ref[...].astype(F32).reshape(1, -1)
            with jax.named_scope('tables'):
                tables()

        def steps(i, c):
            s = p * chunks + 2 * i
            w_copy(s + 1).wait()

            @pl.when(s + 2 < total)
            def _():
                w_copy(s + 2).wait()

            @pl.when(s + 3 < total)
            def _():
                w_copy(s + 3).start()

            @pl.when(s + 4 < total)
            def _():
                w_copy(s + 4).start()

            @pl.when((i == 1) & (p == 2))
            def _():
                with jax.named_scope('flush'):
                    flush(p - 1, 1)

            @pl.when((i == 1) & (p > 2) & (lax.rem(p, 2) == 0))
            def _():
                with jax.named_scope('flush'):
                    flush(p - 1, 2)

            relayout(s + 1, wb1)
            multiply(2 * i, wb0)
            relayout(s + 2, wb0)
            multiply(2 * i + 1, wb1)
            return c

        lax.fori_loop(0, chunks // 2, steps, 0)
        with jax.named_scope('epi'):
            epilogue(p)
        l_copy(p).start()

        @pl.when(mine(p))
        def _():
            own_copy(p).start()

        @pl.when(p == 0)
        def _():
            with jax.named_scope('flush0'):
                flush(p, 1)

        return c

    lax.fori_loop(0, pieces, project, 0)
    with jax.named_scope('lastflush'):
        flush(pieces - 1, 2)
        flush_rows()
    a_copy(1).wait()

    coef = math.log2(math.e) / math.sqrt(dim)
    per = q_blk // chunk
    kn = k_blk // chunk
    ratio = q_blk // k_blk

    def row_copies(b):
        slot = lax.rem(b, 2)
        return [pltpu.make_async_copy(rc.at[kind, b], buf.at[slot], row_sem.at[kind, slot])
                for kind, buf in ((0, qb), (1, kb), (2, vb))]

    def ctx_copies(b):
        slot = lax.rem(b, 2)
        at = pl.ds(pl.multiple_of(b * chunk, chunk), chunk)
        return [pltpu.make_async_copy(cb.at[slot], c_snd.at[:, at], c_sem.at[0, slot]),
                pltpu.make_async_copy(cb.at[slot, me], c_rc.at[me, at], c_sem.at[1, slot])]

    def attend_row(b):
        slot = lax.rem(b, 2)
        ctx = ctx_ref[b]
        step_v = min(512, seq)
        for c in range(seq // step_v):
            m = step_v // chunk
            vt[:, c * step_v:(c + 1) * step_v] = vb[slot, c * m:(c + 1) * m].reshape(step_v, dim).T
        blocks = seq // q_blk

        def scores(qi, j, s_slot, masked, prev):
            k_rows = kb[slot, pl.ds(j * kn, kn)].reshape(k_blk, dim)
            q_rows = qb[slot, pl.ds(qi * per, per)].reshape(q_blk, dim)
            s = lax.dot_general(k_rows, q_rows, (((1,), (1,)), ((), ())), preferred_element_type=F32)
            if masked:
                kpos = j * k_blk + lax.broadcasted_iota(jnp.int32, s.shape, 0)
                lim = jnp.maximum(ctx, qi * q_blk + 1 + lax.broadcasted_iota(jnp.int32, (1, q_blk), 1))
                s = jnp.where(kpos < lim, s, -jnp.inf)
            s_buf[s_slot] = s
            top = jnp.max(s, axis=0, keepdims=True) * coef
            if prev is None:
                m_buf[s_slot] = top
                a_buf[s_slot] = jnp.zeros_like(top)
            else:
                m_old = m_buf[prev]
                m_new = jnp.maximum(m_old, top)
                m_buf[s_slot] = m_new
                a_buf[s_slot] = jnp.exp2(m_old - m_new)

        def values(j, s_slot):
            v_cols = vt[:, pl.ds(pl.multiple_of(j * k_blk, k_blk), k_blk)]
            scale = a_buf[s_slot]
            p = jnp.exp2(s_buf[s_slot] * coef - m_buf[s_slot])
            l_s[...] = l_s[...] * scale + jnp.sum(p.reshape(k_blk // 8, 8, q_blk), axis=0)
            acc_s[...] = acc_s[...] * scale + jnp.dot(v_cols, p.astype(BF16), preferred_element_type=F32)

        def q_loop(qi, _):
            q0 = qi * q_blk
            l_s[...] = jnp.zeros_like(l_s)
            acc_s[...] = jnp.zeros_like(acc_s)

            def pair(i, masked):
                scores(qi, 2 * i + 1, 1, masked, 0)
                values(2 * i, 0)
                scores(qi, 2 * i + 2, 0, masked, 1)
                values(2 * i + 1, 1)

            last = (jnp.maximum(high, q0 + q_blk) + 2 * k_blk - 1) // (2 * k_blk) - 1
            full = jnp.minimum((jnp.maximum(low, q0) // k_blk - 1) // 2, last)
            lax.fori_loop(0, full, lambda i, c: (pair(i, False), c)[1], 0)
            lax.fori_loop(full, last, lambda i, c: (pair(i, True), c)[1], 0)
            scores(qi, 2 * last + 1, 1, True, 0)
            values(2 * last, 0)
            scores(jnp.minimum(qi + 1, blocks - 1), 0, 0, False, None)
            values(2 * last + 1, 1)
            inv = 1.0 / jnp.sum(l_s[...], axis=0, keepdims=True)
            cb[slot, pl.ds(qi * per, per)] = (acc_s[...] * inv).T.astype(BF16).reshape(per, chunk, dim)
            return 0

        scores(0, 0, 0, False, None)
        lax.fori_loop(0, blocks, q_loop, 0)

    def arrived(at, group_id):
        got = rc.at[:, at, pl.ds(0, n - 1)]
        pltpu.make_async_copy(got, got, rcv_sem.at[group_id]).wait()

    def give(b, first, count, sem):
        with jax.named_scope('ctxwait'):
            for r in range(count):
                for copy in ctx_copies(b - count + 1 + r):
                    copy.wait()

        for_peers(lambda dest: c_send(dest, first, count, sem).start())

    starts = ((0, pl.ds(0, half_rows)), (half_rows, pl.ds(half_rows, half_rows - 2)), (rows - 2, pl.ds(rows - 2, 1)), (rows - 1, pl.ds(rows - 1, 1)))

    def attend(b, c):
        for group_id, (row, at) in enumerate(starts):
            @pl.when(b == row)
            def _():
                with jax.named_scope(f'arr{group_id}'):
                    arrived(at, group_id)
                for copy in row_copies(b):
                    copy.start()

        @pl.when((b < half_rows - 1) | ((b >= half_rows) & (b < rows - 3)))
        def _():
            for copy in row_copies(b + 1):
                copy.start()

        with jax.named_scope('rowwait'):
            for copy in row_copies(b):
                copy.wait()
        with jax.named_scope('row'):
            attend_row(b)
        for copy in ctx_copies(b):
            copy.start()

        @pl.when((lax.rem(b, 2) == 1) & (b < half_rows))
        def _():
            give(b, b - 1, 2, 0)

        @pl.when(b == rows - 3)
        def _():
            give(b, b - 1, 2, 1)

        @pl.when(b >= rows - 2)
        def _():
            give(b, b, 1, 1)

        return c

    lax.fori_loop(0, rows, attend, 0)

    steps = depth // k_tile
    wide = group * dim

    def wd_copy(i, buf, slot):
        return pltpu.make_async_copy(
            wd_ref.at[pl.ds(pl.multiple_of(lax.rem(i, steps) * k_tile, k_tile), k_tile), pl.ds(pl.multiple_of(i // steps * wide, wide), wide)],
            buf, w_sem.at[slot])

    def lhs_copy(h):
        return pltpu.make_async_copy(c_rc.at[h, pl.ds(0, half_tok)], ab.at[:, pl.ds(pl.multiple_of(h * dim, dim), dim)], lhs_sem)

    wd_copy(0, wb0, 0).start()
    a_back = pltpu.make_async_copy(a_out.at[pl.ds(0, half_tok)], xb, x_sem)
    a_back.start()
    got = c_rc.at[pl.ds(0, n - 1), pl.ds(0, half_tok)]
    with jax.named_scope('cr0'):
        pltpu.make_async_copy(got, got, cr_sem.at[0]).wait()
    lax.fori_loop(0, heads, lambda h, c: (lhs_copy(h).start(), c)[1], 0)
    with jax.named_scope('lhswait'):
        lax.fori_loop(0, heads, lambda h, c: (lhs_copy(h).wait(), c)[1], 0)
        a_back.wait()

    def dense_half(t, c):
        def two(i, c):
            s = t * steps + 2 * i
            wd_copy(s + 1, wb1, 1).start()
            wd_copy(s, wb0, 0).wait()
            multiply(2 * i, wb0)

            @pl.when(s + 2 < 2 * steps)
            def _():
                wd_copy(s + 2, wb0, 0).start()

            wd_copy(s + 1, wb1, 1).wait()
            multiply(2 * i + 1, wb1)
            return c

        lax.fori_loop(0, steps // 2, two, 0)
        for u in range(wide // 256):
            cols = pl.ds(pl.multiple_of(t * wide + u * 256, 256), 256)
            part = slice(u * 256, (u + 1) * 256)
            shift = bd_row[:, cols]
            xb[:, cols] = (xb[:, cols].astype(F32) * ALPHA + (acc[:, part] + shift)).astype(BF16)
            acc[:, part] = jnp.zeros((half_tok, 256), F32)
        return c

    with jax.named_scope('dense'):
        lax.fori_loop(0, depth // wide, dense_half, 0)
    done = pltpu.make_async_copy(xb, half_out, x_sem)
    done.start()

    for group_id, (_, at) in enumerate(starts):
        gone = snd.at[:, pl.ds(0, n - 1), at]
        with jax.named_scope(f'drainsnd{group_id}'):
            pltpu.make_async_copy(gone, gone, snd_sem.at[group_id]).wait()
    gone = c_snd.at[pl.ds(0, n - 1)]
    with jax.named_scope('draincs'):
        pltpu.make_async_copy(gone, gone, cs_sem).wait()
    got = c_rc.at[pl.ds(0, n - 1), pl.ds(half_tok, half_tok)]
    with jax.named_scope('draincr'):
        pltpu.make_async_copy(got, got, cr_sem.at[1]).wait()
    done.wait()


def exchange(n, ctx_len, x, gamma, beta, w_rows, bias, pos_ids, block_ids, freq, w_dense, b_dense, rows, chunk, k_tile=512, q_blk=512, k_blk=512, low=CTX_LOW, high=CTX_HIGH):
    tokens, depth = x.shape
    _, kinds, heads, dim = w_rows.shape
    half_rows, group = split_sizes(rows, heads)
    half_tok = half_rows * chunk
    seq = n * chunk
    any_spec = pl.BlockSpec(memory_space=pl.ANY)
    vmem = pl.BlockSpec(memory_space=pltpu.VMEM)
    smem = pl.BlockSpec(memory_space=pltpu.SMEM)
    dma = pltpu.SemaphoreType.DMA
    cfg = (n, depth, k_tile, q_blk, k_blk, low, high)
    return pl.pallas_call(
        functools.partial(exchange_kernel, cfg),
        in_specs=[smem, any_spec, vmem, vmem, any_spec, vmem, vmem, vmem, vmem, any_spec, vmem],
        out_specs=[any_spec] * 6,
        out_shape=[
            jax.ShapeDtypeStruct((tokens, depth), BF16),
            jax.ShapeDtypeStruct((kinds, heads, rows, chunk, dim), BF16),
            jax.ShapeDtypeStruct((kinds, rows, n, chunk, dim), BF16),
            jax.ShapeDtypeStruct((n, tokens, dim), BF16),
            jax.ShapeDtypeStruct((heads, tokens, dim), BF16),
            jax.ShapeDtypeStruct((half_tok, depth), BF16),
        ],
        scratch_shapes=[
            pltpu.VMEM((half_tok, depth), BF16),
            pltpu.VMEM((half_tok, depth), BF16),
            pltpu.VMEM((4, k_tile, group, dim), BF16),
            pltpu.VMEM((k_tile, group * dim), BF16),
            pltpu.VMEM((k_tile, group * dim), BF16),
            pltpu.VMEM((half_tok, group * dim), F32),
            pltpu.VMEM((2, group, half_rows, chunk, dim), BF16),
            pltpu.VMEM((2, n, chunk, dim), BF16),
            pltpu.VMEM((2, n, chunk, dim), BF16),
            pltpu.VMEM((2, n, chunk, dim), BF16),
            pltpu.VMEM((2, n, chunk, dim), BF16),
            pltpu.VMEM((dim, seq), BF16),
            pltpu.VMEM((2, k_blk, q_blk), F32),
            pltpu.VMEM((2, 1, q_blk), F32),
            pltpu.VMEM((2, 1, q_blk), F32),
            pltpu.VMEM((8, q_blk), F32),
            pltpu.VMEM((dim, q_blk), F32),
            pltpu.VMEM((tokens, dim), F32),
            pltpu.VMEM((tokens, dim), F32),
            pltpu.VMEM((1, depth), F32),
            dma, dma, dma((4,)), dma((2,)), dma((2,)), dma((4,)), dma((4,)), dma((3, 2)), dma((2, 2)), dma, dma((2,)), dma,
        ],
        compiler_params=pltpu.CompilerParams(vmem_limit_bytes=VMEM_CAP, collective_id=0, has_side_effects=True),
        cost_estimate=pl.CostEstimate(flops=2 * tokens * depth * kinds * heads * dim, bytes_accessed=4 * depth * kinds * heads * dim, transcendentals=0),
        name="exchange",
    )(ctx_len, x, gamma, beta, w_rows, bias, pos_ids, block_ids, freq, w_dense, b_dense)


def dense_kernel(c_ref, w_ref, b_ref, a_hbm, kv_hbm, half_hbm, o_hbm, ko_hbm, vo_hbm, lhs, acc, a_buf, kv_buf, h_buf, a_sem, in_sem, out_sem, o_sem):
    heads_blk, tokens, dim = c_ref.shape
    side, step = pl.program_id(0), pl.program_id(1)
    steps = pl.num_programs(1)
    turns = 2 * steps
    turn = side * steps + step
    wide = w_ref.shape[1]
    rest = pl.ds(tokens, tokens)
    share = tokens // turns

    def cols_of(i):
        return pl.ds(pl.multiple_of(i * wide, wide), wide)

    def a_copy(i):
        return pltpu.make_async_copy(a_hbm.at[rest, cols_of(i)], a_buf.at[i], a_sem.at[i])

    def o_copy(i):
        return pltpu.make_async_copy(a_buf.at[i], o_hbm.at[rest, cols_of(i)], o_sem.at[i])

    def part(i):
        return pl.ds(pl.multiple_of(i * share, share), share)

    def in_copies(i):
        slot = lax.rem(i, 2)
        return [pltpu.make_async_copy(kv_hbm.at[pl.ds(1, 2), i], kv_buf.at[slot], in_sem.at[0, slot]),
                pltpu.make_async_copy(half_hbm.at[part(i)], h_buf.at[slot], in_sem.at[1, slot])]

    def out_copies(i):
        slot = lax.rem(i, 2)
        return [pltpu.make_async_copy(kv_buf.at[slot, 0], ko_hbm.at[i], out_sem.at[0, slot]),
                pltpu.make_async_copy(kv_buf.at[slot, 1], vo_hbm.at[i], out_sem.at[1, slot]),
                pltpu.make_async_copy(h_buf.at[slot], o_hbm.at[part(i)], out_sem.at[2, slot])]

    def start(copies):
        for copy in copies:
            copy.start()

    def wait(copies):
        for copy in copies:
            copy.wait()

    @pl.when(turn == 0)
    def _():
        start(in_copies(0))
        start([a_copy(0), a_copy(1)])

    wait(in_copies(turn))
    start(out_copies(turn))

    @pl.when(turn > 0)
    def _():
        wait(out_copies(turn - 1))

    @pl.when(turn + 1 < turns)
    def _():
        start(in_copies(turn + 1))

    depth_blk = heads_blk * dim
    base = pl.multiple_of(step * depth_blk, depth_blk)

    @pl.when(side == 0)
    def _():
        for h in range(heads_blk):
            lhs[:, pl.ds(base + h * dim, dim)] = c_ref[h]

    left = lhs[:, pl.ds(base, depth_blk)]

    def product(first):
        for t in range(wide // 256):
            cols = slice(t * 256, (t + 1) * 256)
            prod = jnp.dot(left, w_ref[:, cols], preferred_element_type=F32)
            acc[:, cols] = prod if first else acc[:, cols] + prod

    @pl.when(step == 0)
    def _():
        product(True)

    @pl.when(step > 0)
    def _():
        product(False)

    @pl.when(step == steps - 1)
    def _():
        a_copy(side).wait()
        a_buf[side] = (a_buf[side].astype(F32) * ALPHA + (acc[...] + b_ref[...].astype(F32).reshape(1, -1))).astype(BF16)
        o_copy(side).start()

    @pl.when(turn == turns - 1)
    def _():
        wait(out_copies(turn))
        wait([o_copy(0), o_copy(1)])


def dense(context, w_dense, bias, normed, kv, half_out):
    heads, tokens, dim = context.shape
    depth, width = w_dense.shape
    kinds, rows, seq, _ = kv.shape
    half_tok = tokens // 2
    steps = rows // 2
    any_spec = pl.BlockSpec(memory_space=pl.ANY)
    wide = width // 2
    dma = pltpu.SemaphoreType.DMA
    return pl.pallas_call(
        dense_kernel,
        grid=(2, steps),
        in_specs=[
            pl.BlockSpec((heads // steps, half_tok, dim), lambda i, k: (lax.select(i == 0, k, steps - 1), 1, 0)),
            pl.BlockSpec((depth // steps, wide), lambda i, k: (k, i)),
            pl.BlockSpec((wide,), lambda i, k: (i,)),
            any_spec,
            any_spec,
            any_spec,
        ],
        out_specs=[any_spec] * 3,
        out_shape=[
            jax.ShapeDtypeStruct((tokens, width), BF16),
            jax.ShapeDtypeStruct((rows, seq, dim), BF16),
            jax.ShapeDtypeStruct((rows, seq, dim), BF16),
        ],
        scratch_shapes=[
            pltpu.VMEM((half_tok, depth), BF16),
            pltpu.VMEM((half_tok, wide), F32),
            pltpu.VMEM((2, half_tok, wide), BF16),
            pltpu.VMEM((2, 2, seq, dim), BF16),
            pltpu.VMEM((2, half_tok // (2 * steps), width), BF16),
            dma((2,)), dma((2, 2)), dma((3, 2)), dma((2,)),
        ],
        compiler_params=pltpu.CompilerParams(vmem_limit_bytes=VMEM_CAP),
        cost_estimate=pl.CostEstimate(flops=tokens * depth * width, bytes_accessed=2 * depth * width, transcendentals=0),
        name="dense",
    )(context, w_dense, bias, normed, kv, half_out)


def solution(mesh):
    seq_spec = P('dp', 'sp', None)
    row_spec = P('dp', 'sp')
    head_spec = P('dp', None, 'sp', None)
    rep = P()
    devices = mesh.shape['sp']

    def local_block(hidden, pos_ids, block_ids, ctx_len, ln_gamma, ln_beta, w_qkv, b_qkv, w_dense, b_dense):
        rows, chunk, width = hidden.shape
        depth, heads, kinds, dim = w_qkv.shape
        seq = chunk * devices
        tokens = rows * chunk
        w_rows = jnp.transpose(w_qkv, (0, 2, 1, 3))
        bias = jnp.transpose(b_qkv, (1, 0, 2))
        normed, _, recv, _, context, half_out = exchange(
            devices, ctx_len, hidden.reshape(tokens, width), ln_gamma, ln_beta, w_rows, bias, pos_ids, block_ids, rotary_freq(dim), w_dense, b_dense, rows, chunk)
        out, keys, values = dense(context, w_dense, b_dense, normed, recv.reshape(kinds, rows, seq, dim), half_out)
        return out.reshape(rows, chunk, width), keys.reshape(rows, seq, 1, dim), values.reshape(rows, seq, 1, dim)

    return jax.shard_map(local_block, mesh=mesh, in_specs=(seq_spec, row_spec, row_spec, P('dp'), rep, rep, rep, rep, rep, rep), out_specs=(seq_spec, head_spec, head_spec), check_vma=False)
```

```python
import functools
import math

import jax
import jax.numpy as jnp
from jax import lax
from jax.experimental import pallas as pl
from jax.experimental.pallas import tpu as pltpu
from jax.sharding import PartitionSpec as P

ALPHA = math.sqrt(56.0)
ROPE_BASE = 10000.0
LN_EPS = 1e-5
CTX_LOW = 1024
CTX_HIGH = 3072
F32 = jnp.float32
BF16 = jnp.bfloat16
VMEM_CAP = 60000 * 1024
MESH_ID = pl.DeviceIdType.MESH


SHIFT_PAIRS = (((1, 0), (3, 2)), ((1, 1), (3, 3)), ((3, 0), (1, 2)), ((0, 1), (2, 3)),
               ((1, 3), (3, 1)), ((0, 3), (2, 1)), ((2, 0), (0, 2)), ((2, 2), (0, 0)))


def shift_codes(side):
    if side == 4:
        pairs = SHIFT_PAIRS
    else:
        shifts = [(i % side, i // side) for i in range(side * side)]
        pairs = tuple(zip(shifts[0::2], shifts[1::2]))
    return len(pairs), [sum(pair[k // 2][k % 2] * side ** u for u, pair in enumerate(pairs)) for k in range(4)]


def rotary_freq(dim):
    half = dim // 2
    lane = lax.rem(lax.broadcasted_iota(jnp.int32, (1, dim), 1), half // 2)
    return ROPE_BASE ** (-(2 * lane).astype(F32) / half)


def split_sizes(rows, heads):
    return rows // 2, heads // 2


def exchange_kernel(cfg, ctx_ref, x_ref, g_ref, be_ref, w_ref, bias_ref, pos_ref, blk_ref, freq_ref, wd_ref, bd_ref,
                    a_out, snd, rc, c_snd, c_rc, half_out,
                    xb, ab, wbuf, wb0, wb1, acc, sb, qb, kb, vb, cb, vt, s_buf, m_buf, a_buf, l_s, acc_s, cos_ref, sin_ref, bd_row,
                    x_sem, a_sem, w_sem, l_sem, o_sem, snd_sem, rcv_sem, row_sem, c_sem, cs_sem, cr_sem, lhs_sem):
    n, depth, k_tile, q_blk, k_blk, low, high = cfg
    _, heads, rows, chunk, dim = snd.shape
    half_rows, group = split_sizes(rows, heads)
    half_tok = half_rows * chunk
    seq = n * chunk
    pieces = 12
    chunks = depth // k_tile
    total = pieces * chunks
    me = lax.axis_index('sp')

    barrier = pltpu.get_barrier_semaphore()

    def greet(i, c):
        pl.semaphore_signal(barrier, inc=1, device_id={'sp': lax.rem(me + i, n)}, device_id_type=MESH_ID)
        return c

    def piece_of(p):
        hf = p // 6
        kind = 2 - lax.rem(p, 6) // 2
        hh = lax.rem(p, 2)
        return hf, kind, hh

    def w_copy(s):
        _, kind, hh = piece_of(s // chunks)
        c = lax.rem(s, chunks)
        slot = lax.rem(s, 4)
        return pltpu.make_async_copy(
            w_ref.at[pl.ds(pl.multiple_of(c * k_tile, k_tile), k_tile), kind, pl.ds(pl.multiple_of(hh * group, group), group)],
            wbuf.at[slot], w_sem.at[slot])

    def x_copy(hf):
        return pltpu.make_async_copy(x_ref.at[pl.ds(pl.multiple_of(hf * half_tok, half_tok), half_tok)], xb, x_sem)

    def a_copy(hf):
        return pltpu.make_async_copy(ab, a_out.at[pl.ds(pl.multiple_of(hf * half_tok, half_tok), half_tok)], a_sem)

    def l_copy(p):
        hf, kind, hh = piece_of(p)
        slot = lax.rem(p, 2)
        return pltpu.make_async_copy(
            sb.at[slot],
            snd.at[kind, pl.ds(pl.multiple_of(hh * group, group), group), pl.ds(hf * half_rows, half_rows)],
            l_sem.at[slot])

    def own_copy(p):
        hf, kind, hh = piece_of(p)
        slot = lax.rem(p, 2)
        return pltpu.make_async_copy(
            sb.at[slot, lax.rem(me, group)],
            rc.at[kind, pl.ds(hf * half_rows, half_rows), me],
            o_sem.at[slot])

    def mine(p):
        return piece_of(p)[2] == me // group

    def send(kind, head, pair, group_id):
        at = pl.ds(2 * pair, 2)
        pltpu.make_async_remote_copy(
            src_ref=snd.at[kind, head, at], dst_ref=rc.at[kind, at, me],
            send_sem=snd_sem.at[group_id], recv_sem=rcv_sem.at[group_id],
            device_id={'sp': head}, device_id_type=MESH_ID).start()

    def c_send(dest, first, count, sem):
        at = pl.ds(pl.multiple_of(first * chunk, chunk), count * chunk)
        return pltpu.make_async_remote_copy(
            src_ref=c_snd.at[dest, at], dst_ref=c_rc.at[me, at],
            send_sem=cs_sem, recv_sem=cr_sem.at[sem], device_id={'sp': dest}, device_id_type=MESH_ID)

    def layer_norm(hf):
        x_copy(hf).wait()
        sub = 16
        tile = min(64, half_tok)
        lanes = [slice(c * 128, (c + 1) * 128) for c in range(depth // 128)]

        def body(i, c):
            ats = [pl.ds(pl.multiple_of(i * tile + u * sub, sub), sub) for u in range(tile // sub)]
            means, scales = [], []
            for at in ats:
                total = sum(xb[at, cols].astype(F32) for cols in lanes)
                means.append(jnp.sum(total, axis=-1, keepdims=True) * (1.0 / depth))
            for at, mean in zip(ats, means):
                total = sum(jnp.square(xb[at, cols].astype(F32) - mean) for cols in lanes)
                scales.append(lax.rsqrt(jnp.sum(total, axis=-1, keepdims=True) * (1.0 / depth) + LN_EPS))
            for cols in lanes:
                gain = g_ref[cols].astype(F32).reshape(1, 128)
                shift = be_ref[cols].astype(F32).reshape(1, 128)
                for at, mean, scale in zip(ats, means, scales):
                    ab[at, cols] = ((xb[at, cols].astype(F32) - mean) * scale * gain + shift).astype(BF16)
            return c

        lax.fori_loop(0, half_tok // tile, body, 0)

    def tables():
        lane = lax.broadcasted_iota(jnp.int32, (1, dim), 1)

        def body(r, c):
            at = pl.ds(pl.multiple_of(r * chunk, chunk), chunk)
            pos = jnp.broadcast_to(pos_ref[pl.ds(r, 1), :].astype(F32), (dim, chunk)).T
            blk = jnp.broadcast_to(blk_ref[pl.ds(r, 1), :].astype(F32), (dim, chunk)).T
            ang = jnp.where(lane < dim // 2, pos, blk) * freq_ref[...]
            sin = jnp.sin(ang)
            cos_ref[at, :] = jnp.cos(ang)
            sin_ref[at, :] = jnp.where(lax.rem(lane, dim // 2) < dim // 4, -sin, sin)
            return c

        lax.fori_loop(0, rows, body, 0)

    def relayout(s, wb):
        slot = lax.rem(s, 4)
        sub = min(64, k_tile)
        for part in range(k_tile // sub):
            lo = part * sub
            tile = jnp.swapaxes(wbuf[slot, lo:lo + sub], 0, 1)
            for head in range(group):
                wb[lo:lo + sub, head * dim:(head + 1) * dim] = tile[head]

    def multiply(c, wb, count=half_tok):
        lhs = ab[:count, pl.ds(pl.multiple_of(c * k_tile, k_tile), k_tile)]
        wide = min(256, group * dim)
        for t in range(group * dim // wide):
            cols = slice(t * wide, (t + 1) * wide)
            acc[:count, cols] += jnp.dot(lhs, wb[:, cols], preferred_element_type=F32)

    def epilogue(p):
        hf, kind, hh = piece_of(p)
        slot = lax.rem(p, 2)
        toks = pl.ds(pl.multiple_of(hf * half_tok, half_tok), half_tok)
        turn = min(4, group)
        bias = bias_ref[kind, pl.ds(pl.multiple_of(hh * group, group), group), :].astype(F32)
        fill = jnp.zeros((half_tok, dim), F32)
        lane = lax.broadcasted_iota(jnp.int32, (1, dim), 1)
        first = lax.rem(lane, dim // 2) < dim // 4

        def biased(h, row):
            cols = pl.ds(pl.multiple_of(h * dim, dim), dim)
            x = (acc[:, cols] + row).astype(BF16)
            acc[:, cols] = fill
            return x

        def rows_of(t):
            return [bias[t * turn + u:t * turn + u + 1, :] for u in range(turn)]

        for t in range(group // turn):
            @pl.when(kind < 2)
            def _():
                for u, row in enumerate(rows_of(t)):
                    h = t * turn + u
                    x = biased(h, row).astype(F32)
                    pair = jnp.where(first, pltpu.roll(x, dim - dim // 4, 1), pltpu.roll(x, dim // 4, 1))
                    x = (x * cos_ref[toks, :] + pair * sin_ref[toks, :]).astype(BF16)
                    sb[slot, h] = x.reshape(half_rows, chunk, dim)

            @pl.when(kind == 2)
            def _():
                for u, row in enumerate(rows_of(t)):
                    h = t * turn + u
                    sb[slot, h] = biased(h, row).reshape(half_rows, chunk, dim)

    side = math.isqrt(n // 2)
    pair_count, codes = shift_codes(side)

    def for_peers(act):
        core = lax.rem(me, 2)

        def sweep(flip, c):
            def one(u, rest):
                digit = [lax.rem(code, side) for code in rest]
                for r in range(2):
                    second = lax.rem(r + core, 2)
                    dx = digit[0] + second * (digit[2] - digit[0])
                    dy = digit[1] + second * (digit[3] - digit[1])
                    y = lax.rem(me // (2 * side) + dy, side)
                    x = lax.rem(me // 2 + dx, side)
                    peer = (y * side + x) * 2 + lax.rem(me + flip, 2)

                    @pl.when(peer != me)
                    def _():
                        act(peer)

                return tuple(code // side for code in rest)

            lax.fori_loop(0, pair_count, one, tuple(jnp.int32(code) for code in codes))
            return c

        lax.fori_loop(0, 2, sweep, 0)

    def landed(p):
        l_copy(p).wait()

        @pl.when(mine(p))
        def _():
            own_copy(p).wait()

    def flush(p, count):
        hf, kind, hh = piece_of(p)
        landed(p)
        if count == 2:
            landed(p - 1)

        def out(pair, group_id):
            def act(head):
                if count == 2:
                    send(kind, head, pair, group_id)
                else:
                    @pl.when(head // group == hh)
                    def _():
                        send(kind, head, pair, group_id)

            for_peers(act)

        out(2 * hf, hf)

        @pl.when(hf == 0)
        def _():
            out(1, 0)

    def flush_rows():
        def one(i, c):
            for_peers(lambda head: send(2 - i, head, rows // 2 - 1, 2))
            return c

        lax.fori_loop(0, 3, one, 0)

    x_copy(0).start()
    for s in range(3):
        w_copy(s).start()
    lax.fori_loop(1, n, greet, 0)
    acc[...] = jnp.zeros_like(acc)
    w_copy(0).wait()
    relayout(0, wb0)
    with jax.named_scope('ln0'):
        layer_norm(0)
    with jax.named_scope('barrier_wait'):
        pl.semaphore_wait(barrier, n - 1)

    def project(p, c):
        @pl.when(p == 6)
        def _():
            with jax.named_scope('ln1'):
                a_copy(0).wait()
                layer_norm(1)
                a_copy(1).start()

        @pl.when(p == 1)
        def _():
            a_copy(0).start()
            x_copy(1).start()
            bd_row[...] = bd_ref[...].astype(F32).reshape(1, -1)
            with jax.named_scope('tables'):
                tables()

        def steps(i, c):
            s = p * chunks + 2 * i
            w_copy(s + 1).wait()

            @pl.when(s + 2 < total)
            def _():
                w_copy(s + 2).wait()

            @pl.when(s + 3 < total)
            def _():
                w_copy(s + 3).start()

            @pl.when(s + 4 < total)
            def _():
                w_copy(s + 4).start()

            @pl.when((i == 1) & (p == 2))
            def _():
                with jax.named_scope('flush'):
                    flush(p - 1, 1)

            @pl.when((i == 1) & (p > 2) & (lax.rem(p, 2) == 0))
            def _():
                with jax.named_scope('flush'):
                    flush(p - 1, 2)

            relayout(s + 1, wb1)
            multiply(2 * i, wb0)
            relayout(s + 2, wb0)
            multiply(2 * i + 1, wb1)
            return c

        lax.fori_loop(0, chunks // 2, steps, 0)
        with jax.named_scope('epi'):
            epilogue(p)
        l_copy(p).start()

        @pl.when(mine(p))
        def _():
            own_copy(p).start()

        @pl.when(p == 0)
        def _():
            with jax.named_scope('flush0'):
                flush(p, 1)

        return c

    lax.fori_loop(0, pieces, project, 0)
    with jax.named_scope('lastflush'):
        flush(pieces - 1, 2)
        flush_rows()
    a_copy(1).wait()

    coef = math.log2(math.e) / math.sqrt(dim)
    per = q_blk // chunk
    kn = k_blk // chunk
    ratio = q_blk // k_blk

    def row_copies(b):
        slot = lax.rem(b, 2)
        return [pltpu.make_async_copy(rc.at[kind, b], buf.at[slot], row_sem.at[kind, slot])
                for kind, buf in ((0, qb), (1, kb), (2, vb))]

    def ctx_copies(b):
        slot = lax.rem(b, 2)
        at = pl.ds(pl.multiple_of(b * chunk, chunk), chunk)
        return [pltpu.make_async_copy(cb.at[slot], c_snd.at[:, at], c_sem.at[0, slot]),
                pltpu.make_async_copy(cb.at[slot, me], c_rc.at[me, at], c_sem.at[1, slot])]

    def attend_row(b):
        slot = lax.rem(b, 2)
        ctx = ctx_ref[b]
        step_v = min(512, seq)
        for c in range(seq // step_v):
            m = step_v // chunk
            vt[:, c * step_v:(c + 1) * step_v] = vb[slot, c * m:(c + 1) * m].reshape(step_v, dim).T
        blocks = seq // q_blk

        def scores(qi, j, s_slot, masked, prev):
            k_rows = kb[slot, pl.ds(j * kn, kn)].reshape(k_blk, dim)
            q_rows = qb[slot, pl.ds(qi * per, per)].reshape(q_blk, dim)
            s = lax.dot_general(k_rows, q_rows, (((1,), (1,)), ((), ())), preferred_element_type=F32)
            if masked:
                kpos = j * k_blk + lax.broadcasted_iota(jnp.int32, s.shape, 0)
                lim = jnp.maximum(ctx, qi * q_blk + 1 + lax.broadcasted_iota(jnp.int32, (1, q_blk), 1))
                s = jnp.where(kpos < lim, s, -jnp.inf)
            s_buf[s_slot] = s
            top = jnp.max(s, axis=0, keepdims=True) * coef
            if prev is None:
                m_buf[s_slot] = top
                a_buf[s_slot] = jnp.zeros_like(top)
            else:
                m_old = m_buf[prev]
                m_new = jnp.maximum(m_old, top)
                m_buf[s_slot] = m_new
                a_buf[s_slot] = jnp.exp2(m_old - m_new)

        def values(j, s_slot):
            v_cols = vt[:, pl.ds(pl.multiple_of(j * k_blk, k_blk), k_blk)]
            scale = a_buf[s_slot]
            p = jnp.exp2(s_buf[s_slot] * coef - m_buf[s_slot])
            l_s[...] = l_s[...] * scale + jnp.sum(p.reshape(k_blk // 8, 8, q_blk), axis=0)
            acc_s[...] = acc_s[...] * scale + jnp.dot(v_cols, p.astype(BF16), preferred_element_type=F32)

        def q_loop(qi, _):
            q0 = qi * q_blk
            l_s[...] = jnp.zeros_like(l_s)
            acc_s[...] = jnp.zeros_like(acc_s)

            def pair(i, masked):
                scores(qi, 2 * i + 1, 1, masked, 0)
                values(2 * i, 0)
                scores(qi, 2 * i + 2, 0, masked, 1)
                values(2 * i + 1, 1)

            last = (jnp.maximum(high, q0 + q_blk) + 2 * k_blk - 1) // (2 * k_blk) - 1
            full = jnp.minimum((jnp.maximum(low, q0) // k_blk - 1) // 2, last)
            lax.fori_loop(0, full, lambda i, c: (pair(i, False), c)[1], 0)
            lax.fori_loop(full, last, lambda i, c: (pair(i, True), c)[1], 0)
            scores(qi, 2 * last + 1, 1, True, 0)
            values(2 * last, 0)
            scores(jnp.minimum(qi + 1, blocks - 1), 0, 0, False, None)
            values(2 * last + 1, 1)
            inv = 1.0 / jnp.sum(l_s[...], axis=0, keepdims=True)
            cb[slot, pl.ds(qi * per, per)] = (acc_s[...] * inv).T.astype(BF16).reshape(per, chunk, dim)
            return 0

        scores(0, 0, 0, False, None)
        lax.fori_loop(0, blocks, q_loop, 0)

    def arrived(at, group_id):
        got = rc.at[:, at, pl.ds(0, n - 1)]
        pltpu.make_async_copy(got, got, rcv_sem.at[group_id]).wait()

    def give(b, first, count, sem):
        with jax.named_scope('ctxwait'):
            for r in range(count):
                for copy in ctx_copies(b - count + 1 + r):
                    copy.wait()

        for_peers(lambda dest: c_send(dest, first, count, sem).start())

    starts = ((0, pl.ds(0, half_rows)), (half_rows, pl.ds(half_rows, 2)), (rows - 2, pl.ds(rows - 2, 2)))

    def attend(b, c):
        for group_id, (row, at) in enumerate(starts):
            @pl.when(b == row)
            def _():
                with jax.named_scope(f'arr{group_id}'):
                    arrived(at, group_id)
                for copy in row_copies(b):
                    copy.start()

        @pl.when((b < half_rows - 1) | ((b >= half_rows) & (lax.rem(b, 2) == 0)))
        def _():
            for copy in row_copies(b + 1):
                copy.start()

        with jax.named_scope('rowwait'):
            for copy in row_copies(b):
                copy.wait()
        with jax.named_scope('row'):
            attend_row(b)
        for copy in ctx_copies(b):
            copy.start()

        @pl.when((lax.rem(b, 2) == 1) & (b < half_rows))
        def _():
            give(b, b - 1, 2, 0)

        @pl.when(b == rows - 3)
        def _():
            give(b, b - 1, 2, 1)

        @pl.when(b == rows - 1)
        def _():
            give(b, b - 1, 2, 2)

        return c

    lax.fori_loop(0, rows, attend, 0)

    steps = depth // k_tile
    wide = group * dim

    def wd_copy(i, buf, slot):
        return pltpu.make_async_copy(
            wd_ref.at[pl.ds(pl.multiple_of(lax.rem(i, steps) * k_tile, k_tile), k_tile), pl.ds(pl.multiple_of(i // steps * wide, wide), wide)],
            buf, w_sem.at[slot])

    def dense_rows(first, count, sem):
        def lhs_copy(h):
            return pltpu.make_async_copy(
                c_rc.at[h, pl.ds(first, count)], ab.at[pl.ds(0, count), pl.ds(pl.multiple_of(h * dim, dim), dim)], lhs_sem)

        wd_copy(0, wb0, 0).start()
        a_back = pltpu.make_async_copy(a_out.at[pl.ds(first, count)], xb.at[pl.ds(0, count)], x_sem)
        a_back.start()
        got = c_rc.at[pl.ds(0, n - 1), pl.ds(first, count)]
        with jax.named_scope(f'cr{sem}'):
            pltpu.make_async_copy(got, got, cr_sem.at[sem]).wait()
        lax.fori_loop(0, heads, lambda h, c: (lhs_copy(h).start(), c)[1], 0)
        with jax.named_scope('lhswait'):
            lax.fori_loop(0, heads, lambda h, c: (lhs_copy(h).wait(), c)[1], 0)
            a_back.wait()

        def dense_half(t, c):
            def two(i, c):
                s = t * steps + 2 * i
                wd_copy(s + 1, wb1, 1).start()
                wd_copy(s, wb0, 0).wait()
                multiply(2 * i, wb0, count)

                @pl.when(s + 2 < 2 * steps)
                def _():
                    wd_copy(s + 2, wb0, 0).start()

                wd_copy(s + 1, wb1, 1).wait()
                multiply(2 * i + 1, wb1, count)
                return c

            lax.fori_loop(0, steps // 2, two, 0)
            for u in range(wide // 256):
                cols = pl.ds(pl.multiple_of(t * wide + u * 256, 256), 256)
                part = slice(u * 256, (u + 1) * 256)
                shift = bd_row[:, cols]
                xb[:count, cols] = (xb[:count, cols].astype(F32) * ALPHA + (acc[:count, part] + shift)).astype(BF16)
                acc[:count, part] = jnp.zeros((count, 256), F32)
            return c

        with jax.named_scope('dense'):
            lax.fori_loop(0, depth // wide, dense_half, 0)
        done = pltpu.make_async_copy(xb.at[pl.ds(0, count)], half_out.at[pl.ds(first, count)], x_sem)
        done.start()
        done.wait()

    dense_rows(0, half_tok, 0)
    dense_rows(half_tok, 2 * chunk, 1)

    for group_id, (_, at) in enumerate(starts):
        gone = snd.at[:, pl.ds(0, n - 1), at]
        with jax.named_scope(f'drainsnd{group_id}'):
            pltpu.make_async_copy(gone, gone, snd_sem.at[group_id]).wait()
    gone = c_snd.at[pl.ds(0, n - 1)]
    with jax.named_scope('draincs'):
        pltpu.make_async_copy(gone, gone, cs_sem).wait()
    got = c_rc.at[pl.ds(0, n - 1), pl.ds((rows - 2) * chunk, 2 * chunk)]
    with jax.named_scope('draincr'):
        pltpu.make_async_copy(got, got, cr_sem.at[2]).wait()


def exchange(n, ctx_len, x, gamma, beta, w_rows, bias, pos_ids, block_ids, freq, w_dense, b_dense, rows, chunk, k_tile=512, q_blk=512, k_blk=512, low=CTX_LOW, high=CTX_HIGH):
    tokens, depth = x.shape
    _, kinds, heads, dim = w_rows.shape
    half_rows, group = split_sizes(rows, heads)
    half_tok = half_rows * chunk
    seq = n * chunk
    any_spec = pl.BlockSpec(memory_space=pl.ANY)
    vmem = pl.BlockSpec(memory_space=pltpu.VMEM)
    smem = pl.BlockSpec(memory_space=pltpu.SMEM)
    dma = pltpu.SemaphoreType.DMA
    cfg = (n, depth, k_tile, q_blk, k_blk, low, high)
    return pl.pallas_call(
        functools.partial(exchange_kernel, cfg),
        in_specs=[smem, any_spec, vmem, vmem, any_spec, vmem, vmem, vmem, vmem, any_spec, vmem],
        out_specs=[any_spec] * 6,
        out_shape=[
            jax.ShapeDtypeStruct((tokens, depth), BF16),
            jax.ShapeDtypeStruct((kinds, heads, rows, chunk, dim), BF16),
            jax.ShapeDtypeStruct((kinds, rows, n, chunk, dim), BF16),
            jax.ShapeDtypeStruct((n, tokens, dim), BF16),
            jax.ShapeDtypeStruct((heads, tokens, dim), BF16),
            jax.ShapeDtypeStruct((tokens - 2 * chunk, depth), BF16),
        ],
        scratch_shapes=[
            pltpu.VMEM((half_tok, depth), BF16),
            pltpu.VMEM((half_tok, depth), BF16),
            pltpu.VMEM((4, k_tile, group, dim), BF16),
            pltpu.VMEM((k_tile, group * dim), BF16),
            pltpu.VMEM((k_tile, group * dim), BF16),
            pltpu.VMEM((half_tok, group * dim), F32),
            pltpu.VMEM((2, group, half_rows, chunk, dim), BF16),
            pltpu.VMEM((2, n, chunk, dim), BF16),
            pltpu.VMEM((2, n, chunk, dim), BF16),
            pltpu.VMEM((2, n, chunk, dim), BF16),
            pltpu.VMEM((2, n, chunk, dim), BF16),
            pltpu.VMEM((dim, seq), BF16),
            pltpu.VMEM((2, k_blk, q_blk), F32),
            pltpu.VMEM((2, 1, q_blk), F32),
            pltpu.VMEM((2, 1, q_blk), F32),
            pltpu.VMEM((8, q_blk), F32),
            pltpu.VMEM((dim, q_blk), F32),
            pltpu.VMEM((tokens, dim), F32),
            pltpu.VMEM((tokens, dim), F32),
            pltpu.VMEM((1, depth), F32),
            dma, dma, dma((4,)), dma((2,)), dma((2,)), dma((3,)), dma((3,)), dma((3, 2)), dma((2, 2)), dma, dma((3,)), dma,
        ],
        compiler_params=pltpu.CompilerParams(vmem_limit_bytes=VMEM_CAP, collective_id=0, has_side_effects=True),
        cost_estimate=pl.CostEstimate(flops=2 * tokens * depth * kinds * heads * dim, bytes_accessed=4 * depth * kinds * heads * dim, transcendentals=0),
        name="exchange",
    )(ctx_len, x, gamma, beta, w_rows, bias, pos_ids, block_ids, freq, w_dense, b_dense)


def dense_kernel(c_ref, w_ref, b_ref, a_hbm, kv_hbm, half_hbm, o_hbm, ko_hbm, vo_hbm, lhs, acc, a_buf, kv_buf, h_buf, a_sem, in_sem, out_sem, o_sem):
    heads_blk, tokens, dim = c_ref.shape
    side, step = pl.program_id(0), pl.program_id(1)
    steps = pl.num_programs(1)
    turns = 2 * steps
    turn = side * steps + step
    wide = w_ref.shape[1]
    rest = pl.ds(half_hbm.shape[0], tokens)
    share = half_hbm.shape[0] // turns

    def cols_of(i):
        return pl.ds(pl.multiple_of(i * wide, wide), wide)

    def a_copy(i):
        return pltpu.make_async_copy(a_hbm.at[rest, cols_of(i)], a_buf.at[i], a_sem.at[i])

    def o_copy(i):
        return pltpu.make_async_copy(a_buf.at[i], o_hbm.at[rest, cols_of(i)], o_sem.at[i])

    def part(i):
        return pl.ds(pl.multiple_of(i * share, share), share)

    def in_copies(i):
        slot = lax.rem(i, 2)
        return [pltpu.make_async_copy(kv_hbm.at[pl.ds(1, 2), i], kv_buf.at[slot], in_sem.at[0, slot]),
                pltpu.make_async_copy(half_hbm.at[part(i)], h_buf.at[slot], in_sem.at[1, slot])]

    def out_copies(i):
        slot = lax.rem(i, 2)
        return [pltpu.make_async_copy(kv_buf.at[slot, 0], ko_hbm.at[i], out_sem.at[0, slot]),
                pltpu.make_async_copy(kv_buf.at[slot, 1], vo_hbm.at[i], out_sem.at[1, slot]),
                pltpu.make_async_copy(h_buf.at[slot], o_hbm.at[part(i)], out_sem.at[2, slot])]

    def start(copies):
        for copy in copies:
            copy.start()

    def wait(copies):
        for copy in copies:
            copy.wait()

    @pl.when(turn == 0)
    def _():
        start(in_copies(0))
        start([a_copy(0), a_copy(1)])

    wait(in_copies(turn))
    start(out_copies(turn))

    @pl.when(turn > 0)
    def _():
        wait(out_copies(turn - 1))

    @pl.when(turn + 1 < turns)
    def _():
        start(in_copies(turn + 1))

    depth_blk = heads_blk * dim
    base = pl.multiple_of(step * depth_blk, depth_blk)

    @pl.when(side == 0)
    def _():
        for h in range(heads_blk):
            lhs[:, pl.ds(base + h * dim, dim)] = c_ref[h]

    left = lhs[:, pl.ds(base, depth_blk)]

    def product(first):
        for t in range(wide // 256):
            cols = slice(t * 256, (t + 1) * 256)
            prod = jnp.dot(left, w_ref[:, cols], preferred_element_type=F32)
            acc[:, cols] = prod if first else acc[:, cols] + prod

    @pl.when(step == 0)
    def _():
        product(True)

    @pl.when(step > 0)
    def _():
        product(False)

    @pl.when(step == steps - 1)
    def _():
        a_copy(side).wait()
        a_buf[side] = (a_buf[side].astype(F32) * ALPHA + (acc[...] + b_ref[...].astype(F32).reshape(1, -1))).astype(BF16)
        o_copy(side).start()

    @pl.when(turn == turns - 1)
    def _():
        wait(out_copies(turn))
        wait([o_copy(0), o_copy(1)])


def dense(context, w_dense, bias, normed, kv, half_out):
    heads, tokens, dim = context.shape
    depth, width = w_dense.shape
    kinds, rows, seq, _ = kv.shape
    last_tok = tokens - half_out.shape[0]
    steps = rows // 2
    any_spec = pl.BlockSpec(memory_space=pl.ANY)
    wide = width // 2
    dma = pltpu.SemaphoreType.DMA
    return pl.pallas_call(
        dense_kernel,
        grid=(2, steps),
        in_specs=[
            pl.BlockSpec((heads // steps, last_tok, dim), lambda i, k: (lax.select(i == 0, k, steps - 1), tokens // last_tok - 1, 0)),
            pl.BlockSpec((depth // steps, wide), lambda i, k: (k, i)),
            pl.BlockSpec((wide,), lambda i, k: (i,)),
            any_spec,
            any_spec,
            any_spec,
        ],
        out_specs=[any_spec] * 3,
        out_shape=[
            jax.ShapeDtypeStruct((tokens, width), BF16),
            jax.ShapeDtypeStruct((rows, seq, dim), BF16),
            jax.ShapeDtypeStruct((rows, seq, dim), BF16),
        ],
        scratch_shapes=[
            pltpu.VMEM((last_tok, depth), BF16),
            pltpu.VMEM((last_tok, wide), F32),
            pltpu.VMEM((2, last_tok, wide), BF16),
            pltpu.VMEM((2, 2, seq, dim), BF16),
            pltpu.VMEM((2, half_out.shape[0] // (2 * steps), width), BF16),
            dma((2,)), dma((2, 2)), dma((3, 2)), dma((2,)),
        ],
        compiler_params=pltpu.CompilerParams(vmem_limit_bytes=VMEM_CAP),
        cost_estimate=pl.CostEstimate(flops=2 * last_tok * depth * width, bytes_accessed=2 * depth * width, transcendentals=0),
        name="dense",
    )(context, w_dense, bias, normed, kv, half_out)


def solution(mesh):
    seq_spec = P('dp', 'sp', None)
    row_spec = P('dp', 'sp')
    head_spec = P('dp', None, 'sp', None)
    rep = P()
    devices = mesh.shape['sp']

    def local_block(hidden, pos_ids, block_ids, ctx_len, ln_gamma, ln_beta, w_qkv, b_qkv, w_dense, b_dense):
        rows, chunk, width = hidden.shape
        depth, heads, kinds, dim = w_qkv.shape
        seq = chunk * devices
        tokens = rows * chunk
        w_rows = jnp.transpose(w_qkv, (0, 2, 1, 3))
        bias = jnp.transpose(b_qkv, (1, 0, 2))
        normed, _, recv, _, context, half_out = exchange(
            devices, ctx_len, hidden.reshape(tokens, width), ln_gamma, ln_beta, w_rows, bias, pos_ids, block_ids, rotary_freq(dim), w_dense, b_dense, rows, chunk)
        out, keys, values = dense(context, w_dense, b_dense, normed, recv.reshape(kinds, rows, seq, dim), half_out)
        return out.reshape(rows, chunk, width), keys.reshape(rows, seq, 1, dim), values.reshape(rows, seq, 1, dim)

    return jax.shard_map(local_block, mesh=mesh, in_specs=(seq_spec, row_spec, row_spec, P('dp'), rep, rep, rep, rep, rep, rep), out_specs=(seq_spec, head_spec, head_spec), check_vma=False)
```

```python
import functools
import math

import jax
import jax.numpy as jnp
from jax import lax
from jax.experimental import pallas as pl
from jax.experimental.pallas import tpu as pltpu
from jax.sharding import PartitionSpec as P

ALPHA = math.sqrt(56.0)
ROPE_BASE = 10000.0
LN_EPS = 1e-5
CTX_LOW = 1024
CTX_HIGH = 3072
F32 = jnp.float32
BF16 = jnp.bfloat16
VMEM_CAP = 60000 * 1024
MESH_ID = pl.DeviceIdType.MESH


SHIFT_PAIRS = (((1, 0), (3, 2)), ((1, 1), (3, 3)), ((3, 0), (1, 2)), ((0, 1), (2, 3)),
               ((1, 3), (3, 1)), ((0, 3), (2, 1)), ((2, 0), (0, 2)), ((2, 2), (0, 0)))


def shift_codes(side):
    if side == 4:
        pairs = SHIFT_PAIRS
    else:
        shifts = [(i % side, i // side) for i in range(side * side)]
        pairs = tuple(zip(shifts[0::2], shifts[1::2]))
    return len(pairs), [sum(pair[k // 2][k % 2] * side ** u for u, pair in enumerate(pairs)) for k in range(4)]


def rotary_freq(dim):
    half = dim // 2
    lane = lax.rem(lax.broadcasted_iota(jnp.int32, (1, dim), 1), half // 2)
    return ROPE_BASE ** (-(2 * lane).astype(F32) / half)


def split_sizes(rows, heads):
    return rows // 2, heads // 2


def exchange_kernel(cfg, ctx_ref, x_ref, g_ref, be_ref, w_ref, bias_ref, pos_ref, blk_ref, freq_ref, wd_ref, bd_ref,
                    a_out, snd, rc, c_snd, c_rc, half_out,
                    xb, ab, wbuf, wb0, wb1, acc, sb, qb, kb, vb, cb, vt, s_buf, m_buf, a_buf, l_s, acc_s, cos_ref, sin_ref, bd_row,
                    x_sem, a_sem, w_sem, l_sem, o_sem, snd_sem, rcv_sem, row_sem, c_sem, cs_sem, cr_sem, lhs_sem):
    n, depth, k_tile, q_blk, k_blk, low, high = cfg
    _, heads, rows, chunk, dim = snd.shape
    half_rows, group = split_sizes(rows, heads)
    half_tok = half_rows * chunk
    seq = n * chunk
    pieces = 12
    chunks = depth // k_tile
    total = pieces * chunks
    me = lax.axis_index('sp')

    barrier = pltpu.get_barrier_semaphore()

    def greet(i, c):
        pl.semaphore_signal(barrier, inc=1, device_id={'sp': lax.rem(me + i, n)}, device_id_type=MESH_ID)
        return c

    def piece_of(p):
        hf = p // 6
        kind = 2 - lax.rem(p, 6) // 2
        hh = lax.rem(p, 2)
        return hf, kind, hh

    def w_copy(s):
        _, kind, hh = piece_of(s // chunks)
        c = lax.rem(s, chunks)
        slot = lax.rem(s, 4)
        return pltpu.make_async_copy(
            w_ref.at[pl.ds(pl.multiple_of(c * k_tile, k_tile), k_tile), kind, pl.ds(pl.multiple_of(hh * group, group), group)],
            wbuf.at[slot], w_sem.at[slot])

    def x_copy(hf):
        return pltpu.make_async_copy(x_ref.at[pl.ds(pl.multiple_of(hf * half_tok, half_tok), half_tok)], xb, x_sem)

    def a_copy(hf):
        return pltpu.make_async_copy(ab, a_out.at[pl.ds(pl.multiple_of(hf * half_tok, half_tok), half_tok)], a_sem)

    def l_copy(p):
        hf, kind, hh = piece_of(p)
        slot = lax.rem(p, 2)
        return pltpu.make_async_copy(
            sb.at[slot],
            snd.at[kind, pl.ds(pl.multiple_of(hh * group, group), group), pl.ds(hf * half_rows, half_rows)],
            l_sem.at[slot])

    def own_copy(p):
        hf, kind, hh = piece_of(p)
        slot = lax.rem(p, 2)
        return pltpu.make_async_copy(
            sb.at[slot, lax.rem(me, group)],
            rc.at[kind, pl.ds(hf * half_rows, half_rows), me],
            o_sem.at[slot])

    def mine(p):
        return piece_of(p)[2] == me // group

    def send(kind, head, pair, group_id):
        at = pl.ds(2 * pair, 2)
        pltpu.make_async_remote_copy(
            src_ref=snd.at[kind, head, at], dst_ref=rc.at[kind, at, me],
            send_sem=snd_sem.at[group_id], recv_sem=rcv_sem.at[group_id],
            device_id={'sp': head}, device_id_type=MESH_ID).start()

    def c_send(dest, first, count, sem):
        at = pl.ds(pl.multiple_of(first * chunk, chunk), count * chunk)
        return pltpu.make_async_remote_copy(
            src_ref=c_snd.at[dest, at], dst_ref=c_rc.at[me, at],
            send_sem=cs_sem, recv_sem=cr_sem.at[sem], device_id={'sp': dest}, device_id_type=MESH_ID)

    def layer_norm(hf):
        x_copy(hf).wait()
        sub = 16
        tile = min(64, half_tok)
        lanes = [slice(c * 128, (c + 1) * 128) for c in range(depth // 128)]

        def body(i, c):
            ats = [pl.ds(pl.multiple_of(i * tile + u * sub, sub), sub) for u in range(tile // sub)]
            means, scales = [], []
            for at in ats:
                total = sum(xb[at, cols].astype(F32) for cols in lanes)
                means.append(jnp.sum(total, axis=-1, keepdims=True) * (1.0 / depth))
            for at, mean in zip(ats, means):
                total = sum(jnp.square(xb[at, cols].astype(F32) - mean) for cols in lanes)
                scales.append(lax.rsqrt(jnp.sum(total, axis=-1, keepdims=True) * (1.0 / depth) + LN_EPS))
            for cols in lanes:
                gain = g_ref[cols].astype(F32).reshape(1, 128)
                shift = be_ref[cols].astype(F32).reshape(1, 128)
                for at, mean, scale in zip(ats, means, scales):
                    ab[at, cols] = ((xb[at, cols].astype(F32) - mean) * scale * gain + shift).astype(BF16)
            return c

        lax.fori_loop(0, half_tok // tile, body, 0)

    def tables():
        lane = lax.broadcasted_iota(jnp.int32, (1, dim), 1)

        def body(r, c):
            at = pl.ds(pl.multiple_of(r * chunk, chunk), chunk)
            pos = jnp.broadcast_to(pos_ref[pl.ds(r, 1), :].astype(F32), (dim, chunk)).T
            blk = jnp.broadcast_to(blk_ref[pl.ds(r, 1), :].astype(F32), (dim, chunk)).T
            ang = jnp.where(lane < dim // 2, pos, blk) * freq_ref[...]
            sin = jnp.sin(ang)
            cos_ref[at, :] = jnp.cos(ang)
            sin_ref[at, :] = jnp.where(lax.rem(lane, dim // 2) < dim // 4, -sin, sin)
            return c

        lax.fori_loop(0, rows, body, 0)

    def relayout(s, wb):
        slot = lax.rem(s, 4)
        sub = min(64, k_tile)
        for part in range(k_tile // sub):
            lo = part * sub
            tile = jnp.swapaxes(wbuf[slot, lo:lo + sub], 0, 1)
            for head in range(group):
                wb[lo:lo + sub, head * dim:(head + 1) * dim] = tile[head]

    def multiply(c, wb, count=half_tok):
        lhs = ab[:count, pl.ds(pl.multiple_of(c * k_tile, k_tile), k_tile)]
        wide = min(256, group * dim)
        for t in range(group * dim // wide):
            cols = slice(t * wide, (t + 1) * wide)
            acc[:count, cols] += jnp.dot(lhs, wb[:, cols], preferred_element_type=F32)

    def epilogue(p):
        hf, kind, hh = piece_of(p)
        slot = lax.rem(p, 2)
        toks = pl.ds(pl.multiple_of(hf * half_tok, half_tok), half_tok)
        turn = min(4, group)
        bias = bias_ref[kind, pl.ds(pl.multiple_of(hh * group, group), group), :].astype(F32)
        fill = jnp.zeros((half_tok, dim), F32)
        lane = lax.broadcasted_iota(jnp.int32, (1, dim), 1)
        first = lax.rem(lane, dim // 2) < dim // 4

        def biased(h, row):
            cols = pl.ds(pl.multiple_of(h * dim, dim), dim)
            x = (acc[:, cols] + row).astype(BF16)
            acc[:, cols] = fill
            return x

        def rows_of(t):
            return [bias[t * turn + u:t * turn + u + 1, :] for u in range(turn)]

        for t in range(group // turn):
            @pl.when(kind < 2)
            def _():
                for u, row in enumerate(rows_of(t)):
                    h = t * turn + u
                    x = biased(h, row).astype(F32)
                    pair = jnp.where(first, pltpu.roll(x, dim - dim // 4, 1), pltpu.roll(x, dim // 4, 1))
                    x = (x * cos_ref[toks, :] + pair * sin_ref[toks, :]).astype(BF16)
                    sb[slot, h] = x.reshape(half_rows, chunk, dim)

            @pl.when(kind == 2)
            def _():
                for u, row in enumerate(rows_of(t)):
                    h = t * turn + u
                    sb[slot, h] = biased(h, row).reshape(half_rows, chunk, dim)

    side = math.isqrt(n // 2)
    pair_count, codes = shift_codes(side)

    def for_peers(act):
        core = lax.rem(me, 2)

        def sweep(flip, c):
            def one(u, rest):
                digit = [lax.rem(code, side) for code in rest]
                for r in range(2):
                    second = lax.rem(r + core, 2)
                    dx = digit[0] + second * (digit[2] - digit[0])
                    dy = digit[1] + second * (digit[3] - digit[1])
                    y = lax.rem(me // (2 * side) + dy, side)
                    x = lax.rem(me // 2 + dx, side)
                    peer = (y * side + x) * 2 + lax.rem(me + flip, 2)

                    @pl.when(peer != me)
                    def _():
                        act(peer)

                return tuple(code // side for code in rest)

            lax.fori_loop(0, pair_count, one, tuple(jnp.int32(code) for code in codes))
            return c

        lax.fori_loop(0, 2, sweep, 0)

    def landed(p):
        l_copy(p).wait()

        @pl.when(mine(p))
        def _():
            own_copy(p).wait()

    def flush(p, count):
        hf, kind, hh = piece_of(p)
        landed(p)
        if count == 2:
            landed(p - 1)

        def out(pair, group_id):
            def act(head):
                if count == 2:
                    send(kind, head, pair, group_id)
                else:
                    @pl.when(head // group == hh)
                    def _():
                        send(kind, head, pair, group_id)

            for_peers(act)

        out(2 * hf, hf)

        @pl.when(hf == 0)
        def _():
            out(1, 0)

    def flush_rows():
        def one(i, c):
            for_peers(lambda head: send(2 - i, head, rows // 2 - 1, 2))
            return c

        lax.fori_loop(0, 3, one, 0)

    x_copy(0).start()
    for s in range(3):
        w_copy(s).start()
    lax.fori_loop(1, n, greet, 0)
    acc[...] = jnp.zeros_like(acc)
    w_copy(0).wait()
    relayout(0, wb0)
    with jax.named_scope('ln0'):
        layer_norm(0)
    with jax.named_scope('barrier_wait'):
        pl.semaphore_wait(barrier, n - 1)

    def project(p, c):
        @pl.when(p == 6)
        def _():
            with jax.named_scope('ln1'):
                a_copy(0).wait()
                layer_norm(1)
                a_copy(1).start()

        @pl.when(p == 1)
        def _():
            a_copy(0).start()
            x_copy(1).start()
            bd_row[...] = bd_ref[...].astype(F32).reshape(1, -1)
            with jax.named_scope('tables'):
                tables()

        def steps(i, c):
            s = p * chunks + 2 * i
            w_copy(s + 1).wait()

            @pl.when(s + 2 < total)
            def _():
                w_copy(s + 2).wait()

            @pl.when(s + 3 < total)
            def _():
                w_copy(s + 3).start()

            @pl.when(s + 4 < total)
            def _():
                w_copy(s + 4).start()

            @pl.when((i == 1) & (p == 2))
            def _():
                with jax.named_scope('flush'):
                    flush(p - 1, 1)

            @pl.when((i == 1) & (p > 2) & (lax.rem(p, 2) == 0))
            def _():
                with jax.named_scope('flush'):
                    flush(p - 1, 2)

            relayout(s + 1, wb1)
            multiply(2 * i, wb0)
            relayout(s + 2, wb0)
            multiply(2 * i + 1, wb1)
            return c

        lax.fori_loop(0, chunks // 2, steps, 0)
        with jax.named_scope('epi'):
            epilogue(p)
        l_copy(p).start()

        @pl.when(mine(p))
        def _():
            own_copy(p).start()

        @pl.when(p == 0)
        def _():
            with jax.named_scope('flush0'):
                flush(p, 1)

        return c

    lax.fori_loop(0, pieces, project, 0)
    with jax.named_scope('lastflush'):
        flush(pieces - 1, 2)
        flush_rows()
    a_copy(1).wait()

    coef = math.log2(math.e) / math.sqrt(dim)
    per = q_blk // chunk
    kn = k_blk // chunk
    ratio = q_blk // k_blk

    def row_copies(b):
        slot = lax.rem(b, 2)
        return [pltpu.make_async_copy(rc.at[kind, b], buf.at[slot], row_sem.at[kind, slot])
                for kind, buf in ((0, qb), (1, kb), (2, vb))]

    def ctx_copies(b):
        slot = lax.rem(b, 2)
        at = pl.ds(pl.multiple_of(b * chunk, chunk), chunk)
        return [pltpu.make_async_copy(cb.at[slot], c_snd.at[:, at], c_sem.at[0, slot]),
                pltpu.make_async_copy(cb.at[slot, me], c_rc.at[me, at], c_sem.at[1, slot])]

    def attend_row(b):
        slot = lax.rem(b, 2)
        ctx = ctx_ref[b]
        step_v = min(512, seq)
        for c in range(seq // step_v):
            m = step_v // chunk
            vt[:, c * step_v:(c + 1) * step_v] = vb[slot, c * m:(c + 1) * m].reshape(step_v, dim).T
        blocks = seq // q_blk

        def scores(qi, j, s_slot, masked, prev):
            k_rows = kb[slot, pl.ds(j * kn, kn)].reshape(k_blk, dim)
            q_rows = qb[slot, pl.ds(qi * per, per)].reshape(q_blk, dim)
            s = lax.dot_general(k_rows, q_rows, (((1,), (1,)), ((), ())), preferred_element_type=F32)
            if masked:
                kpos = j * k_blk + lax.broadcasted_iota(jnp.int32, s.shape, 0)
                lim = jnp.maximum(ctx, qi * q_blk + 1 + lax.broadcasted_iota(jnp.int32, (1, q_blk), 1))
                s = jnp.where(kpos < lim, s, -jnp.inf)
            s_buf[s_slot] = s
            top = jnp.max(s, axis=0, keepdims=True) * coef
            if prev is None:
                m_buf[s_slot] = top
                a_buf[s_slot] = jnp.zeros_like(top)
            else:
                m_old = m_buf[prev]
                m_new = jnp.maximum(m_old, top)
                m_buf[s_slot] = m_new
                a_buf[s_slot] = jnp.exp2(m_old - m_new)

        def values(j, s_slot):
            v_cols = vt[:, pl.ds(pl.multiple_of(j * k_blk, k_blk), k_blk)]
            scale = a_buf[s_slot]
            p = jnp.exp2(s_buf[s_slot] * coef - m_buf[s_slot])
            l_s[...] = l_s[...] * scale + jnp.sum(p.reshape(k_blk // 8, 8, q_blk), axis=0)
            acc_s[...] = acc_s[...] * scale + jnp.dot(v_cols, p.astype(BF16), preferred_element_type=F32)

        def q_loop(qi, _):
            q0 = qi * q_blk
            l_s[...] = jnp.zeros_like(l_s)
            acc_s[...] = jnp.zeros_like(acc_s)

            def pair(i, masked):
                scores(qi, 2 * i + 1, 1, masked, 0)
                values(2 * i, 0)
                scores(qi, 2 * i + 2, 0, masked, 1)
                values(2 * i + 1, 1)

            last = (jnp.maximum(high, q0 + q_blk) + 2 * k_blk - 1) // (2 * k_blk) - 1
            full = jnp.minimum((jnp.maximum(low, q0) // k_blk - 1) // 2, last)
            lax.fori_loop(0, full, lambda i, c: (pair(i, False), c)[1], 0)
            lax.fori_loop(full, last, lambda i, c: (pair(i, True), c)[1], 0)
            scores(qi, 2 * last + 1, 1, True, 0)
            values(2 * last, 0)
            scores(jnp.minimum(qi + 1, blocks - 1), 0, 0, False, None)
            values(2 * last + 1, 1)
            inv = 1.0 / jnp.sum(l_s[...], axis=0, keepdims=True)
            cb[slot, pl.ds(qi * per, per)] = (acc_s[...] * inv).T.astype(BF16).reshape(per, chunk, dim)
            return 0

        scores(0, 0, 0, False, None)
        lax.fori_loop(0, blocks, q_loop, 0)

    def arrived(at, group_id):
        got = rc.at[:, at, pl.ds(0, n - 1)]
        pltpu.make_async_copy(got, got, rcv_sem.at[group_id]).wait()

    def give(b, first, count, sem):
        with jax.named_scope('ctxwait'):
            for r in range(count):
                for copy in ctx_copies(b - count + 1 + r):
                    copy.wait()

        for_peers(lambda dest: c_send(dest, first, count, sem).start())

    starts = ((0, pl.ds(0, half_rows)), (half_rows, pl.ds(half_rows, 2)), (rows - 2, pl.ds(rows - 2, 2)))

    def attend(b, c):
        for group_id, (row, at) in enumerate(starts):
            @pl.when(b == row)
            def _():
                with jax.named_scope(f'arr{group_id}'):
                    arrived(at, group_id)
                for copy in row_copies(b):
                    copy.start()

        @pl.when((b < half_rows - 1) | ((b >= half_rows) & (lax.rem(b, 2) == 0)))
        def _():
            for copy in row_copies(b + 1):
                copy.start()

        with jax.named_scope('rowwait'):
            for copy in row_copies(b):
                copy.wait()
        with jax.named_scope('row'):
            attend_row(b)
        for copy in ctx_copies(b):
            copy.start()

        @pl.when((lax.rem(b, 2) == 1) & (b < half_rows))
        def _():
            give(b, b - 1, 2, 0)

        @pl.when(b == rows - 3)
        def _():
            give(b, b - 1, 2, 1)

        @pl.when(b == rows - 1)
        def _():
            give(b, b - 1, 2, 2)

        return c

    lax.fori_loop(0, rows, attend, 0)

    steps = depth // k_tile
    wide = group * dim

    def wd_copy(i, buf, slot):
        return pltpu.make_async_copy(
            wd_ref.at[pl.ds(pl.multiple_of(lax.rem(i, steps) * k_tile, k_tile), k_tile), pl.ds(pl.multiple_of(i // steps * wide, wide), wide)],
            buf, w_sem.at[slot])

    def dense_rows(first, count, sem):
        def lhs_copy(h):
            return pltpu.make_async_copy(
                c_rc.at[h, pl.ds(first, count)], ab.at[pl.ds(0, count), pl.ds(pl.multiple_of(h * dim, dim), dim)], lhs_sem)

        wd_copy(0, wb0, 0).start()
        a_back = pltpu.make_async_copy(a_out.at[pl.ds(first, count)], xb.at[pl.ds(0, count)], x_sem)
        a_back.start()
        got = c_rc.at[pl.ds(0, n - 1), pl.ds(first, count)]
        with jax.named_scope(f'cr{sem}'):
            pltpu.make_async_copy(got, got, cr_sem.at[sem]).wait()
        lax.fori_loop(0, heads, lambda h, c: (lhs_copy(h).start(), c)[1], 0)
        with jax.named_scope('lhswait'):
            lax.fori_loop(0, heads, lambda h, c: (lhs_copy(h).wait(), c)[1], 0)
            a_back.wait()

        def dense_half(t, c):
            def two(i, c):
                s = t * steps + 2 * i
                wd_copy(s + 1, wb1, 1).start()
                wd_copy(s, wb0, 0).wait()
                multiply(2 * i, wb0, count)

                @pl.when(s + 2 < 2 * steps)
                def _():
                    wd_copy(s + 2, wb0, 0).start()

                wd_copy(s + 1, wb1, 1).wait()
                multiply(2 * i + 1, wb1, count)
                return c

            lax.fori_loop(0, steps // 2, two, 0)
            for u in range(wide // 256):
                cols = pl.ds(pl.multiple_of(t * wide + u * 256, 256), 256)
                part = slice(u * 256, (u + 1) * 256)
                shift = bd_row[:, cols]
                xb[:count, cols] = (xb[:count, cols].astype(F32) * ALPHA + (acc[:count, part] + shift)).astype(BF16)
                acc[:count, part] = jnp.zeros((count, 256), F32)
            return c

        with jax.named_scope('dense'):
            lax.fori_loop(0, depth // wide, dense_half, 0)
        done = pltpu.make_async_copy(xb.at[pl.ds(0, count)], half_out.at[pl.ds(first, count)], x_sem)
        done.start()
        done.wait()

    dense_rows(0, half_tok, 0)

    for group_id, (_, at) in enumerate(starts):
        gone = snd.at[:, pl.ds(0, n - 1), at]
        with jax.named_scope(f'drainsnd{group_id}'):
            pltpu.make_async_copy(gone, gone, snd_sem.at[group_id]).wait()
    gone = c_snd.at[pl.ds(0, n - 1)]
    with jax.named_scope('draincs'):
        pltpu.make_async_copy(gone, gone, cs_sem).wait()
    for sem in range(2):
        got = c_rc.at[pl.ds(0, n - 1), pl.ds(half_tok + sem * 2 * chunk, 2 * chunk)]
        with jax.named_scope(f'draincr{sem}'):
            pltpu.make_async_copy(got, got, cr_sem.at[1 + sem]).wait()


def exchange(n, ctx_len, x, gamma, beta, w_rows, bias, pos_ids, block_ids, freq, w_dense, b_dense, rows, chunk, k_tile=512, q_blk=512, k_blk=512, low=CTX_LOW, high=CTX_HIGH):
    tokens, depth = x.shape
    _, kinds, heads, dim = w_rows.shape
    half_rows, group = split_sizes(rows, heads)
    half_tok = half_rows * chunk
    seq = n * chunk
    any_spec = pl.BlockSpec(memory_space=pl.ANY)
    vmem = pl.BlockSpec(memory_space=pltpu.VMEM)
    smem = pl.BlockSpec(memory_space=pltpu.SMEM)
    dma = pltpu.SemaphoreType.DMA
    cfg = (n, depth, k_tile, q_blk, k_blk, low, high)
    return pl.pallas_call(
        functools.partial(exchange_kernel, cfg),
        in_specs=[smem, any_spec, vmem, vmem, any_spec, vmem, vmem, vmem, vmem, any_spec, vmem],
        out_specs=[any_spec] * 6,
        out_shape=[
            jax.ShapeDtypeStruct((tokens, depth), BF16),
            jax.ShapeDtypeStruct((kinds, heads, rows, chunk, dim), BF16),
            jax.ShapeDtypeStruct((kinds, rows, n, chunk, dim), BF16),
            jax.ShapeDtypeStruct((n, tokens, dim), BF16),
            jax.ShapeDtypeStruct((heads, tokens, dim), BF16),
            jax.ShapeDtypeStruct((half_tok, depth), BF16),
        ],
        scratch_shapes=[
            pltpu.VMEM((half_tok, depth), BF16),
            pltpu.VMEM((half_tok, depth), BF16),
            pltpu.VMEM((4, k_tile, group, dim), BF16),
            pltpu.VMEM((k_tile, group * dim), BF16),
            pltpu.VMEM((k_tile, group * dim), BF16),
            pltpu.VMEM((half_tok, group * dim), F32),
            pltpu.VMEM((2, group, half_rows, chunk, dim), BF16),
            pltpu.VMEM((2, n, chunk, dim), BF16),
            pltpu.VMEM((2, n, chunk, dim), BF16),
            pltpu.VMEM((2, n, chunk, dim), BF16),
            pltpu.VMEM((2, n, chunk, dim), BF16),
            pltpu.VMEM((dim, seq), BF16),
            pltpu.VMEM((2, k_blk, q_blk), F32),
            pltpu.VMEM((2, 1, q_blk), F32),
            pltpu.VMEM((2, 1, q_blk), F32),
            pltpu.VMEM((8, q_blk), F32),
            pltpu.VMEM((dim, q_blk), F32),
            pltpu.VMEM((tokens, dim), F32),
            pltpu.VMEM((tokens, dim), F32),
            pltpu.VMEM((1, depth), F32),
            dma, dma, dma((4,)), dma((2,)), dma((2,)), dma((3,)), dma((3,)), dma((3, 2)), dma((2, 2)), dma, dma((3,)), dma,
        ],
        compiler_params=pltpu.CompilerParams(vmem_limit_bytes=VMEM_CAP, collective_id=0, has_side_effects=True),
        cost_estimate=pl.CostEstimate(flops=2 * tokens * depth * kinds * heads * dim, bytes_accessed=4 * depth * kinds * heads * dim, transcendentals=0),
        name="exchange",
    )(ctx_len, x, gamma, beta, w_rows, bias, pos_ids, block_ids, freq, w_dense, b_dense)


def dense_kernel(c_ref, w_ref, b_ref, a_hbm, kv_hbm, half_hbm, o_hbm, ko_hbm, vo_hbm, lhs, acc, a_buf, kv_buf, h_buf, a_sem, in_sem, out_sem, o_sem):
    heads_blk, tokens, dim = c_ref.shape
    side, step = pl.program_id(0), pl.program_id(1)
    steps = pl.num_programs(1)
    turns = 2 * steps
    turn = side * steps + step
    wide = w_ref.shape[1]
    rest = pl.ds(half_hbm.shape[0], tokens)
    share = half_hbm.shape[0] // turns

    def cols_of(i):
        return pl.ds(pl.multiple_of(i * wide, wide), wide)

    def a_copy(i):
        return pltpu.make_async_copy(a_hbm.at[rest, cols_of(i)], a_buf.at[i], a_sem.at[i])

    def o_copy(i):
        return pltpu.make_async_copy(a_buf.at[i], o_hbm.at[rest, cols_of(i)], o_sem.at[i])

    def part(i):
        return pl.ds(pl.multiple_of(i * share, share), share)

    def in_copies(i):
        slot = lax.rem(i, 2)
        return [pltpu.make_async_copy(kv_hbm.at[pl.ds(1, 2), i], kv_buf.at[slot], in_sem.at[0, slot]),
                pltpu.make_async_copy(half_hbm.at[part(i)], h_buf.at[slot], in_sem.at[1, slot])]

    def out_copies(i):
        slot = lax.rem(i, 2)
        return [pltpu.make_async_copy(kv_buf.at[slot, 0], ko_hbm.at[i], out_sem.at[0, slot]),
                pltpu.make_async_copy(kv_buf.at[slot, 1], vo_hbm.at[i], out_sem.at[1, slot]),
                pltpu.make_async_copy(h_buf.at[slot], o_hbm.at[part(i)], out_sem.at[2, slot])]

    def start(copies):
        for copy in copies:
            copy.start()

    def wait(copies):
        for copy in copies:
            copy.wait()

    @pl.when(turn == 0)
    def _():
        start(in_copies(0))
        start([a_copy(0), a_copy(1)])

    wait(in_copies(turn))
    start(out_copies(turn))

    @pl.when(turn > 0)
    def _():
        wait(out_copies(turn - 1))

    @pl.when(turn + 1 < turns)
    def _():
        start(in_copies(turn + 1))

    depth_blk = heads_blk * dim
    base = pl.multiple_of(step * depth_blk, depth_blk)

    @pl.when(side == 0)
    def _():
        for h in range(heads_blk):
            lhs[:, pl.ds(base + h * dim, dim)] = c_ref[h]

    left = lhs[:, pl.ds(base, depth_blk)]

    def product(first):
        for t in range(wide // 256):
            cols = slice(t * 256, (t + 1) * 256)
            prod = jnp.dot(left, w_ref[:, cols], preferred_element_type=F32)
            acc[:, cols] = prod if first else acc[:, cols] + prod

    @pl.when(step == 0)
    def _():
        product(True)

    @pl.when(step > 0)
    def _():
        product(False)

    @pl.when(step == steps - 1)
    def _():
        a_copy(side).wait()
        a_buf[side] = (a_buf[side].astype(F32) * ALPHA + (acc[...] + b_ref[...].astype(F32).reshape(1, -1))).astype(BF16)
        o_copy(side).start()

    @pl.when(turn == turns - 1)
    def _():
        wait(out_copies(turn))
        wait([o_copy(0), o_copy(1)])


def dense(context, w_dense, bias, normed, kv, half_out):
    heads, tokens, dim = context.shape
    depth, width = w_dense.shape
    kinds, rows, seq, _ = kv.shape
    last_tok = tokens - half_out.shape[0]
    steps = rows // 2
    any_spec = pl.BlockSpec(memory_space=pl.ANY)
    wide = width // 2
    dma = pltpu.SemaphoreType.DMA
    return pl.pallas_call(
        dense_kernel,
        grid=(2, steps),
        in_specs=[
            pl.BlockSpec((heads // steps, last_tok, dim), lambda i, k: (lax.select(i == 0, k, steps - 1), tokens // last_tok - 1, 0)),
            pl.BlockSpec((depth // steps, wide), lambda i, k: (k, i)),
            pl.BlockSpec((wide,), lambda i, k: (i,)),
            any_spec,
            any_spec,
            any_spec,
        ],
        out_specs=[any_spec] * 3,
        out_shape=[
            jax.ShapeDtypeStruct((tokens, width), BF16),
            jax.ShapeDtypeStruct((rows, seq, dim), BF16),
            jax.ShapeDtypeStruct((rows, seq, dim), BF16),
        ],
        scratch_shapes=[
            pltpu.VMEM((last_tok, depth), BF16),
            pltpu.VMEM((last_tok, wide), F32),
            pltpu.VMEM((2, last_tok, wide), BF16),
            pltpu.VMEM((2, 2, seq, dim), BF16),
            pltpu.VMEM((2, half_out.shape[0] // (2 * steps), width), BF16),
            dma((2,)), dma((2, 2)), dma((3, 2)), dma((2,)),
        ],
        compiler_params=pltpu.CompilerParams(vmem_limit_bytes=VMEM_CAP),
        cost_estimate=pl.CostEstimate(flops=2 * last_tok * depth * width, bytes_accessed=2 * depth * width, transcendentals=0),
        name="dense",
    )(context, w_dense, bias, normed, kv, half_out)


def solution(mesh):
    seq_spec = P('dp', 'sp', None)
    row_spec = P('dp', 'sp')
    head_spec = P('dp', None, 'sp', None)
    rep = P()
    devices = mesh.shape['sp']

    def local_block(hidden, pos_ids, block_ids, ctx_len, ln_gamma, ln_beta, w_qkv, b_qkv, w_dense, b_dense):
        rows, chunk, width = hidden.shape
        depth, heads, kinds, dim = w_qkv.shape
        seq = chunk * devices
        tokens = rows * chunk
        w_rows = jnp.transpose(w_qkv, (0, 2, 1, 3))
        bias = jnp.transpose(b_qkv, (1, 0, 2))
        normed, _, recv, _, context, half_out = exchange(
            devices, ctx_len, hidden.reshape(tokens, width), ln_gamma, ln_beta, w_rows, bias, pos_ids, block_ids, rotary_freq(dim), w_dense, b_dense, rows, chunk)
        out, keys, values = dense(context, w_dense, b_dense, normed, recv.reshape(kinds, rows, seq, dim), half_out)
        return out.reshape(rows, chunk, width), keys.reshape(rows, seq, 1, dim), values.reshape(rows, seq, 1, dim)

    return jax.shard_map(local_block, mesh=mesh, in_specs=(seq_spec, row_spec, row_spec, P('dp'), rep, rep, rep, rep, rep, rep), out_specs=(seq_spec, head_spec, head_spec), check_vma=False)
```

```python
import functools
import math

import jax
import jax.numpy as jnp
from jax import lax
from jax.experimental import pallas as pl
from jax.experimental.pallas import tpu as pltpu
from jax.sharding import PartitionSpec as P

ALPHA = math.sqrt(56.0)
ROPE_BASE = 10000.0
LN_EPS = 1e-5
CTX_LOW = 1024
CTX_HIGH = 3072
F32 = jnp.float32
BF16 = jnp.bfloat16
VMEM_CAP = 60000 * 1024
MESH_ID = pl.DeviceIdType.MESH


SHIFT_PAIRS = (((1, 0), (3, 2)), ((1, 1), (3, 3)), ((3, 0), (1, 2)), ((0, 1), (2, 3)),
               ((1, 3), (3, 1)), ((0, 3), (2, 1)), ((2, 0), (0, 2)), ((2, 2), (0, 0)))


def shift_codes(side):
    if side == 4:
        pairs = SHIFT_PAIRS
    else:
        shifts = [(i % side, i // side) for i in range(side * side)]
        pairs = tuple(zip(shifts[0::2], shifts[1::2]))
    return len(pairs), [sum(pair[k // 2][k % 2] * side ** u for u, pair in enumerate(pairs)) for k in range(4)]


def rotary_freq(dim):
    half = dim // 2
    lane = lax.rem(lax.broadcasted_iota(jnp.int32, (1, dim), 1), half // 2)
    return ROPE_BASE ** (-(2 * lane).astype(F32) / half)


def split_sizes(rows, heads):
    return rows // 2, heads // 2


def exchange_kernel(cfg, ctx_ref, x_ref, g_ref, be_ref, w_ref, bias_ref, pos_ref, blk_ref, freq_ref, wd_ref, bd_ref,
                    a_out, snd, rc, c_snd, c_rc, half_out,
                    xb, ab, wbuf, wb0, wb1, acc, sb, qb, kb, vb, cb, vt, s_buf, m_buf, a_buf, l_s, acc_s, cos_ref, sin_ref, bd_row,
                    x_sem, a_sem, w_sem, l_sem, o_sem, snd_sem, rcv_sem, row_sem, c_sem, cs_sem, cr_sem, lhs_sem):
    n, depth, k_tile, q_blk, k_blk, low, high = cfg
    _, heads, rows, chunk, dim = snd.shape
    half_rows, group = split_sizes(rows, heads)
    half_tok = half_rows * chunk
    seq = n * chunk
    pieces = 12
    chunks = depth // k_tile
    total = pieces * chunks
    me = lax.axis_index('sp')

    barrier = pltpu.get_barrier_semaphore()

    def greet(i, c):
        pl.semaphore_signal(barrier, inc=1, device_id={'sp': lax.rem(me + i, n)}, device_id_type=MESH_ID)
        return c

    def piece_of(p):
        hf = p // 6
        kind = 2 - lax.rem(p, 6) // 2
        hh = lax.rem(p, 2)
        return hf, kind, hh

    def w_copy(s):
        _, kind, hh = piece_of(s // chunks)
        c = lax.rem(s, chunks)
        slot = lax.rem(s, 4)
        return pltpu.make_async_copy(
            w_ref.at[pl.ds(pl.multiple_of(c * k_tile, k_tile), k_tile), kind, pl.ds(pl.multiple_of(hh * group, group), group)],
            wbuf.at[slot], w_sem.at[slot])

    def x_copy(hf):
        return pltpu.make_async_copy(x_ref.at[pl.ds(pl.multiple_of(hf * half_tok, half_tok), half_tok)], xb, x_sem)

    def a_copy(hf):
        return pltpu.make_async_copy(ab, a_out.at[pl.ds(pl.multiple_of(hf * half_tok, half_tok), half_tok)], a_sem)

    def l_copy(p):
        hf, kind, hh = piece_of(p)
        slot = lax.rem(p, 2)
        return pltpu.make_async_copy(
            sb.at[slot],
            snd.at[kind, pl.ds(pl.multiple_of(hh * group, group), group), pl.ds(hf * half_rows, half_rows)],
            l_sem.at[slot])

    def own_copy(p):
        hf, kind, hh = piece_of(p)
        slot = lax.rem(p, 2)
        return pltpu.make_async_copy(
            sb.at[slot, lax.rem(me, group)],
            rc.at[kind, pl.ds(hf * half_rows, half_rows), me],
            o_sem.at[slot])

    def mine(p):
        return piece_of(p)[2] == me // group

    def send(kind, head, pair, group_id):
        at = pl.ds(2 * pair, 2)
        pltpu.make_async_remote_copy(
            src_ref=snd.at[kind, head, at], dst_ref=rc.at[kind, at, me],
            send_sem=snd_sem.at[group_id], recv_sem=rcv_sem.at[group_id],
            device_id={'sp': head}, device_id_type=MESH_ID).start()

    def c_send(dest, first, count, sem):
        at = pl.ds(pl.multiple_of(first * chunk, chunk), count * chunk)
        return pltpu.make_async_remote_copy(
            src_ref=c_snd.at[dest, at], dst_ref=c_rc.at[me, at],
            send_sem=cs_sem, recv_sem=cr_sem.at[sem], device_id={'sp': dest}, device_id_type=MESH_ID)

    def layer_norm(hf):
        x_copy(hf).wait()
        sub = 16
        tile = min(64, half_tok)
        lanes = [slice(c * 128, (c + 1) * 128) for c in range(depth // 128)]

        def body(i, c):
            ats = [pl.ds(pl.multiple_of(i * tile + u * sub, sub), sub) for u in range(tile // sub)]
            means, scales = [], []
            for at in ats:
                total = sum(xb[at, cols].astype(F32) for cols in lanes)
                means.append(jnp.sum(total, axis=-1, keepdims=True) * (1.0 / depth))
            for at, mean in zip(ats, means):
                total = sum(jnp.square(xb[at, cols].astype(F32) - mean) for cols in lanes)
                scales.append(lax.rsqrt(jnp.sum(total, axis=-1, keepdims=True) * (1.0 / depth) + LN_EPS))
            for cols in lanes:
                gain = g_ref[cols].astype(F32).reshape(1, 128)
                shift = be_ref[cols].astype(F32).reshape(1, 128)
                for at, mean, scale in zip(ats, means, scales):
                    ab[at, cols] = ((xb[at, cols].astype(F32) - mean) * scale * gain + shift).astype(BF16)
            return c

        lax.fori_loop(0, half_tok // tile, body, 0)

    def tables():
        lane = lax.broadcasted_iota(jnp.int32, (1, dim), 1)

        def body(r, c):
            at = pl.ds(pl.multiple_of(r * chunk, chunk), chunk)
            pos = jnp.broadcast_to(pos_ref[pl.ds(r, 1), :].astype(F32), (dim, chunk)).T
            blk = jnp.broadcast_to(blk_ref[pl.ds(r, 1), :].astype(F32), (dim, chunk)).T
            ang = jnp.where(lane < dim // 2, pos, blk) * freq_ref[...]
            sin = jnp.sin(ang)
            cos_ref[at, :] = jnp.cos(ang)
            sin_ref[at, :] = jnp.where(lax.rem(lane, dim // 2) < dim // 4, -sin, sin)
            return c

        lax.fori_loop(0, rows, body, 0)

    def relayout(s, wb):
        slot = lax.rem(s, 4)
        sub = min(64, k_tile)
        for part in range(k_tile // sub):
            lo = part * sub
            tile = jnp.swapaxes(wbuf[slot, lo:lo + sub], 0, 1)
            for head in range(group):
                wb[lo:lo + sub, head * dim:(head + 1) * dim] = tile[head]

    def multiply(c, wb, count=half_tok):
        lhs = ab[:count, pl.ds(pl.multiple_of(c * k_tile, k_tile), k_tile)]
        wide = min(256, group * dim)
        for t in range(group * dim // wide):
            cols = slice(t * wide, (t + 1) * wide)
            acc[:count, cols] += jnp.dot(lhs, wb[:, cols], preferred_element_type=F32)

    def epilogue(p):
        hf, kind, hh = piece_of(p)
        slot = lax.rem(p, 2)
        toks = pl.ds(pl.multiple_of(hf * half_tok, half_tok), half_tok)
        turn = min(4, group)
        bias = bias_ref[kind, pl.ds(pl.multiple_of(hh * group, group), group), :].astype(F32)
        fill = jnp.zeros((half_tok, dim), F32)
        lane = lax.broadcasted_iota(jnp.int32, (1, dim), 1)
        first = lax.rem(lane, dim // 2) < dim // 4

        def biased(h, row):
            cols = pl.ds(pl.multiple_of(h * dim, dim), dim)
            x = (acc[:, cols] + row).astype(BF16)
            acc[:, cols] = fill
            return x

        def rows_of(t):
            return [bias[t * turn + u:t * turn + u + 1, :] for u in range(turn)]

        for t in range(group // turn):
            @pl.when(kind < 2)
            def _():
                for u, row in enumerate(rows_of(t)):
                    h = t * turn + u
                    x = biased(h, row).astype(F32)
                    pair = jnp.where(first, pltpu.roll(x, dim - dim // 4, 1), pltpu.roll(x, dim // 4, 1))
                    x = (x * cos_ref[toks, :] + pair * sin_ref[toks, :]).astype(BF16)
                    sb[slot, h] = x.reshape(half_rows, chunk, dim)

            @pl.when(kind == 2)
            def _():
                for u, row in enumerate(rows_of(t)):
                    h = t * turn + u
                    sb[slot, h] = biased(h, row).reshape(half_rows, chunk, dim)

    side = math.isqrt(n // 2)
    pair_count, codes = shift_codes(side)

    def for_peers(act):
        core = lax.rem(me, 2)

        def sweep(flip, c):
            def one(u, rest):
                digit = [lax.rem(code, side) for code in rest]
                for r in range(2):
                    second = lax.rem(r + core, 2)
                    dx = digit[0] + second * (digit[2] - digit[0])
                    dy = digit[1] + second * (digit[3] - digit[1])
                    y = lax.rem(me // (2 * side) + dy, side)
                    x = lax.rem(me // 2 + dx, side)
                    peer = (y * side + x) * 2 + lax.rem(me + flip, 2)

                    @pl.when(peer != me)
                    def _():
                        act(peer)

                return tuple(code // side for code in rest)

            lax.fori_loop(0, pair_count, one, tuple(jnp.int32(code) for code in codes))
            return c

        lax.fori_loop(0, 2, sweep, 0)

    def landed(p):
        l_copy(p).wait()

        @pl.when(mine(p))
        def _():
            own_copy(p).wait()

    def flush(p, count):
        hf, kind, hh = piece_of(p)
        landed(p)
        if count == 2:
            landed(p - 1)

        def out(pair, group_id):
            def act(head):
                if count == 2:
                    send(kind, head, pair, group_id)
                else:
                    @pl.when(head // group == hh)
                    def _():
                        send(kind, head, pair, group_id)

            for_peers(act)

        out(2 * hf, hf)

        @pl.when(hf == 0)
        def _():
            out(1, 0)

    def flush_rows():
        def one(i, c):
            for_peers(lambda head: send(2 - i, head, rows // 2 - 1, 2))
            return c

        lax.fori_loop(0, 3, one, 0)

    x_copy(0).start()
    for s in range(3):
        w_copy(s).start()
    lax.fori_loop(1, n, greet, 0)
    acc[...] = jnp.zeros_like(acc)
    w_copy(0).wait()
    relayout(0, wb0)
    with jax.named_scope('ln0'):
        layer_norm(0)
    with jax.named_scope('barrier_wait'):
        pl.semaphore_wait(barrier, n - 1)

    def project(p, c):
        @pl.when(p == 6)
        def _():
            with jax.named_scope('ln1'):
                a_copy(0).wait()
                layer_norm(1)
                a_copy(1).start()

        @pl.when(p == 1)
        def _():
            a_copy(0).start()
            x_copy(1).start()
            bd_row[...] = bd_ref[...].astype(F32).reshape(1, -1)
            with jax.named_scope('tables'):
                tables()

        def steps(i, c):
            s = p * chunks + 2 * i
            w_copy(s + 1).wait()

            @pl.when(s + 2 < total)
            def _():
                w_copy(s + 2).wait()

            @pl.when(s + 3 < total)
            def _():
                w_copy(s + 3).start()

            @pl.when(s + 4 < total)
            def _():
                w_copy(s + 4).start()

            @pl.when((i == 1) & (p == 2))
            def _():
                with jax.named_scope('flush'):
                    flush(p - 1, 1)

            @pl.when((i == 1) & (p > 2) & (lax.rem(p, 2) == 0))
            def _():
                with jax.named_scope('flush'):
                    flush(p - 1, 2)

            relayout(s + 1, wb1)
            multiply(2 * i, wb0)
            relayout(s + 2, wb0)
            multiply(2 * i + 1, wb1)
            return c

        lax.fori_loop(0, chunks // 2, steps, 0)
        with jax.named_scope('epi'):
            epilogue(p)
        l_copy(p).start()

        @pl.when(mine(p))
        def _():
            own_copy(p).start()

        @pl.when(p == 0)
        def _():
            with jax.named_scope('flush0'):
                flush(p, 1)

        return c

    lax.fori_loop(0, pieces, project, 0)
    with jax.named_scope('lastflush'):
        flush(pieces - 1, 2)
        flush_rows()
    a_copy(1).wait()

    coef = math.log2(math.e) / math.sqrt(dim)
    per = q_blk // chunk
    kn = k_blk // chunk
    ratio = q_blk // k_blk

    def row_copies(b):
        slot = lax.rem(b, 2)
        return [pltpu.make_async_copy(rc.at[kind, b], buf.at[slot], row_sem.at[kind, slot])
                for kind, buf in ((0, qb), (1, kb), (2, vb))]

    def ctx_copies(b):
        slot = lax.rem(b, 2)
        at = pl.ds(pl.multiple_of(b * chunk, chunk), chunk)
        return [pltpu.make_async_copy(cb.at[slot], c_snd.at[:, at], c_sem.at[0, slot]),
                pltpu.make_async_copy(cb.at[slot, me], c_rc.at[me, at], c_sem.at[1, slot])]

    def attend_row(b):
        slot = lax.rem(b, 2)
        ctx = ctx_ref[b]
        step_v = min(512, seq)
        for c in range(seq // step_v):
            m = step_v // chunk
            vt[:, c * step_v:(c + 1) * step_v] = vb[slot, c * m:(c + 1) * m].reshape(step_v, dim).T
        blocks = seq // q_blk

        def scores(qi, j, s_slot, masked, prev):
            k_rows = kb[slot, pl.ds(j * kn, kn)].reshape(k_blk, dim)
            q_rows = qb[slot, pl.ds(qi * per, per)].reshape(q_blk, dim)
            s = lax.dot_general(k_rows, q_rows, (((1,), (1,)), ((), ())), preferred_element_type=F32)
            if masked:
                kpos = j * k_blk + lax.broadcasted_iota(jnp.int32, s.shape, 0)
                lim = jnp.maximum(ctx, qi * q_blk + 1 + lax.broadcasted_iota(jnp.int32, (1, q_blk), 1))
                s = jnp.where(kpos < lim, s, -jnp.inf)
            s_buf[s_slot] = s
            top = jnp.max(s, axis=0, keepdims=True) * coef
            if prev is None:
                m_buf[s_slot] = top
                a_buf[s_slot] = jnp.zeros_like(top)
            else:
                m_old = m_buf[prev]
                m_new = jnp.maximum(m_old, top)
                m_buf[s_slot] = m_new
                a_buf[s_slot] = jnp.exp2(m_old - m_new)

        def values(j, s_slot):
            v_cols = vt[:, pl.ds(pl.multiple_of(j * k_blk, k_blk), k_blk)]
            scale = a_buf[s_slot]
            p = jnp.exp2(s_buf[s_slot] * coef - m_buf[s_slot])
            l_s[...] = l_s[...] * scale + jnp.sum(p.reshape(k_blk // 8, 8, q_blk), axis=0)
            acc_s[...] = acc_s[...] * scale + jnp.dot(v_cols, p.astype(BF16), preferred_element_type=F32)

        def q_loop(qi, _):
            q0 = qi * q_blk
            l_s[...] = jnp.zeros_like(l_s)
            acc_s[...] = jnp.zeros_like(acc_s)

            def pair(i, masked):
                scores(qi, 2 * i + 1, 1, masked, 0)
                values(2 * i, 0)
                scores(qi, 2 * i + 2, 0, masked, 1)
                values(2 * i + 1, 1)

            last = (jnp.maximum(high, q0 + q_blk) + 2 * k_blk - 1) // (2 * k_blk) - 1
            full = jnp.minimum((jnp.maximum(low, q0) // k_blk - 1) // 2, last)
            lax.fori_loop(0, full, lambda i, c: (pair(i, False), c)[1], 0)
            lax.fori_loop(full, last, lambda i, c: (pair(i, True), c)[1], 0)
            scores(qi, 2 * last + 1, 1, True, 0)
            values(2 * last, 0)
            scores(jnp.minimum(qi + 1, blocks - 1), 0, 0, False, None)
            values(2 * last + 1, 1)
            inv = 1.0 / jnp.sum(l_s[...], axis=0, keepdims=True)
            cb[slot, pl.ds(qi * per, per)] = (acc_s[...] * inv).T.astype(BF16).reshape(per, chunk, dim)
            return 0

        scores(0, 0, 0, False, None)
        lax.fori_loop(0, blocks, q_loop, 0)

    def arrived(at, group_id):
        got = rc.at[:, at, pl.ds(0, n - 1)]
        pltpu.make_async_copy(got, got, rcv_sem.at[group_id]).wait()

    def give(b, first, count, sem):
        with jax.named_scope('ctxwait'):
            for r in range(count):
                for copy in ctx_copies(b - count + 1 + r):
                    copy.wait()

        for_peers(lambda dest: c_send(dest, first, count, sem).start())

    starts = ((0, pl.ds(0, half_rows)), (half_rows, pl.ds(half_rows, 2)), (rows - 2, pl.ds(rows - 2, 2)))

    def attend(b, c):
        for group_id, (row, at) in enumerate(starts):
            @pl.when(b == row)
            def _():
                with jax.named_scope(f'arr{group_id}'):
                    arrived(at, group_id)
                for copy in row_copies(b):
                    copy.start()

        @pl.when((b < half_rows - 1) | ((b >= half_rows) & (lax.rem(b, 2) == 0)))
        def _():
            for copy in row_copies(b + 1):
                copy.start()

        with jax.named_scope('rowwait'):
            for copy in row_copies(b):
                copy.wait()
        with jax.named_scope('row'):
            attend_row(b)
        for copy in ctx_copies(b):
            copy.start()

        @pl.when((lax.rem(b, 2) == 1) & (b < half_rows))
        def _():
            give(b, b - 1, 2, 0)

        @pl.when(b == rows - 3)
        def _():
            give(b, b - 1, 2, 1)

        @pl.when(b >= rows - 2)
        def _():
            give(b, b, 1, 2)

        return c

    lax.fori_loop(0, rows, attend, 0)

    steps = depth // k_tile
    wide = group * dim

    def wd_copy(i, buf, slot):
        return pltpu.make_async_copy(
            wd_ref.at[pl.ds(pl.multiple_of(lax.rem(i, steps) * k_tile, k_tile), k_tile), pl.ds(pl.multiple_of(i // steps * wide, wide), wide)],
            buf, w_sem.at[slot])

    def dense_rows(first, count, sem):
        def lhs_copy(h):
            return pltpu.make_async_copy(
                c_rc.at[h, pl.ds(first, count)], ab.at[pl.ds(0, count), pl.ds(pl.multiple_of(h * dim, dim), dim)], lhs_sem)

        wd_copy(0, wb0, 0).start()
        a_back = pltpu.make_async_copy(a_out.at[pl.ds(first, count)], xb.at[pl.ds(0, count)], x_sem)
        a_back.start()
        got = c_rc.at[pl.ds(0, n - 1), pl.ds(first, count)]
        with jax.named_scope(f'cr{sem}'):
            pltpu.make_async_copy(got, got, cr_sem.at[sem]).wait()
        lax.fori_loop(0, heads, lambda h, c: (lhs_copy(h).start(), c)[1], 0)
        with jax.named_scope('lhswait'):
            lax.fori_loop(0, heads, lambda h, c: (lhs_copy(h).wait(), c)[1], 0)
            a_back.wait()

        def dense_half(t, c):
            def two(i, c):
                s = t * steps + 2 * i
                wd_copy(s + 1, wb1, 1).start()
                wd_copy(s, wb0, 0).wait()
                multiply(2 * i, wb0, count)

                @pl.when(s + 2 < 2 * steps)
                def _():
                    wd_copy(s + 2, wb0, 0).start()

                wd_copy(s + 1, wb1, 1).wait()
                multiply(2 * i + 1, wb1, count)
                return c

            lax.fori_loop(0, steps // 2, two, 0)
            for u in range(wide // 256):
                cols = pl.ds(pl.multiple_of(t * wide + u * 256, 256), 256)
                part = slice(u * 256, (u + 1) * 256)
                shift = bd_row[:, cols]
                xb[:count, cols] = (xb[:count, cols].astype(F32) * ALPHA + (acc[:count, part] + shift)).astype(BF16)
                acc[:count, part] = jnp.zeros((count, 256), F32)
            return c

        with jax.named_scope('dense'):
            lax.fori_loop(0, depth // wide, dense_half, 0)
        done = pltpu.make_async_copy(xb.at[pl.ds(0, count)], half_out.at[pl.ds(first, count)], x_sem)
        done.start()
        return done

    done = dense_rows(0, half_tok, 0)

    for group_id, (_, at) in enumerate(starts):
        gone = snd.at[:, pl.ds(0, n - 1), at]
        with jax.named_scope(f'drainsnd{group_id}'):
            pltpu.make_async_copy(gone, gone, snd_sem.at[group_id]).wait()
    gone = c_snd.at[pl.ds(0, n - 1)]
    with jax.named_scope('draincs'):
        pltpu.make_async_copy(gone, gone, cs_sem).wait()
    for sem in range(2):
        got = c_rc.at[pl.ds(0, n - 1), pl.ds(half_tok + sem * 2 * chunk, 2 * chunk)]
        with jax.named_scope(f'draincr{sem}'):
            pltpu.make_async_copy(got, got, cr_sem.at[1 + sem]).wait()
    done.wait()


def exchange(n, ctx_len, x, gamma, beta, w_rows, bias, pos_ids, block_ids, freq, w_dense, b_dense, rows, chunk, k_tile=512, q_blk=512, k_blk=512, low=CTX_LOW, high=CTX_HIGH):
    tokens, depth = x.shape
    _, kinds, heads, dim = w_rows.shape
    half_rows, group = split_sizes(rows, heads)
    half_tok = half_rows * chunk
    seq = n * chunk
    any_spec = pl.BlockSpec(memory_space=pl.ANY)
    vmem = pl.BlockSpec(memory_space=pltpu.VMEM)
    smem = pl.BlockSpec(memory_space=pltpu.SMEM)
    dma = pltpu.SemaphoreType.DMA
    cfg = (n, depth, k_tile, q_blk, k_blk, low, high)
    return pl.pallas_call(
        functools.partial(exchange_kernel, cfg),
        in_specs=[smem, any_spec, vmem, vmem, any_spec, vmem, vmem, vmem, vmem, any_spec, vmem],
        out_specs=[any_spec] * 6,
        out_shape=[
            jax.ShapeDtypeStruct((tokens, depth), BF16),
            jax.ShapeDtypeStruct((kinds, heads, rows, chunk, dim), BF16),
            jax.ShapeDtypeStruct((kinds, rows, n, chunk, dim), BF16),
            jax.ShapeDtypeStruct((n, tokens, dim), BF16),
            jax.ShapeDtypeStruct((heads, tokens, dim), BF16),
            jax.ShapeDtypeStruct((half_tok, depth), BF16),
        ],
        scratch_shapes=[
            pltpu.VMEM((half_tok, depth), BF16),
            pltpu.VMEM((half_tok, depth), BF16),
            pltpu.VMEM((4, k_tile, group, dim), BF16),
            pltpu.VMEM((k_tile, group * dim), BF16),
            pltpu.VMEM((k_tile, group * dim), BF16),
            pltpu.VMEM((half_tok, group * dim), F32),
            pltpu.VMEM((2, group, half_rows, chunk, dim), BF16),
            pltpu.VMEM((2, n, chunk, dim), BF16),
            pltpu.VMEM((2, n, chunk, dim), BF16),
            pltpu.VMEM((2, n, chunk, dim), BF16),
            pltpu.VMEM((2, n, chunk, dim), BF16),
            pltpu.VMEM((dim, seq), BF16),
            pltpu.VMEM((2, k_blk, q_blk), F32),
            pltpu.VMEM((2, 1, q_blk), F32),
            pltpu.VMEM((2, 1, q_blk), F32),
            pltpu.VMEM((8, q_blk), F32),
            pltpu.VMEM((dim, q_blk), F32),
            pltpu.VMEM((tokens, dim), F32),
            pltpu.VMEM((tokens, dim), F32),
            pltpu.VMEM((1, depth), F32),
            dma, dma, dma((4,)), dma((2,)), dma((2,)), dma((3,)), dma((3,)), dma((3, 2)), dma((2, 2)), dma, dma((3,)), dma,
        ],
        compiler_params=pltpu.CompilerParams(vmem_limit_bytes=VMEM_CAP, collective_id=0, has_side_effects=True),
        cost_estimate=pl.CostEstimate(flops=2 * tokens * depth * kinds * heads * dim, bytes_accessed=4 * depth * kinds * heads * dim, transcendentals=0),
        name="exchange",
    )(ctx_len, x, gamma, beta, w_rows, bias, pos_ids, block_ids, freq, w_dense, b_dense)


def dense_kernel(c_ref, w_ref, b_ref, a_hbm, kv_hbm, half_hbm, o_hbm, ko_hbm, vo_hbm, lhs, acc, a_buf, kv_buf, h_buf, a_sem, in_sem, out_sem, o_sem):
    heads_blk, tokens, dim = c_ref.shape
    side, step = pl.program_id(0), pl.program_id(1)
    steps = pl.num_programs(1)
    turns = 2 * steps
    turn = side * steps + step
    wide = w_ref.shape[1]
    rest = pl.ds(half_hbm.shape[0], tokens)
    share = half_hbm.shape[0] // turns

    def cols_of(i):
        return pl.ds(pl.multiple_of(i * wide, wide), wide)

    def a_copy(i):
        return pltpu.make_async_copy(a_hbm.at[rest, cols_of(i)], a_buf.at[i], a_sem.at[i])

    def o_copy(i):
        return pltpu.make_async_copy(a_buf.at[i], o_hbm.at[rest, cols_of(i)], o_sem.at[i])

    def part(i):
        return pl.ds(pl.multiple_of(i * share, share), share)

    def in_copies(i):
        slot = lax.rem(i, 2)
        return [pltpu.make_async_copy(kv_hbm.at[pl.ds(1, 2), i], kv_buf.at[slot], in_sem.at[0, slot]),
                pltpu.make_async_copy(half_hbm.at[part(i)], h_buf.at[slot], in_sem.at[1, slot])]

    def out_copies(i):
        slot = lax.rem(i, 2)
        return [pltpu.make_async_copy(kv_buf.at[slot, 0], ko_hbm.at[i], out_sem.at[0, slot]),
                pltpu.make_async_copy(kv_buf.at[slot, 1], vo_hbm.at[i], out_sem.at[1, slot]),
                pltpu.make_async_copy(h_buf.at[slot], o_hbm.at[part(i)], out_sem.at[2, slot])]

    def start(copies):
        for copy in copies:
            copy.start()

    def wait(copies):
        for copy in copies:
            copy.wait()

    @pl.when(turn == 0)
    def _():
        start(in_copies(0))
        start([a_copy(0), a_copy(1)])

    wait(in_copies(turn))
    start(out_copies(turn))

    @pl.when(turn > 0)
    def _():
        wait(out_copies(turn - 1))

    @pl.when(turn + 1 < turns)
    def _():
        start(in_copies(turn + 1))

    depth_blk = heads_blk * dim
    base = pl.multiple_of(step * depth_blk, depth_blk)

    @pl.when(side == 0)
    def _():
        for h in range(heads_blk):
            lhs[:, pl.ds(base + h * dim, dim)] = c_ref[h]

    left = lhs[:, pl.ds(base, depth_blk)]

    def product(first):
        for t in range(wide // 256):
            cols = slice(t * 256, (t + 1) * 256)
            prod = jnp.dot(left, w_ref[:, cols], preferred_element_type=F32)
            acc[:, cols] = prod if first else acc[:, cols] + prod

    @pl.when(step == 0)
    def _():
        product(True)

    @pl.when(step > 0)
    def _():
        product(False)

    @pl.when(step == steps - 1)
    def _():
        a_copy(side).wait()
        a_buf[side] = (a_buf[side].astype(F32) * ALPHA + (acc[...] + b_ref[...].astype(F32).reshape(1, -1))).astype(BF16)
        o_copy(side).start()

    @pl.when(turn == turns - 1)
    def _():
        wait(out_copies(turn))
        wait([o_copy(0), o_copy(1)])


def dense(context, w_dense, bias, normed, kv, half_out):
    heads, tokens, dim = context.shape
    depth, width = w_dense.shape
    kinds, rows, seq, _ = kv.shape
    last_tok = tokens - half_out.shape[0]
    steps = rows // 2
    any_spec = pl.BlockSpec(memory_space=pl.ANY)
    wide = width // 2
    dma = pltpu.SemaphoreType.DMA
    return pl.pallas_call(
        dense_kernel,
        grid=(2, steps),
        in_specs=[
            pl.BlockSpec((heads // steps, last_tok, dim), lambda i, k: (lax.select(i == 0, k, steps - 1), tokens // last_tok - 1, 0)),
            pl.BlockSpec((depth // steps, wide), lambda i, k: (k, i)),
            pl.BlockSpec((wide,), lambda i, k: (i,)),
            any_spec,
            any_spec,
            any_spec,
        ],
        out_specs=[any_spec] * 3,
        out_shape=[
            jax.ShapeDtypeStruct((tokens, width), BF16),
            jax.ShapeDtypeStruct((rows, seq, dim), BF16),
            jax.ShapeDtypeStruct((rows, seq, dim), BF16),
        ],
        scratch_shapes=[
            pltpu.VMEM((last_tok, depth), BF16),
            pltpu.VMEM((last_tok, wide), F32),
            pltpu.VMEM((2, last_tok, wide), BF16),
            pltpu.VMEM((2, 2, seq, dim), BF16),
            pltpu.VMEM((2, half_out.shape[0] // (2 * steps), width), BF16),
            dma((2,)), dma((2, 2)), dma((3, 2)), dma((2,)),
        ],
        compiler_params=pltpu.CompilerParams(vmem_limit_bytes=VMEM_CAP),
        cost_estimate=pl.CostEstimate(flops=2 * last_tok * depth * width, bytes_accessed=2 * depth * width, transcendentals=0),
        name="dense",
    )(context, w_dense, bias, normed, kv, half_out)


def solution(mesh):
    seq_spec = P('dp', 'sp', None)
    row_spec = P('dp', 'sp')
    head_spec = P('dp', None, 'sp', None)
    rep = P()
    devices = mesh.shape['sp']

    def local_block(hidden, pos_ids, block_ids, ctx_len, ln_gamma, ln_beta, w_qkv, b_qkv, w_dense, b_dense):
        rows, chunk, width = hidden.shape
        depth, heads, kinds, dim = w_qkv.shape
        seq = chunk * devices
        tokens = rows * chunk
        w_rows = jnp.transpose(w_qkv, (0, 2, 1, 3))
        bias = jnp.transpose(b_qkv, (1, 0, 2))
        normed, _, recv, _, context, half_out = exchange(
            devices, ctx_len, hidden.reshape(tokens, width), ln_gamma, ln_beta, w_rows, bias, pos_ids, block_ids, rotary_freq(dim), w_dense, b_dense, rows, chunk)
        out, keys, values = dense(context, w_dense, b_dense, normed, recv.reshape(kinds, rows, seq, dim), half_out)
        return out.reshape(rows, chunk, width), keys.reshape(rows, seq, 1, dim), values.reshape(rows, seq, 1, dim)

    return jax.shard_map(local_block, mesh=mesh, in_specs=(seq_spec, row_spec, row_spec, P('dp'), rep, rep, rep, rep, rep, rep), out_specs=(seq_spec, head_spec, head_spec), check_vma=False)
```
